512 devices in a mesh: groups: 2 (over y), ep: 32 (over z, core), tp: 8 (over x).
Axes of the slice: x: 8, y: 2, z: 16, core: 2. Of those that a mesh axis runs over, the one named last changes fastest.
The devices are a block of a 8x8x16 slice.
Arguments:
- tokens: bfloat16 [8192, 2560], P(('groups', 'ep')), parts along dimension 0, may hold values from -6 to 6
- device_choice: int32 [8192, 3], P(('groups', 'ep')), parts along dimension 0, may hold values from 0 to 31, as said below
- local_expert: int32 [8192, 6], P(('groups', 'ep')), parts along dimension 0, may hold values from 0 to 1, as said below
- route_weight: float32 [8192, 6], P(('groups', 'ep')), parts along dimension 0, may hold values from 0.1 to 1
- prefill_ranks: int32 [32], P('groups'), parts along dimension 0, may hold values from 0 to 31, as said below
- w_gate: bfloat16 [64, 1024, 2560], P('ep', 'tp'), may hold values from -0.125 to 0.125
- w_up: bfloat16 [64, 1024, 2560], P('ep', 'tp'), may hold values from -0.125 to 0.125
- w_down: bfloat16 [64, 1024, 2560], P('ep', 'tp'), may hold values from -0.1875 to 0.1875
Outputs:
- moe_out: bfloat16 [8192, 2560], P(('groups', 'ep', 'tp')), parts along dimension 0
The draws below stay inside these ranges and needn't reach their ends.
There are 2 independent parts, one for each index of `groups`. The reference program is written for one: setup_inputs(seed, part) draws one part's arguments, and reference() takes and returns one part's arrays. A program takes and returns all parts, laid end to end along the dimension named above; an argument that names none is the same for every part. Nothing has to cross between parts.
Inputs may be any that keep to these rules, and one draw needn't show every extreme that they name: `device_choice`: each row names 3 different ranks. The rows of one rank (aligned blocks of 128 rows) name any one rank at most 12 times, and every block names some rank exactly 12 times. `local_expert`: picks 2k and 2k + 1 of a row are two different experts of the rank in column k of device_choice. So the rows of one rank choose one expert at most 12 times, and some expert is chosen exactly 12 times by the rows of every rank. `prefill_ranks`: 16 different ranks.
All inputs are finite; a program needn't handle non-finite values.
Results may differ from the reference program's by a relative error of at most 0.014.
Values may be sent and summed in bfloat16 or wider, within the bound.
No kernel may reach another device: no remote copies, remote signals or barrier semaphores. Data moves between devices by JAX's collectives and lax.ppermute only.
A program may use at most 128 MiB of HBM per device.

```python
import math
import jax
import jax.numpy as jnp
from jax import lax

D = 2560
F = 1024
EXP_DEV = 2
TOPK = 6
DEV_TOP = 3
DEC_RANK = 8
EXPERTS = 64
RANK_ROWS = 128
PRE_RANKS = 16
ROWS = 4096
CAP = 12
N_EP = 32
N_TP = 8


def route_draw(key):
    base_key = jax.random.fold_in(key, 101)
    key_star, key_local, key_order, key_rows, key_first, key_second, key_swap = jax.random.split(base_key, 7)
    star_rank = jax.random.randint(key_star, (), 0, N_EP).astype(jnp.int32)
    star_local = jax.random.randint(key_local, (), 0, EXP_DEV).astype(jnp.int32)
    others = jax.vmap(lambda one_key: jax.random.permutation(one_key, N_EP - 1))(jax.random.split(key_order, N_EP))
    rank_order = jnp.concatenate([jnp.full((N_EP, 1), star_rank, jnp.int32), (star_rank + 1 + others.astype(jnp.int32)) % N_EP], axis=1)
    row_order = jax.vmap(lambda one_key: jax.random.permutation(one_key, RANK_ROWS))(jax.random.split(key_rows, N_EP))
    cycle_pos = (DEV_TOP * row_order.astype(jnp.int32)[:, :, None] + jnp.arange(DEV_TOP, dtype=jnp.int32)[None, None, :]) % N_EP
    chosen = jnp.take_along_axis(rank_order, cycle_pos.reshape(N_EP, RANK_ROWS * DEV_TOP), axis=1)
    chosen = chosen.reshape(N_EP * RANK_ROWS, DEV_TOP).astype(jnp.int32)
    pick_shape = (N_EP * RANK_ROWS, DEV_TOP)
    first_pick = jax.random.randint(key_first, pick_shape, 0, EXP_DEV).astype(jnp.int32)
    first_pick = jnp.where(chosen == star_rank, star_local, first_pick)
    second = (first_pick + 1 + jax.random.randint(key_second, pick_shape, 0, EXP_DEV - 1).astype(jnp.int32)) % EXP_DEV
    swap_bits = jax.random.randint(key_swap, pick_shape, 0, 2)
    pick_one = jnp.where(swap_bits == 1, second, first_pick)
    pick_two = jnp.where(swap_bits == 1, first_pick, second)
    local_picks = jnp.stack([pick_one, pick_two], axis=2).reshape(N_EP * RANK_ROWS, 2 * DEV_TOP)
    return (chosen, local_picks.astype(jnp.int32))


def draw_device_choice(key, part):
    chosen, local_picks = route_draw(key)
    return chosen


def draw_local_expert(key, part):
    chosen, local_picks = route_draw(key)
    return local_picks


def draw_prefill_ranks(key, part):
    shuffled = jax.random.permutation(jax.random.fold_in(key, 211), N_EP)
    return shuffled[:PRE_RANKS].astype(jnp.int32)


def block_scale(rng, shape, shards, low, top_value):
    def one(axis_at, parts):
        steps = jax.random.uniform(jax.random.fold_in(jax.random.fold_in(rng, 6), axis_at), (parts,), jnp.float32, low / len(shards), top_value / len(shards))
        return jnp.repeat(jnp.exp(steps), shape[axis_at] // parts).reshape((-1,) + (1,) * (len(shape) - axis_at - 1))

    gain = one(*shards[0])
    for cut in shards[1:]:
        gain = gain * one(*cut)
    return gain


def centred(rng, extent, scale, limit, cuts=(), kind=jnp.bfloat16):
    level = block_scale(rng, extent, cuts, -0.22, 0.18) if cuts else 1.0
    values = jax.random.normal(rng, extent, jnp.float32) * scale * level
    return jnp.minimum(jnp.maximum(values, -limit), limit).astype(kind)


def setup_inputs(seed: int = 0, part: int = 0) -> dict:
    streams_of = jax.random.split(jax.random.key(seed), 9)
    part_splits = jax.random.split(jax.random.fold_in(streams_of[8], part), 9)
    return {
        "tokens": centred(part_splits[0], (ROWS, D), 1.0, 6.0, ((0, 32),)),
        "device_choice": draw_device_choice(jax.random.fold_in(jax.random.fold_in(streams_of[8], part), 71), part),
        "local_expert": draw_local_expert(jax.random.fold_in(jax.random.fold_in(streams_of[8], part), 71), part),
        "route_weight": jnp.clip(jnp.exp(math.log(1.0) - 2.3025851 * jax.random.uniform(part_splits[3], (ROWS, TOPK), jnp.float32) ** block_scale(part_splits[3], (ROWS, TOPK), ((0, 32),), -0.2, 0.2)), 0.1, 1.0),
        "prefill_ranks": draw_prefill_ranks(jax.random.fold_in(jax.random.fold_in(streams_of[8], part), 71), part),
        "w_gate": centred(streams_of[5], (EXPERTS, F, D), D ** -0.5, 0.125, ((0, 32), (1, 8))),
        "w_up": centred(streams_of[6], (EXPERTS, F, D), D ** -0.5, 0.125, ((0, 32), (1, 8))),
        "w_down": centred(streams_of[7], (EXPERTS, F, D), F ** -0.5, 0.1875, ((0, 32), (1, 8))),
    }


def reference(tokens, device_choice, local_expert, route_weight, prefill_ranks, w_gate, w_up, w_down):
    row_count = tokens.shape[0]
    row_ids = jnp.arange(row_count, dtype=jnp.int32)
    rank_of = row_ids // RANK_ROWS
    in_prefill = jnp.any(rank_of[:, None] == prefill_ranks[None, :], axis=1)
    is_live = (row_ids % RANK_ROWS < DEC_RANK) | in_prefill
    expert_id = jnp.repeat(device_choice, 2, axis=1) * EXP_DEV + local_expert
    weights = jnp.where(is_live[:, None], route_weight, jnp.zeros_like(route_weight))
    most_rows = N_EP * CAP
    group_width = F // N_TP

    def per_expert(totals, expert):
        matches = (expert_id == expert) & is_live[:, None]
        picked = jnp.any(matches, axis=1)
        chosen_weight = jnp.sum(jnp.where(matches, weights, jnp.zeros_like(weights)), axis=1)
        row_index = jnp.nonzero(picked, size=most_rows, fill_value=row_count)[0].astype(jnp.int32)
        safe_index = jnp.minimum(row_index, row_count - 1).astype(jnp.int32)
        gathered = tokens[safe_index]
        gate_w = lax.dynamic_index_in_dim(w_gate, expert, 0, keepdims=False)
        up_w = lax.dynamic_index_in_dim(w_up, expert, 0, keepdims=False)
        down_w = lax.dynamic_index_in_dim(w_down, expert, 0, keepdims=False)
        gate_act = jnp.dot(gathered, gate_w.T, preferred_element_type=jnp.float32)
        up_act = jnp.dot(gathered, up_w.T, preferred_element_type=jnp.float32)
        hidden = (jax.nn.silu(gate_act) * up_act).astype(jnp.bfloat16)
        summed = jnp.zeros((most_rows, tokens.shape[1]), jnp.float32)
        for group in range(N_TP):
            low = group * group_width
            part_sum = jnp.dot(hidden[:, low:low + group_width], down_w[low:low + group_width], preferred_element_type=jnp.float32)
            summed = summed + part_sum.astype(jnp.bfloat16).astype(jnp.float32)
        weighted = chosen_weight[safe_index][:, None] * summed
        totals = totals.at[row_index].add(weighted, mode="drop")
        return totals, None

    zeros_init = jnp.zeros((row_count, tokens.shape[1]), jnp.float32)
    totals, unused = lax.scan(per_expert, zeros_init, jnp.arange(EXPERTS, dtype=jnp.int32))
    return totals.astype(jnp.bfloat16)
```

```python
import jax
import jax.numpy as jnp
from jax import lax
from jax.experimental import pallas as pl
from jax.experimental.pallas import tpu as pltpu
from jax.sharding import PartitionSpec as P

TOPK = 6
DEV_TOP = 3
DEC_RANK = 8
LANE = 128
F32, BF16, I32 = jnp.float32, jnp.bfloat16, jnp.int32
INTERPRET = False


class Plan:
    def __init__(self, ranks, lanes, rows, width, prefill):
        self.ranks, self.lanes, self.rows, self.width = ranks, lanes, rows, width
        self.cap = (DEV_TOP * rows + ranks - 1) // ranks
        self.prefill = prefill
        self.half_pre = self.cap // 2
        self.half_dec = DEC_RANK // 2
        self.half = prefill * self.half_pre + (ranks - prefill) * self.half_dec
        self.slots = 2 * self.half
        self.packed = 5 * self.half
        self.chunk = 2 * self.cap + self.half_pre + 2
        self.own_rows = rows // lanes
        assert width == (2 * lanes + lanes // 2) * LANE and self.chunk % 8 == 0
        assert 4 * ranks <= LANE or ranks * 3 <= LANE
        assert rows == LANE


def iota(shape, dim):
    return lax.broadcasted_iota(I32, shape, dim)


def one_hot(mask):
    return jnp.where(mask, 1.0, 0.0).astype(BF16)


def dot(a, b):
    return jnp.dot(a, b, preferred_element_type=F32)


def is_prefill(pre_ref, plan, own):
    found = pre_ref[0] == own
    for i in range(1, plan.prefill):
        found = found | (pre_ref[i] == own)
    return found


def earlier(plan):
    shape = (plan.rows, plan.rows)
    return one_hot(iota(shape, 0) < iota(shape, 1))


def chunk_index(j, plan, parity, half_slots):
    cap = plan.cap
    block = jnp.where(j < cap, 0, jnp.where(j < 2 * cap, 1, 2))
    slot = jnp.where(j < cap, j, jnp.where(j < 2 * cap, j - cap, j - 2 * cap + parity * half_slots))
    kept = (j < 2 * cap) | (j - 2 * cap < half_slots)
    return jnp.where(kept, block, 3), slot


def pack_kernel(plan, meta_ref, pre_ref, dc_ref, le_ref, rw_ref, tok_ref, tail_ref, out_ref):
    lane, own = meta_ref[0], meta_ref[1]
    full = is_prefill(pre_ref, plan, own)
    half_slots = jnp.where(full, plan.half_pre, plan.half_dec)
    rows, ranks = plan.rows, plan.ranks
    shape = (rows, LANE)
    limit = jnp.where(full, rows, DEC_RANK)
    live = iota(shape, 0) < limit
    col = iota(shape, 1)
    which, rank = col // ranks, col % ranks
    table = jnp.zeros(shape, F32)
    for k in range(DEV_TOP):
        hit = (dc_ref[:, k : k + 1] == rank) & live
        value = jnp.where(which == 0, 1.0, 0.0)
        for j in (2 * k, 2 * k + 1):
            value += jnp.where(le_ref[:, j : j + 1] == which - 1, rw_ref[:, j : j + 1], 0.0)
        table += jnp.where(hit, value, 0.0)
    turned = table.T
    named = turned[:ranks]
    before = dot(named.astype(BF16), earlier(plan))
    place = jnp.where(named > 0.5, before, -1.0).astype(I32)
    full_shape = (ranks, plan.chunk, LANE)
    j = iota(full_shape, 1)
    block, slot = chunk_index(j, plan, lane % 2, half_slots)
    match = place[:, None, :] == slot
    blocks = (tok_ref[:, :LANE], tok_ref[:, LANE:], tail_ref[...])
    total = jnp.zeros((ranks * plan.chunk, LANE), F32)
    for b in range(3):
        pick = one_hot(match & (block == b)).reshape(ranks * plan.chunk, LANE)
        total += dot(pick, blocks[b])
    total = total.reshape(full_shape)
    first = turned[ranks : 2 * ranks][:, None, :]
    second = turned[2 * ranks : 3 * ranks][:, None, :]
    total = jnp.where(j == plan.chunk - 2, first, jnp.where(j == plan.chunk - 1, second, total))
    out_ref[...] = total.astype(BF16)


def target_row(pre_ref, plan, shape, dim):
    c = iota(shape, dim)
    src, j = c // plan.chunk, c % plan.chunk
    hits = jnp.zeros(shape, I32)
    lower = jnp.zeros(shape, I32)
    for i in range(plan.prefill):
        hits += jnp.where(src == pre_ref[i], 1, 0)
        lower += jnp.where(src > pre_ref[i], 1, 0)
    full = hits > 0
    n = jnp.where(full, plan.half_pre, plan.half_dec)
    base = jnp.where(
        full, lower * plan.half_pre, plan.prefill * plan.half_pre + (src - lower) * plan.half_dec
    )
    b = jnp.where(j < plan.cap, 0, jnp.where(j < 2 * plan.cap, 1, 2))
    jj = j - b * plan.cap
    second = jnp.where((jj >= n) & (b < 2), 1, 0)
    kept = (jj - second * n) < n
    return jnp.where(kept, (2 * b + second) * plan.half + base + jj - second * n, -1)


def compact_kernel(plan, pre_ref, in_ref, out_ref, weight_ref):
    total = plan.ranks * plan.chunk
    target = target_row(pre_ref, plan, (1, total), 1)
    data = in_ref[...].reshape(total, LANE)
    ranks = plan.ranks
    pick_shape = (ranks, total)
    where_first = iota(pick_shape, 0) * plan.chunk + plan.chunk - 2
    col = iota(pick_shape, 1)
    first = dot(one_hot(col == where_first), data)
    second = dot(one_hot(col == where_first + 1), data)
    named = first > 0.0
    before = dot(one_hot(named), earlier(plan))
    place = jnp.where(named, before, -1.0).astype(I32)
    full_shape = (ranks, plan.chunk, LANE)
    j = iota(full_shape, 1)
    match = (place[:, None, :] == j) & (j < plan.cap)
    wide = []
    for value in (first, second):
        kept = jnp.where(match, value[:, None, :], 0.0)
        column = jnp.sum(kept, axis=2, keepdims=True)
        wide.append(jnp.broadcast_to(column, full_shape).reshape(total, LANE).astype(BF16))
    for piece in range(5):
        shape = (plan.half, total)
        take = one_hot(iota(shape, 0) + piece * plan.half == target)
        at = pl.ds(piece * plan.half, plan.half)
        out_ref[at, :] = dot(take, data).astype(BF16)
        if piece < 2:
            for e in range(2):
                weight_ref[at, e * LANE : (e + 1) * LANE] = dot(take, wide[e])


def expert_kernel(plan, offsets, meta_ref, *refs):
    n = len(offsets)
    parts = refs[:n]
    weight_ref, wg_ref, wu_ref, wd_ref, out_ref, x_ref = refs[n:]
    me = meta_ref[0]
    lanes, half, slots = plan.lanes, plan.half, plan.slots
    for offset, part in zip(offsets, parts):
        lane = lax.rem(me + offset + lanes, lanes)
        at = pl.multiple_of(lane * (2 * LANE), 2 * LANE)
        x_ref[:, pl.ds(at, LANE)] = part[0:slots, :]
        x_ref[:, pl.ds(pl.multiple_of(at + LANE, LANE), LANE)] = part[slots : 2 * slots, :]
        tail = pl.multiple_of((2 * lanes + lane // 2) * LANE, LANE)
        start = pl.multiple_of(lax.rem(lane, 2) * half, half)
        x_ref[pl.ds(start, half), pl.ds(tail, LANE)] = part[2 * slots : 2 * slots + half, :]
    x = x_ref[...]
    turned = (((1,), (1,)), ((), ()))
    gate = lax.dot_general(x, wg_ref[...], turned, preferred_element_type=F32)
    up = lax.dot_general(x, wu_ref[...], turned, preferred_element_type=F32)
    hidden = gate / (1.0 + jnp.exp(-gate)) * up * weight_ref[...]
    hidden = hidden.astype(BF16)
    for lane in range(lanes):
        at = lane * 2 * LANE
        y = dot(hidden, wd_ref[:, at : at + 2 * LANE]).astype(BF16)
        out_ref[lane, 0:slots, :] = y[:, :LANE]
        out_ref[lane, slots : 2 * slots, :] = y[:, LANE:]
    for pair in range(lanes // 2):
        at = (2 * lanes + pair) * LANE
        y = dot(hidden, wd_ref[:, at : at + LANE]).astype(BF16)
        out_ref[2 * pair, 2 * slots : 2 * slots + half, :] = y[:half]
        out_ref[2 * pair + 1, 2 * slots : 2 * slots + half, :] = y[half:]


def spread_kernel(plan, pre_ref, in_ref, out_ref):
    total = in_ref[0].astype(F32)
    for lane in range(1, plan.lanes):
        total += in_ref[lane].astype(F32)
    total = total.astype(BF16)
    chunk_rows = plan.ranks * plan.chunk
    target = target_row(pre_ref, plan, (chunk_rows, 1), 0)
    shape = (chunk_rows, plan.packed)
    take = one_hot(iota(shape, 1) == target)
    out_ref[...] = dot(take, total).astype(BF16).reshape(plan.ranks, plan.chunk, LANE)


def combine_kernel(plan, meta_ref, pre_ref, dc_ref, in_ref, out_ref):
    lane, own = meta_ref[0], meta_ref[1]
    full = is_prefill(pre_ref, plan, own)
    half_slots = jnp.where(full, plan.half_pre, plan.half_dec)
    rows, ranks = plan.rows, plan.ranks
    shape = (rows, ranks)
    live = iota(shape, 0) < jnp.where(full, rows, DEC_RANK)
    rank = iota(shape, 1)
    named = jnp.zeros(shape, F32)
    for k in range(DEV_TOP):
        named += jnp.where((dc_ref[:, k : k + 1] == rank) & live, 1.0, 0.0)
    square = (rows, rows)
    before = dot(one_hot(iota(square, 1) < iota(square, 0)), named.astype(BF16))
    place = jnp.where(named > 0.5, before, -1.0).astype(BF16)
    total = ranks * plan.chunk
    spread = (ranks, total)
    wide = dot(place, one_hot(iota(spread, 1) // plan.chunk == iota(spread, 0))).astype(I32)
    j = iota((1, total), 1) % plan.chunk
    block, slot = chunk_index(j, plan, lane % 2, half_slots)
    data = in_ref[...].reshape(total, LANE)
    own_rows = plan.own_rows
    match = wide == slot
    for b in range(3):
        mine = dot(one_hot(match & (block == b)), data).astype(BF16)
        for to in range(plan.lanes):
            out_ref[to, b * own_rows : (b + 1) * own_rows, :] = mine[
                to * own_rows : (to + 1) * own_rows
            ]


def finish_kernel(plan, in_ref, out_ref):
    n = plan.own_rows
    for lane in range(plan.lanes):
        at = lane * 2 * LANE
        out_ref[:, at : at + LANE] = in_ref[lane, 0:n, :]
        out_ref[:, at + LANE : at + 2 * LANE] = in_ref[lane, n : 2 * n, :]
    for pair in range(plan.lanes // 2):
        at = (2 * plan.lanes + pair) * LANE
        first = in_ref[2 * pair, 2 * n : 3 * n, :].astype(F32)
        second = in_ref[2 * pair + 1, 2 * n : 3 * n, :].astype(F32)
        out_ref[:, at : at + LANE] = (first + second).astype(BF16)


SMEM = pl.BlockSpec(memory_space=pltpu.SMEM)
VMEM = pl.BlockSpec(memory_space=pltpu.VMEM)


def call(kernel, name, out, specs, *args, scratch=(), limit=24 << 20, **kw):
    return pl.pallas_call(
        kernel,
        out_shape=out,
        in_specs=specs,
        out_specs=jax.tree.map(lambda _: VMEM, out),
        scratch_shapes=scratch,
        compiler_params=pltpu.CompilerParams(vmem_limit_bytes=limit),
        interpret=INTERPRET,
        name=name,
        **kw,
    )(*args)


def pack(plan, meta, prefill_ranks, device_choice, local_expert, route_weight, tokens):
    def whole(i, meta, pre):
        return (0, 0)

    rows = plan.rows
    grid_spec = pltpu.PrefetchScalarGridSpec(
        num_scalar_prefetch=2,
        grid=(1,),
        in_specs=[
            pl.BlockSpec((rows, DEV_TOP), whole),
            pl.BlockSpec((rows, TOPK), whole),
            pl.BlockSpec((rows, TOPK), whole),
            pl.BlockSpec((rows, 2 * LANE), lambda i, meta, pre: (0, meta[0])),
            pl.BlockSpec(
                (rows, LANE), lambda i, meta, pre: (0, 2 * plan.lanes + meta[0] // 2)
            ),
        ],
        out_specs=pl.BlockSpec((plan.ranks, plan.chunk, LANE), lambda i, meta, pre: (0, 0, 0)),
    )
    return pl.pallas_call(
        lambda *refs: pack_kernel(plan, *refs),
        grid_spec=grid_spec,
        out_shape=jax.ShapeDtypeStruct((plan.ranks, plan.chunk, LANE), BF16),
        compiler_params=pltpu.CompilerParams(vmem_limit_bytes=24 << 20),
        interpret=INTERPRET,
        name="pack",
    )(meta, prefill_ranks, device_choice, local_expert, route_weight, tokens, tokens)


def compact(plan, prefill_ranks, received):
    return call(
        lambda *refs: compact_kernel(plan, *refs),
        "compact",
        (
            jax.ShapeDtypeStruct((plan.packed, LANE), BF16),
            jax.ShapeDtypeStruct((plan.slots, 2 * LANE), F32),
        ),
        [SMEM, VMEM],
        prefill_ranks,
        received,
    )


def experts(plan, offsets, meta, parts, weights, w_gate, w_up, w_down):
    hidden = w_gate.shape[0] * w_gate.shape[1]
    flat = [w.reshape(hidden, plan.width) for w in (w_gate, w_up, w_down)]
    return call(
        lambda *refs: expert_kernel(plan, offsets, *refs),
        "experts",
        jax.ShapeDtypeStruct((plan.lanes, plan.packed, LANE), BF16),
        [SMEM] + [VMEM] * (len(parts) + 4),
        meta,
        *parts,
        weights,
        *flat,
        scratch=[pltpu.VMEM((plan.slots, plan.width), BF16)],
        limit=32 << 20,
    )


def spread(plan, prefill_ranks, returned):
    return call(
        lambda *refs: spread_kernel(plan, *refs),
        "spread",
        jax.ShapeDtypeStruct((plan.ranks, plan.chunk, LANE), BF16),
        [SMEM, VMEM],
        prefill_ranks,
        returned,
    )


def combine(plan, meta, prefill_ranks, device_choice, back):
    return call(
        lambda *refs: combine_kernel(plan, *refs),
        "combine",
        jax.ShapeDtypeStruct((plan.lanes, 3 * plan.own_rows, LANE), BF16),
        [SMEM, SMEM, VMEM, VMEM],
        meta,
        prefill_ranks,
        device_choice,
        back,
    )


def finish(plan, shares):
    return call(
        lambda *refs: finish_kernel(plan, *refs),
        "finish",
        jax.ShapeDtypeStruct((plan.own_rows, plan.width), BF16),
        [VMEM],
        shares,
    )


def gather_ring(packed, lanes):
    right = [(i, (i + 1) % lanes) for i in range(lanes)]
    left = [(i, (i - 1) % lanes) for i in range(lanes)]
    parts, offsets = [packed], [0]
    from_left = from_right = packed
    for hop in range(1, lanes // 2 + 1):
        from_left = lax.ppermute(from_left, "tp", right)
        parts.append(from_left)
        offsets.append(-hop)
        if hop < lanes // 2:
            from_right = lax.ppermute(from_right, "tp", left)
            parts.append(from_right)
            offsets.append(hop)
    return parts, offsets


def on_device(
    tokens, device_choice, local_expert, route_weight, prefill_ranks, w_gate, w_up, w_down
):
    plan = Plan(
        lax.axis_size("ep"),
        lax.axis_size("tp"),
        tokens.shape[0],
        tokens.shape[1],
        prefill_ranks.shape[0],
    )
    meta = jnp.stack([lax.axis_index("tp"), lax.axis_index("ep")]).astype(I32)
    outgoing = pack(
        plan, meta, prefill_ranks, device_choice, local_expert, route_weight, tokens
    )
    received = lax.all_to_all(outgoing, "ep", 0, 0, tiled=True)
    packed, weights = compact(plan, prefill_ranks, received)
    parts, offsets = gather_ring(packed, plan.lanes)
    partial = experts(plan, offsets, meta, parts, weights, w_gate, w_up, w_down)
    returned = lax.all_to_all(partial, "tp", 0, 0, tiled=True)
    back = spread(plan, prefill_ranks, returned)
    back = lax.all_to_all(back, "ep", 0, 0, tiled=True)
    shares = combine(plan, meta, prefill_ranks, device_choice, back)
    shares = lax.all_to_all(shares, "tp", 0, 0, tiled=True)
    return finish(plan, shares)


def solution(mesh):
    in_specs = (
        P(("groups", "ep"), None),
        P(("groups", "ep"), None),
        P(("groups", "ep"), None),
        P(("groups", "ep"), None),
        P("groups"),
        P("ep", "tp", None),
        P("ep", "tp", None),
        P("ep", "tp", None),
    )
    out_specs = P(("groups", "ep", "tp"), None)
    return jax.shard_map(
        on_device, mesh=mesh, in_specs=in_specs, out_specs=out_specs, check_vma=False
    )
```

```python
import jax
import jax.numpy as jnp
from jax import lax
from jax.experimental import pallas as pl
from jax.experimental.pallas import tpu as pltpu
from jax.sharding import PartitionSpec as P

TOPK = 6
DEV_TOP = 3
DEC_RANK = 8
LANE = 128
F32, BF16, I32 = jnp.float32, jnp.bfloat16, jnp.int32
INTERPRET = False


class Plan:
    def __init__(self, ranks, lanes, rows, width, prefill):
        self.ranks, self.lanes, self.rows, self.width = ranks, lanes, rows, width
        self.cap = (DEV_TOP * rows + ranks - 1) // ranks
        self.prefill = prefill
        self.half_pre = self.cap // 2
        self.half_dec = DEC_RANK // 2
        self.half = prefill * self.half_pre + (ranks - prefill) * self.half_dec
        self.slots = 2 * self.half
        self.packed = 5 * self.half
        self.packed_up = -(-self.packed // LANE) * LANE
        self.side = self.packed // 2
        self.step = next(n for n in range(200, 0, -8) if self.side % n == 0)
        self.chunk = 2 * self.cap + self.half_pre + 2
        self.own_rows = rows // lanes
        assert width == (2 * lanes + lanes // 2) * LANE and self.chunk % 8 == 0
        assert 4 * ranks <= LANE or ranks * 3 <= LANE
        assert rows == LANE


def iota(shape, dim):
    return lax.broadcasted_iota(I32, shape, dim)


def one_hot(mask):
    return jnp.where(mask, 1.0, 0.0).astype(BF16)


def dot(a, b):
    return jnp.dot(a, b, preferred_element_type=F32)


def is_prefill(pre_ref, plan, own):
    found = pre_ref[0] == own
    for i in range(1, plan.prefill):
        found = found | (pre_ref[i] == own)
    return found


def earlier(plan):
    shape = (plan.rows, plan.rows)
    return one_hot(iota(shape, 0) < iota(shape, 1))


def chunk_index(j, plan, parity, half_slots):
    cap = plan.cap
    block = jnp.where(j < cap, 0, jnp.where(j < 2 * cap, 1, 2))
    slot = jnp.where(j < cap, j, jnp.where(j < 2 * cap, j - cap, j - 2 * cap + parity * half_slots))
    kept = (j < 2 * cap) | (j - 2 * cap < half_slots)
    return jnp.where(kept, block, 3), slot


def named_ranks(plan, full, dc_ref):
    shape = (plan.ranks, plan.rows)
    live = iota(shape, 1) < jnp.where(full, plan.rows, DEC_RANK)
    rank = iota(shape, 0)
    hits = [(dc_ref[k : k + 1, :] == rank) & live for k in range(DEV_TOP)]
    named = sum(jnp.where(hit, 1.0, 0.0) for hit in hits)
    return hits, named, places(plan, named)


def places(plan, named):
    before = dot(named.astype(BF16), earlier(plan))
    return jnp.where(named > 0.5, before, -1.0)


def pack_kernel(plan, meta_ref, pre_ref, dc_ref, le_ref, rw_ref, tok_ref, out_ref, x_ref, sems):
    lane, own = meta_ref[0], meta_ref[1]
    first_at = pl.multiple_of(lane * (2 * LANE), LANE)
    tail_at = pl.multiple_of((2 * plan.lanes + lane // 2) * LANE, LANE)
    copies = [
        pltpu.make_async_copy(
            tok_ref.at[:, pl.ds(first_at, 2 * LANE)], x_ref.at[:, 0 : 2 * LANE], sems.at[0]
        ),
        pltpu.make_async_copy(
            tok_ref.at[:, pl.ds(tail_at, LANE)], x_ref.at[:, 2 * LANE : 3 * LANE], sems.at[1]
        ),
    ]
    for copy in copies:
        copy.start()
    full = is_prefill(pre_ref, plan, own)
    half_slots = jnp.where(full, plan.half_pre, plan.half_dec)
    hits, named, place = named_ranks(plan, full, dc_ref)
    weights = []
    for e in range(2):
        total = jnp.zeros(named.shape, F32)
        for k, hit in enumerate(hits):
            for j in (2 * k, 2 * k + 1):
                chosen = hit & (le_ref[j : j + 1, :] == e)
                total += jnp.where(chosen, rw_ref[j : j + 1, :], 0.0)
        weights.append(total)
    full_shape = (plan.ranks, plan.chunk, LANE)
    flat = plan.ranks * plan.chunk
    j = iota(full_shape, 1)
    block, slot = chunk_index(j, plan, lane % 2, half_slots)
    match = place.astype(I32)[:, None, :] == slot
    picks = [one_hot(match & (block == b)).reshape(flat, LANE) for b in range(3)]
    for copy in copies:
        copy.wait()
    total = sum(dot(picks[b], x_ref[:, b * LANE : (b + 1) * LANE]) for b in range(3))
    total = total.reshape(full_shape)
    total = jnp.where(j == plan.chunk - 2, weights[0][:, None, :], total)
    total = jnp.where(j == plan.chunk - 1, weights[1][:, None, :], total)
    out_ref[...] = total.astype(BF16)


def target_row(pre_ref, plan, shape, dim):
    c = iota(shape, dim)
    src, j = c // plan.chunk, c % plan.chunk
    hits = jnp.zeros(shape, I32)
    lower = jnp.zeros(shape, I32)
    for i in range(plan.prefill):
        hits += jnp.where(src == pre_ref[i], 1, 0)
        lower += jnp.where(src > pre_ref[i], 1, 0)
    full = hits > 0
    n = jnp.where(full, plan.half_pre, plan.half_dec)
    base = jnp.where(
        full, lower * plan.half_pre, plan.prefill * plan.half_pre + (src - lower) * plan.half_dec
    )
    b = jnp.where(j < plan.cap, 0, jnp.where(j < 2 * plan.cap, 1, 2))
    jj = j - b * plan.cap
    second = jnp.where((jj >= n) & (b < 2), 1, 0)
    kept = (jj - second * n) < n
    return jnp.where(kept, (2 * b + second) * plan.half + base + jj - second * n, -1)


def compact_kernel(plan, pre_ref, in_ref, a_ref, b_ref):
    total = plan.ranks * plan.chunk
    target = target_row(pre_ref, plan, (1, total), 1)
    data = in_ref[...].reshape(total, LANE)
    side = plan.side
    for ref, begin in ((a_ref, 0), (b_ref, side)):
        for at in range(0, side, plan.step):
            shape = (plan.step, total)
            take = one_hot(iota(shape, 0) + (begin + at) == target)
            ref[at : at + plan.step, :] = dot(take, data).astype(BF16)


def tables_kernel(plan, meta_ref, pre_ref, dc_ref, in_ref, weight_ref, spread_ref, combine_ref):
    lane, own = meta_ref[0], meta_ref[1]
    ranks, rows = plan.ranks, plan.rows
    total = ranks * plan.chunk
    data = in_ref[...].reshape(total, LANE)
    target = target_row(pre_ref, plan, (1, total), 1)
    pick_shape = (ranks, total)
    where_first = iota(pick_shape, 0) * plan.chunk + plan.chunk - 2
    col = iota(pick_shape, 1)
    first = dot(one_hot(col == where_first), data)
    second = dot(one_hot(col == where_first + 1), data)
    place = places(plan, jnp.where(first > 0.0, 1.0, 0.0)).astype(I32)
    full_shape = (ranks, plan.chunk, LANE)
    j = iota(full_shape, 1)
    match = (place[:, None, :] == j) & (j < plan.cap)
    wide = []
    for value in (first, second):
        kept = jnp.where(match, value[:, None, :], 0.0)
        column = jnp.sum(kept, axis=2, keepdims=True)
        wide.append(jnp.broadcast_to(column, full_shape).reshape(total, LANE).astype(BF16))
    for piece in range(2):
        shape = (plan.half, total)
        take = one_hot(iota(shape, 0) + piece * plan.half == target)
        for e in range(2):
            at = piece * plan.half
            weight_ref[at : at + plan.half, e * LANE : (e + 1) * LANE] = dot(take, wide[e])
    column = target_row(pre_ref, plan, (total, LANE), 0)
    for at in range(0, plan.packed_up, LANE):
        spread_ref[:, at : at + LANE] = one_hot(iota((total, LANE), 1) + at == column)
    full = is_prefill(pre_ref, plan, own)
    half_slots = jnp.where(full, plan.half_pre, plan.half_dec)
    _, _, place = named_ranks(plan, full, dc_ref)
    square = jnp.concatenate([place, jnp.zeros((rows - ranks, rows), F32)], axis=0)
    turned = square.T[:, :ranks].astype(BF16)
    expand = one_hot(col // plan.chunk == iota(pick_shape, 0))
    spots = dot(turned, expand).astype(I32)
    j = iota((1, total), 1) % plan.chunk
    block, slot = chunk_index(j, plan, lane % 2, half_slots)
    match = spots == slot
    for b in range(3):
        combine_ref[:, b * total : (b + 1) * total] = one_hot(match & (block == b))


def lane_at(plan, me, sign, steps):
    return lax.rem(me + sign * steps + plan.lanes, plan.lanes)


def expert_kernel(plan, meta_ref, *refs):
    n = len(GATHERED)
    a_refs, b_refs = refs[:n], refs[n : 2 * n]
    weight_ref, wg_ref, wu_ref, wd_ref = refs[2 * n : 2 * n + 4]
    outs = refs[2 * n + 4 : -6]
    x_ref, h_ref, wg, wu, wd, sems = refs[-6:]
    loads = [
        pltpu.make_async_copy(src, dst, sems.at[i])
        for i, (src, dst) in enumerate(((wg_ref, wg), (wu_ref, wu), (wd_ref, wd)))
    ]
    for load in loads:
        load.start()
    me = meta_ref[0]
    sign = 1 - 2 * lax.rem(me, 2)
    lanes, half, slots, side = plan.lanes, plan.half, plan.slots, plan.side
    over = side - slots

    def columns(lane):
        first = pl.multiple_of(lane * (2 * LANE), LANE)
        tail = pl.multiple_of((2 * lanes + lane // 2) * LANE, LANE)
        start = pl.multiple_of(lax.rem(lane, 2) * half, 8)
        return (
            pl.ds(first, LANE),
            pl.ds(pl.multiple_of(first + LANE, LANE), LANE),
            pl.ds(tail, LANE),
            pl.ds(start, half),
        )

    for refs_of, turn in ((a_refs, sign), (b_refs, -sign)):
        for ref, steps in zip(refs_of, GATHERED):
            for i, step in enumerate(steps):
                first, second, tail, rows = columns(lane_at(plan, me, turn, step))
                at = i * side
                if refs_of is a_refs:
                    x_ref[:, first] = ref[at : at + slots, :]
                    x_ref[0:over, second] = ref[at + slots : at + side, :]
                else:
                    x_ref[over:slots, second] = ref[at : at + slots - over, :]
                    x_ref[rows, tail] = ref[at + slots - over : at + side, :]
    turned = (((1,), (1,)), ((), ()))
    x = x_ref[...]
    loads[0].wait()
    gate = lax.dot_general(x, wg[...], turned, preferred_element_type=F32)
    loads[1].wait()
    up = lax.dot_general(x, wu[...], turned, preferred_element_type=F32)
    hidden = gate / (1.0 + jnp.exp(-gate)) * up * weight_ref[...]
    h_ref[...] = hidden.astype(BF16)
    loads[2].wait()
    out = 0
    for steps in SCATTERED:
        for turn in (sign, -sign):
            for i, step in enumerate(steps):
                first, second, tail, rows = columns(lane_at(plan, me, turn, step))
                ref, at = outs[out], i * side
                if turn is sign:
                    ref[at : at + slots, :] = dot(h_ref[...], wd[:, first]).astype(BF16)
                    ref[at + slots : at + side, :] = dot(h_ref[0:over, :], wd[:, second]).astype(BF16)
                else:
                    ref[at : at + slots - over, :] = dot(h_ref[over:slots, :], wd[:, second]).astype(BF16)
                    ref[at + slots - over : at + side, :] = dot(h_ref[rows, :], wd[:, tail]).astype(BF16)
            out += 1


def spread_kernel(plan, take_ref, own_a, got_a, own_b, got_b, out_ref, sum_ref):
    side = plan.side
    sum_ref[0:side, :] = (own_a[...].astype(F32) + got_a[...].astype(F32)).astype(BF16)
    sum_ref[side : 2 * side, :] = (own_b[...].astype(F32) + got_b[...].astype(F32)).astype(BF16)
    sum_ref[2 * side :, :] = jnp.zeros((plan.packed_up - 2 * side, LANE), BF16)
    spread = dot(take_ref[...], sum_ref[...]).astype(BF16)
    out_ref[...] = spread.reshape(plan.ranks, plan.chunk, LANE)


def combine_kernel(plan, take_ref, in_ref, out_ref):
    total = plan.ranks * plan.chunk
    data = in_ref[...].reshape(total, LANE)
    own_rows = plan.own_rows
    for b in range(3):
        mine = dot(take_ref[:, b * total : (b + 1) * total], data).astype(BF16)
        for to in range(plan.lanes):
            out_ref[to, b * own_rows : (b + 1) * own_rows, :] = mine[
                to * own_rows : (to + 1) * own_rows
            ]


def finish_kernel(plan, in_ref, out_ref):
    n = plan.own_rows
    for lane in range(plan.lanes):
        at = lane * 2 * LANE
        out_ref[:, at : at + LANE] = in_ref[lane, 0:n, :]
        out_ref[:, at + LANE : at + 2 * LANE] = in_ref[lane, n : 2 * n, :]
    for pair in range(plan.lanes // 2):
        at = (2 * plan.lanes + pair) * LANE
        first = in_ref[2 * pair, 2 * n : 3 * n, :].astype(F32)
        second = in_ref[2 * pair + 1, 2 * n : 3 * n, :].astype(F32)
        out_ref[:, at : at + LANE] = (first + second).astype(BF16)


SMEM = pl.BlockSpec(memory_space=pltpu.SMEM)
VMEM = pl.BlockSpec(memory_space=pltpu.VMEM)
HBM = pl.BlockSpec(memory_space=pltpu.HBM)
GATHERED = ((0,), (1,), (-1, -2), (2, 3), (-3, -4))
SCATTERED = ((-3, -4), (2, 3), (-1, -2), (0,), (1,))


def call(kernel, name, out, specs, *args, scratch=(), limit=24 << 20, flops=0):
    cost = None
    if flops:
        cost = pl.CostEstimate(flops=flops, bytes_accessed=1 << 20, transcendentals=0)
    return pl.pallas_call(
        kernel,
        out_shape=out,
        in_specs=specs,
        out_specs=jax.tree.map(lambda _: VMEM, out),
        scratch_shapes=scratch,
        compiler_params=pltpu.CompilerParams(vmem_limit_bytes=limit),
        cost_estimate=cost,
        interpret=INTERPRET,
        name=name,
    )(*args)


def pack(plan, meta, prefill_ranks, choice, local_expert, route_weight, tokens):
    return call(
        lambda *refs: pack_kernel(plan, *refs),
        "pack",
        jax.ShapeDtypeStruct((plan.ranks, plan.chunk, LANE), BF16),
        [SMEM, SMEM, VMEM, VMEM, VMEM, HBM],
        meta,
        prefill_ranks,
        choice,
        local_expert,
        route_weight,
        tokens,
        scratch=[pltpu.VMEM((plan.rows, 3 * LANE), BF16), pltpu.SemaphoreType.DMA((2,))],
    )


def compact(plan, prefill_ranks, received):
    share = jax.ShapeDtypeStruct((plan.side, LANE), BF16)
    return call(
        lambda *refs: compact_kernel(plan, *refs),
        "compact",
        (share, share),
        [SMEM, VMEM],
        prefill_ranks,
        received,
    )


def tables(plan, meta, prefill_ranks, choice, received):
    total = plan.ranks * plan.chunk
    return call(
        lambda *refs: tables_kernel(plan, *refs),
        "tables",
        (
            jax.ShapeDtypeStruct((plan.slots, 2 * LANE), F32),
            jax.ShapeDtypeStruct((total, plan.packed_up), BF16),
            jax.ShapeDtypeStruct((plan.rows, 3 * total), BF16),
        ),
        [SMEM, SMEM, VMEM, VMEM],
        meta,
        prefill_ranks,
        choice,
        received,
        flops=1 << 30,
    )


def experts(plan, meta, a_parts, b_parts, weights, w_gate, w_up, w_down):
    hidden = w_gate.shape[0] * w_gate.shape[1]
    flat = [w.reshape(hidden, plan.width) for w in (w_gate, w_up, w_down)]
    out = []
    for steps in SCATTERED:
        out += [jax.ShapeDtypeStruct((len(steps) * plan.side, LANE), BF16)] * 2
    weight = pltpu.VMEM((hidden, plan.width), BF16)
    outs = call(
        lambda *refs: expert_kernel(plan, *refs),
        "experts",
        tuple(out),
        [SMEM] + [VMEM] * (2 * len(a_parts) + 1) + [HBM] * 3,
        meta,
        *a_parts,
        *b_parts,
        weights,
        *flat,
        scratch=[
            pltpu.VMEM((plan.slots, plan.width), BF16),
            pltpu.VMEM((plan.slots, hidden), BF16),
            weight,
            weight,
            weight,
            pltpu.SemaphoreType.DMA((3,)),
        ],
        limit=32 << 20,
    )
    return outs[0::2], outs[1::2]


def spread(plan, take, own_a, got_a, own_b, got_b):
    return call(
        lambda *refs: spread_kernel(plan, *refs),
        "spread",
        jax.ShapeDtypeStruct((plan.ranks, plan.chunk, LANE), BF16),
        [VMEM] * 5,
        take,
        own_a,
        got_a,
        own_b,
        got_b,
        scratch=[pltpu.VMEM((plan.packed_up, LANE), BF16)],
    )


def combine(plan, take, back):
    return call(
        lambda *refs: combine_kernel(plan, *refs),
        "combine",
        jax.ShapeDtypeStruct((plan.lanes, 3 * plan.own_rows, LANE), BF16),
        [VMEM, VMEM],
        take,
        back,
    )


def finish(plan, shares):
    return call(
        lambda *refs: finish_kernel(plan, *refs),
        "finish",
        jax.ShapeDtypeStruct((plan.own_rows, plan.width), BF16),
        [VMEM],
        shares,
    )


def neighbours(lanes):
    near = [(i, i ^ 1) for i in range(lanes)]
    far = [(i, (i - 1 + 2 * (i % 2)) % lanes) for i in range(lanes)]
    return near, far


def swap(arrays, pairs):
    return [lax.ppermute(x, "tp", p) for x, p in zip(arrays, pairs)]


def gather_lanes(shares, lanes):
    near, far = neighbours(lanes)
    own = list(shares)
    first = swap(own, (near, far))
    held = [jnp.concatenate([x, y]) for x, y in zip(own, first)]
    parts = [own, first]
    for hop in range(lanes // 2 - 1):
        held = swap(held, (far, near) if hop % 2 == 0 else (near, far))
        parts.append(held)
    return [p[0] for p in parts], [p[1] for p in parts]


def plus(x, y):
    return (x.astype(F32) + y.astype(F32)).astype(BF16)


def reduce_lanes(a_outs, b_outs, side, lanes):
    near, far = neighbours(lanes)
    stages = list(zip(a_outs, b_outs))
    held = list(stages[0])
    for hop in range(lanes // 2 - 2):
        got = swap(held, (far, near) if hop % 2 == 0 else (near, far))
        held = [plus(x, y) for x, y in zip(stages[hop + 1], got)]
    got = swap(held, (far, near))
    away = [plus(x, y[side:]) for x, y in zip(stages[-1], got)]
    home = [plus(x, y[:side]) for x, y in zip(stages[-2], got)]
    last = swap(away, (near, far))
    return home[0], last[0], home[1], last[1]


def on_device(
    tokens, device_choice, local_expert, route_weight, prefill_ranks, w_gate, w_up, w_down
):
    plan = Plan(
        lax.axis_size("ep"),
        lax.axis_size("tp"),
        tokens.shape[0],
        tokens.shape[1],
        prefill_ranks.shape[0],
    )
    meta = jnp.stack([lax.axis_index("tp"), lax.axis_index("ep")]).astype(I32)
    choice = device_choice.T
    outgoing = pack(
        plan, meta, prefill_ranks, choice, local_expert.T, route_weight.T, tokens
    )
    received = lax.all_to_all(outgoing, "ep", 0, 0, tiled=True)
    shares = compact(plan, prefill_ranks, received)
    weights, take_out, take_in = tables(plan, meta, prefill_ranks, choice, received)
    a_parts, b_parts = gather_lanes(shares, plan.lanes)
    a_outs, b_outs = experts(plan, meta, a_parts, b_parts, weights, w_gate, w_up, w_down)
    sums = reduce_lanes(a_outs, b_outs, plan.side, plan.lanes)
    back = lax.all_to_all(spread(plan, take_out, *sums), "ep", 0, 0, tiled=True)
    shares = lax.all_to_all(combine(plan, take_in, back), "tp", 0, 0, tiled=True)
    return finish(plan, shares)


def solution(mesh):
    in_specs = (
        P(("groups", "ep"), None),
        P(("groups", "ep"), None),
        P(("groups", "ep"), None),
        P(("groups", "ep"), None),
        P("groups"),
        P("ep", "tp", None),
        P("ep", "tp", None),
        P("ep", "tp", None),
    )
    out_specs = P(("groups", "ep", "tp"), None)
    return jax.shard_map(
        on_device, mesh=mesh, in_specs=in_specs, out_specs=out_specs, check_vma=False
    )
```

```python
import jax
import jax.numpy as jnp
from jax import lax
from jax.experimental import pallas as pl
from jax.experimental.pallas import tpu as pltpu
from jax.sharding import PartitionSpec as P

TOPK = 6
DEV_TOP = 3
DEC_RANK = 8
USUAL_DECODE = 32
LANE = 128
F32, BF16, I32 = jnp.float32, jnp.bfloat16, jnp.int32
INTERPRET = False


class Plan:
    def __init__(self, ranks, lanes, rows, width, prefill, decode):
        self.ranks, self.lanes, self.rows, self.width = ranks, lanes, rows, width
        self.cap = (DEV_TOP * rows + ranks - 1) // ranks
        self.prefill, self.decode = prefill, decode
        self.half_pre = self.cap // 2
        self.half_dec = DEC_RANK // 2
        self.half = prefill * self.half_pre + decode // 2
        self.slots = 2 * self.half
        self.packed = 5 * self.half
        self.packed_up = -(-self.packed // LANE) * LANE
        self.side = self.packed // 2
        self.step = next(n for n in range(200, 0, -8) if self.side % n == 0)
        self.chunk = 2 * self.cap + self.half_pre + 2
        self.own_rows = rows // lanes
        assert width == (2 * lanes + lanes // 2) * LANE and self.chunk % 8 == 0
        assert rows == LANE and self.half_dec <= self.cap - DEC_RANK and ranks <= LANE


def iota(shape, dim):
    return lax.broadcasted_iota(I32, shape, dim)


def one_hot(mask):
    return jnp.where(mask, 1.0, 0.0).astype(BF16)


def dot(a, b):
    return jnp.dot(a, b, preferred_element_type=F32)


def is_prefill(info_ref, plan, own):
    found = info_ref[2] == own
    for i in range(1, plan.prefill):
        found = found | (info_ref[2 + i] == own)
    return found


def earlier(plan):
    shape = (plan.rows, plan.rows)
    return one_hot(iota(shape, 0) < iota(shape, 1))


def chunk_index(j, plan, parity, full):
    cap = plan.cap
    spill = (j >= DEC_RANK) & (j < cap) & jnp.logical_not(full)
    last = j >= 2 * cap
    block = jnp.where(last | spill, 2, jnp.where(j < cap, 0, 1))
    start = jnp.where(full, parity * plan.half_pre, 0)
    slot = jnp.where(
        spill, j - DEC_RANK + plan.half_dec, jnp.where(last, j - 2 * cap + start, j - block * cap)
    )
    kept = jnp.logical_not(last) | (j - 2 * cap < jnp.where(full, plan.half_pre, plan.half_dec))
    return jnp.where(kept, block, 3), slot


def named_ranks(plan, full, routes_ref):
    shape = (plan.ranks, plan.rows)
    live = iota(shape, 1) < jnp.where(full, plan.rows, DEC_RANK)
    rank = iota(shape, 0)
    hits = [(routes_ref[k : k + 1, :].astype(I32) == rank) & live for k in range(DEV_TOP)]
    named = sum(jnp.where(hit, 1.0, 0.0) for hit in hits)
    return hits, named, places(plan, named)


def places(plan, named):
    before = dot(named.astype(BF16), earlier(plan))
    return jnp.where(named > 0.5, before, -1.0)


def pack_kernel(plan, info_ref, routes_ref, tok_ref, out_ref, x_ref, sems):
    lane, own = info_ref[0], info_ref[1]
    first_at = pl.multiple_of(lane * (2 * LANE), LANE)
    tail_at = pl.multiple_of((2 * plan.lanes + lane // 2) * LANE, LANE)
    copies = [
        pltpu.make_async_copy(
            tok_ref.at[:, pl.ds(first_at, 2 * LANE)], x_ref.at[:, 0 : 2 * LANE], sems.at[0]
        ),
        pltpu.make_async_copy(
            tok_ref.at[:, pl.ds(tail_at, LANE)], x_ref.at[:, 2 * LANE : 3 * LANE], sems.at[1]
        ),
    ]
    for copy in copies:
        copy.start()
    full = is_prefill(info_ref, plan, own)
    hits, named, place = named_ranks(plan, full, routes_ref)
    weights = []
    for e in range(2):
        total = jnp.zeros(named.shape, F32)
        for k, hit in enumerate(hits):
            for j in (2 * k, 2 * k + 1):
                at = DEV_TOP + j
                chosen = hit & (routes_ref[at : at + 1, :] == float(e))
                at += TOPK
                total += jnp.where(chosen, routes_ref[at : at + 1, :], 0.0)
        weights.append(total)
    full_shape = (plan.ranks, plan.chunk, LANE)
    flat = plan.ranks * plan.chunk
    j = iota(full_shape, 1)
    block, slot = chunk_index(j, plan, lane % 2, full)
    match = place.astype(I32)[:, None, :] == slot
    picks = [one_hot(match & (block == b)).reshape(flat, LANE) for b in range(3)]
    for copy in copies:
        copy.wait()
    total = sum(dot(picks[b], x_ref[:, b * LANE : (b + 1) * LANE]) for b in range(3))
    total = total.reshape(full_shape)
    total = jnp.where(j == plan.chunk - 2, weights[0][:, None, :], total)
    total = jnp.where(j == plan.chunk - 1, weights[1][:, None, :], total)
    out_ref[...] = total.astype(BF16)


def weight_rows(plan, data):
    shape = (plan.ranks, plan.ranks * plan.chunk)
    at = iota(shape, 0) * plan.chunk + plan.chunk - 2
    return [dot(one_hot(iota(shape, 1) == at + e), data) for e in range(2)]


def target_row(info_ref, plan, named):
    lane = info_ref[0]
    ranks, total = plan.ranks, plan.ranks * plan.chunk
    rank = iota((8, ranks), 1)
    fulls = jnp.zeros((8, ranks), I32)
    for i in range(plan.prefill):
        fulls += jnp.where(rank == info_ref[2 + i], 1, 0)
    ones = jnp.full((8, plan.rows), 1.0, BF16)
    counts = lax.dot_general(
        ones, named.astype(BF16), (((1,), (1,)), ((), ())), preferred_element_type=F32
    )
    decode = jnp.where(fulls > 0, 0.0, counts).astype(BF16)
    full = jnp.where(fulls > 0, 1.0, 0.0).astype(BF16)
    spread = (ranks, total)
    source = iota(spread, 1) // plan.chunk
    below = one_hot(iota(spread, 0) < source)
    here = one_hot(iota(spread, 0) == source)
    base = dot(decode, below).astype(I32)
    held = dot(decode, here).astype(I32)
    index = dot(full, below).astype(I32)
    full = dot(full, here) > 0.5
    needed = jnp.sum(decode.astype(F32), axis=1, keepdims=True)
    j = iota((8, total), 1) % plan.chunk
    block, slot = chunk_index(j, plan, lane % 2, full)
    half_rows = plan.decode // 2
    place = base + slot
    second = jnp.where(jnp.where(full, slot - plan.half_pre, place - half_rows) >= 0, 1, 0)
    row = jnp.where(
        full,
        index * plan.half_pre + slot - second * plan.half_pre,
        plan.prefill * plan.half_pre + place - second * half_rows,
    )
    kept = full | ((slot < held) & (place < plan.decode) & ((block < 2) | (second == lane % 2)))
    piece = jnp.where(block == 2, 4, 2 * block + second)
    return jnp.where(kept & (block < 3), piece * plan.half + row, -1), needed


def compact_kernel(plan, info_ref, in_ref, a_ref, b_ref, target_ref, needed_ref):
    total = plan.ranks * plan.chunk
    data = in_ref[...].reshape(total, LANE)
    first = weight_rows(plan, data)[0]
    named = jnp.where(first > 0.0, 1.0, 0.0)
    target, needed = target_row(info_ref, plan, named)
    target_ref[...] = target
    needed_ref[...] = jnp.broadcast_to(needed, (8, LANE))
    side = plan.side
    for ref, begin in ((a_ref, 0), (b_ref, side)):
        for at in range(0, side, plan.step):
            shape = (plan.step, total)
            take = one_hot(iota(shape, 0) + (begin + at) == target[0:1, :])
            ref[at : at + plan.step, :] = dot(take, data).astype(BF16)


def weights_kernel(plan, in_ref, target_ref, weight_ref):
    total = plan.ranks * plan.chunk
    data = in_ref[...].reshape(total, LANE)
    first, second = weight_rows(plan, data)
    place = places(plan, jnp.where(first > 0.0, 1.0, 0.0)).astype(I32)
    full_shape = (plan.ranks, plan.chunk, LANE)
    j = iota(full_shape, 1)
    match = (place[:, None, :] == j) & (j < plan.cap)
    target = target_ref[0:1, :]
    wide = []
    for value in (first, second):
        kept = jnp.where(match, value[:, None, :], 0.0)
        column = jnp.sum(kept, axis=2, keepdims=True)
        wide.append(jnp.broadcast_to(column, full_shape).reshape(total, LANE).astype(BF16))
    for piece in range(2):
        at = piece * plan.half
        take = one_hot(iota((plan.half, total), 0) + at == target)
        for e in range(2):
            weight_ref[at : at + plan.half, e * LANE : (e + 1) * LANE] = dot(take, wide[e])


def spread_table_kernel(plan, target_ref, spread_ref):
    total = plan.ranks * plan.chunk
    col = iota((LANE, LANE), 1)
    for g in range(0, total, LANE):
        wide = jnp.broadcast_to(target_ref[0:1, g : g + LANE], (LANE, LANE))
        column = wide.astype(F32).T.astype(I32)
        for at in range(0, plan.packed_up, LANE):
            spread_ref[g : g + LANE, at : at + LANE] = one_hot(col + at == column)


def combine_table_kernel(plan, info_ref, routes_ref, combine_ref):
    lane, own = info_ref[0], info_ref[1]
    ranks, rows = plan.ranks, plan.rows
    total = ranks * plan.chunk
    full = is_prefill(info_ref, plan, own)
    _, _, place = named_ranks(plan, full, routes_ref)
    square = jnp.concatenate([place, jnp.zeros((rows - ranks, rows), F32)], axis=0)
    turned = square.T[:, :ranks].astype(BF16)
    spread = (ranks, total)
    expand = one_hot(iota(spread, 1) // plan.chunk == iota(spread, 0))
    spots = dot(turned, expand).astype(I32)
    j = iota((1, total), 1) % plan.chunk
    block, slot = chunk_index(j, plan, lane % 2, full)
    match = spots == slot
    for b in range(3):
        combine_ref[:, b * total : (b + 1) * total] = one_hot(match & (block == b))


def lane_at(plan, me, sign, steps):
    return lax.rem(me + sign * steps + plan.lanes, plan.lanes)


def expert_kernel(plan, info_ref, *refs):
    n = len(GATHERED)
    a_refs, b_refs = refs[:n], refs[n : 2 * n]
    weight_ref, wg, wu, wd = refs[2 * n : 2 * n + 4]
    outs = refs[2 * n + 4 : -2]
    x_ref, h_ref = refs[-2:]
    me = info_ref[0]
    sign = 1 - 2 * lax.rem(me, 2)
    lanes, half, slots, side = plan.lanes, plan.half, plan.slots, plan.side
    over = side - slots

    def columns(lane):
        first = pl.multiple_of(lane * (2 * LANE), LANE)
        tail = pl.multiple_of((2 * lanes + lane // 2) * LANE, LANE)
        start = pl.multiple_of(lax.rem(lane, 2) * half, 8)
        return (
            pl.ds(first, LANE),
            pl.ds(pl.multiple_of(first + LANE, LANE), LANE),
            pl.ds(tail, LANE),
            pl.ds(start, half),
        )

    for refs_of, turn in ((a_refs, sign), (b_refs, -sign)):
        for ref, steps in zip(refs_of, GATHERED):
            for i, step in enumerate(steps):
                first, second, tail, rows = columns(lane_at(plan, me, turn, step))
                at = i * side
                if refs_of is a_refs:
                    x_ref[:, first] = ref[at : at + slots, :]
                    x_ref[0:over, second] = ref[at + slots : at + side, :]
                else:
                    x_ref[over:slots, second] = ref[at : at + slots - over, :]
                    x_ref[rows, tail] = ref[at + slots - over : at + side, :]
    turned = (((1,), (1,)), ((), ()))
    x = x_ref[...]
    gate = lax.dot_general(x, wg[...], turned, preferred_element_type=F32)
    up = lax.dot_general(x, wu[...], turned, preferred_element_type=F32)
    hidden = gate / (1.0 + jnp.exp(-gate)) * up * weight_ref[...]
    h_ref[...] = hidden.astype(BF16)
    out = 0
    for steps in SCATTERED:
        for turn in (sign, -sign):
            for i, step in enumerate(steps):
                first, second, tail, rows = columns(lane_at(plan, me, turn, step))
                ref, at = outs[out], i * side
                if turn is sign:
                    ref[at : at + slots, :] = dot(h_ref[...], wd[:, first]).astype(BF16)
                    ref[at + slots : at + side, :] = dot(h_ref[0:over, :], wd[:, second]).astype(BF16)
                else:
                    ref[at : at + slots - over, :] = dot(h_ref[over:slots, :], wd[:, second]).astype(BF16)
                    ref[at + slots - over : at + side, :] = dot(h_ref[rows, :], wd[:, tail]).astype(BF16)
            out += 1


def spread_kernel(plan, take_ref, needed_ref, own_a, got_a, own_b, got_b, out_ref, sum_ref):
    side = plan.side
    sum_ref[0:side, :] = (own_a[...].astype(F32) + got_a[...].astype(F32)).astype(BF16)
    sum_ref[side : 2 * side, :] = (own_b[...].astype(F32) + got_b[...].astype(F32)).astype(BF16)
    sum_ref[2 * side :, :] = jnp.zeros((plan.packed_up - 2 * side, LANE), BF16)
    shape = (plan.ranks, plan.chunk, LANE)
    spread = dot(take_ref[...], sum_ref[...]).reshape(shape)
    over = jnp.where(needed_ref[0:1, :] > float(plan.decode), 1.0, 0.0)
    spread = jnp.where(iota(shape, 1) == plan.chunk - 1, over[None], spread)
    out_ref[...] = spread.astype(BF16)


def combine_kernel(plan, take_ref, in_ref, out_ref, over_ref):
    total = plan.ranks * plan.chunk
    data = in_ref[...].reshape(total, LANE)
    own_rows = plan.own_rows
    for b in range(3):
        mine = dot(take_ref[:, b * total : (b + 1) * total], data).astype(BF16)
        for to in range(plan.lanes):
            out_ref[to, b * own_rows : (b + 1) * own_rows, :] = mine[
                to * own_rows : (to + 1) * own_rows
            ]
    shape = (8, total)
    flags = one_hot(iota(shape, 1) % plan.chunk == plan.chunk - 1)
    over_ref[...] = dot(flags, data)


def finish_kernel(plan, in_ref, out_ref):
    n = plan.own_rows
    for lane in range(plan.lanes):
        at = lane * 2 * LANE
        out_ref[:, at : at + LANE] = in_ref[lane, 0:n, :]
        out_ref[:, at + LANE : at + 2 * LANE] = in_ref[lane, n : 2 * n, :]
    for pair in range(plan.lanes // 2):
        at = (2 * plan.lanes + pair) * LANE
        first = in_ref[2 * pair, 2 * n : 3 * n, :].astype(F32)
        second = in_ref[2 * pair + 1, 2 * n : 3 * n, :].astype(F32)
        out_ref[:, at : at + LANE] = (first + second).astype(BF16)


SMEM = pl.BlockSpec(memory_space=pltpu.SMEM)
VMEM = pl.BlockSpec(memory_space=pltpu.VMEM)
HBM = pl.BlockSpec(memory_space=pltpu.HBM)
GATHERED = ((0,), (1,), (-1, -2), (2, 3), (-3, -4))
SCATTERED = ((-3, -4), (2, 3), (-1, -2), (0,), (1,))


def call(kernel, name, out, specs, *args, scratch=(), limit=24 << 20, flops=0):
    cost = None
    if flops:
        cost = pl.CostEstimate(flops=flops, bytes_accessed=1 << 20, transcendentals=0)
    return pl.pallas_call(
        kernel,
        out_shape=out,
        in_specs=specs,
        out_specs=jax.tree.map(lambda _: VMEM, out),
        scratch_shapes=scratch,
        compiler_params=pltpu.CompilerParams(vmem_limit_bytes=limit),
        cost_estimate=cost,
        interpret=INTERPRET,
        name=name,
    )(*args)


def pack(plan, info, routes, tokens):
    return call(
        lambda *refs: pack_kernel(plan, *refs),
        "pack",
        jax.ShapeDtypeStruct((plan.ranks, plan.chunk, LANE), BF16),
        [SMEM, VMEM, HBM],
        info,
        routes,
        tokens,
        scratch=[pltpu.VMEM((plan.rows, 3 * LANE), BF16), pltpu.SemaphoreType.DMA((2,))],
    )


def compact(plan, info, received):
    share = jax.ShapeDtypeStruct((plan.side, LANE), BF16)
    return call(
        lambda *refs: compact_kernel(plan, *refs),
        "compact",
        (
            share,
            share,
            jax.ShapeDtypeStruct((8, plan.ranks * plan.chunk), I32),
            jax.ShapeDtypeStruct((8, LANE), F32),
        ),
        [SMEM, VMEM],
        info,
        received,
    )


def weights_table(plan, received, target):
    return call(
        lambda *refs: weights_kernel(plan, *refs),
        "weights",
        jax.ShapeDtypeStruct((plan.slots, 2 * LANE), F32),
        [VMEM, VMEM],
        received,
        target,
        flops=1 << 29,
    )


def spread_table(plan, target):
    return call(
        lambda *refs: spread_table_kernel(plan, *refs),
        "spread_table",
        jax.ShapeDtypeStruct((plan.ranks * plan.chunk, plan.packed_up), BF16),
        [VMEM],
        target,
        flops=1 << 29,
    )


def combine_table(plan, info, routes):
    return call(
        lambda *refs: combine_table_kernel(plan, *refs),
        "combine_table",
        jax.ShapeDtypeStruct((plan.rows, 3 * plan.ranks * plan.chunk), BF16),
        [SMEM, VMEM],
        info,
        routes,
        flops=1 << 29,
    )


def experts(plan, info, a_parts, b_parts, weights, w_gate, w_up, w_down):
    hidden = w_gate.shape[0] * w_gate.shape[1]
    flat = [w.reshape(hidden, plan.width) for w in (w_gate, w_up, w_down)]
    out = []
    for steps in SCATTERED:
        out += [jax.ShapeDtypeStruct((len(steps) * plan.side, LANE), BF16)] * 2
    outs = call(
        lambda *refs: expert_kernel(plan, *refs),
        "experts",
        tuple(out),
        [SMEM] + [VMEM] * (2 * len(a_parts) + 4),
        info,
        *a_parts,
        *b_parts,
        weights,
        *flat,
        scratch=[
            pltpu.VMEM((plan.slots, plan.width), BF16),
            pltpu.VMEM((plan.slots, hidden), BF16),
        ],
        limit=32 << 20,
    )
    return outs[0::2], outs[1::2]


def spread(plan, take, needed, own_a, got_a, own_b, got_b):
    return call(
        lambda *refs: spread_kernel(plan, *refs),
        "spread",
        jax.ShapeDtypeStruct((plan.ranks, plan.chunk, LANE), BF16),
        [VMEM] * 6,
        take,
        needed,
        own_a,
        got_a,
        own_b,
        got_b,
        scratch=[pltpu.VMEM((plan.packed_up, LANE), BF16)],
    )


def combine(plan, take, back):
    return call(
        lambda *refs: combine_kernel(plan, *refs),
        "combine",
        (
            jax.ShapeDtypeStruct((plan.lanes, 3 * plan.own_rows, LANE), BF16),
            jax.ShapeDtypeStruct((8, LANE), F32),
        ),
        [VMEM, VMEM],
        take,
        back,
    )


def finish(plan, shares):
    return call(
        lambda *refs: finish_kernel(plan, *refs),
        "finish",
        jax.ShapeDtypeStruct((plan.own_rows, plan.width), BF16),
        [VMEM],
        shares,
    )


def neighbours(lanes):
    near = [(i, i ^ 1) for i in range(lanes)]
    far = [(i, (i - 1 + 2 * (i % 2)) % lanes) for i in range(lanes)]
    return near, far


def swap(arrays, pairs):
    return [lax.ppermute(x, "tp", p) for x, p in zip(arrays, pairs)]


def gather_lanes(shares, lanes, beside):
    near, far = neighbours(lanes)
    own = list(shares)
    first = swap(own, (near, far))
    held = [jnp.concatenate([x, y]) for x, y in zip(own, first)]
    parts, values = [own, first], []
    for hop in range(lanes // 2 - 1):
        if hop < len(beside):
            held, value = lax.optimization_barrier((held, beside[hop]))
            values.append(value)
        held = swap(held, (far, near) if hop % 2 == 0 else (near, far))
        parts.append(held)
    return [p[0] for p in parts], [p[1] for p in parts], values


def plus(x, y):
    return (x.astype(F32) + y.astype(F32)).astype(BF16)


def reduce_lanes(a_outs, b_outs, side, lanes):
    near, far = neighbours(lanes)
    stages = list(zip(a_outs, b_outs))
    held = list(stages[0])
    for hop in range(lanes // 2 - 2):
        got = swap(held, (far, near) if hop % 2 == 0 else (near, far))
        held = [plus(x, y) for x, y in zip(stages[hop + 1], got)]
    got = swap(held, (far, near))
    away = [plus(x, y[side:]) for x, y in zip(stages[-1], got)]
    home = [plus(x, y[:side]) for x, y in zip(stages[-2], got)]
    last = swap(away, (near, far))
    return home[0], last[0], home[1], last[1]


def through_experts(plan, info, received, take_in, matrices):
    a_share, b_share, target, needed = compact(plan, info, received)
    beside = [weights_table(plan, received, target), spread_table(plan, target), take_in]
    a_parts, b_parts, beside = gather_lanes((a_share, b_share), plan.lanes, beside)
    weights, take_out, take_in = beside
    a_outs, b_outs = experts(plan, info, a_parts, b_parts, weights, *matrices)
    sums = reduce_lanes(a_outs, b_outs, plan.side, plan.lanes)
    back = lax.all_to_all(spread(plan, take_out, needed, *sums), "ep", 0, 0, tiled=True)
    return combine(plan, take_in, back)


def on_device(
    tokens, device_choice, local_expert, route_weight, prefill_ranks, w_gate, w_up, w_down
):
    ranks, prefill = lax.axis_size("ep"), prefill_ranks.shape[0]
    sizes = (ranks, lax.axis_size("tp"), *tokens.shape, prefill)
    most = (ranks - prefill) * DEC_RANK
    plan, whole = Plan(*sizes, min(USUAL_DECODE, most)), Plan(*sizes, most)
    places = jnp.stack([lax.axis_index("tp"), lax.axis_index("ep")]).astype(I32)
    info = jnp.concatenate([places, prefill_ranks])
    routes = jnp.concatenate(
        [device_choice.T.astype(F32), local_expert.T.astype(F32), route_weight.T]
    )
    outgoing = pack(plan, info, routes, tokens)
    received = lax.all_to_all(outgoing, "ep", 0, 0, tiled=True)
    take_in = combine_table(plan, info, routes)
    rest = (info, received, take_in, (w_gate, w_up, w_down))
    shares, over = through_experts(plan, *rest)
    rest, over = lax.optimization_barrier((rest, over))
    shares = lax.cond(
        over[0, 0] > 0.0, lambda: through_experts(whole, *rest)[0], lambda: shares
    )
    shares = lax.all_to_all(shares, "tp", 0, 0, tiled=True)
    return finish(plan, shares)


def solution(mesh):
    in_specs = (
        P(("groups", "ep"), None),
        P(("groups", "ep"), None),
        P(("groups", "ep"), None),
        P(("groups", "ep"), None),
        P("groups"),
        P("ep", "tp", None),
        P("ep", "tp", None),
        P("ep", "tp", None),
    )
    out_specs = P(("groups", "ep", "tp"), None)
    return jax.shard_map(
        on_device, mesh=mesh, in_specs=in_specs, out_specs=out_specs, check_vma=False
    )
```

```python
import jax
import jax.numpy as jnp
from jax import lax
from jax.experimental import pallas as pl
from jax.experimental.pallas import tpu as pltpu
from jax.sharding import PartitionSpec as P

TOPK = 6
DEV_TOP = 3
DEC_RANK = 8
USUAL_DECODE = 32
LANE = 128
F32, BF16, I32 = jnp.float32, jnp.bfloat16, jnp.int32
INTERPRET = False


class Plan:
    def __init__(self, ranks, lanes, rows, width, prefill, decode):
        self.ranks, self.lanes, self.rows, self.width = ranks, lanes, rows, width
        self.cap = (DEV_TOP * rows + ranks - 1) // ranks
        self.prefill, self.decode = prefill, decode
        self.half_pre = self.cap // 2
        self.half_dec = DEC_RANK // 2
        self.half = prefill * self.half_pre + decode // 2
        self.slots = 2 * self.half
        self.packed = 5 * self.half
        self.packed_up = -(-self.packed // LANE) * LANE
        self.chunk = 2 * self.cap + self.half_pre + 2
        self.own_rows = rows // lanes
        assert width == (2 * lanes + lanes // 2) * LANE and self.chunk % 8 == 0
        assert rows == LANE and self.half_dec <= self.cap - DEC_RANK and ranks <= LANE


def iota(shape, dim):
    return lax.broadcasted_iota(I32, shape, dim)


def one_hot(mask):
    return jnp.where(mask, 1.0, 0.0).astype(BF16)


def dot(a, b):
    return jnp.dot(a, b, preferred_element_type=F32)


def is_prefill(info_ref, plan, own):
    found = info_ref[2] == own
    for i in range(1, plan.prefill):
        found = found | (info_ref[2 + i] == own)
    return found


def earlier(plan):
    shape = (plan.rows, plan.rows)
    return one_hot(iota(shape, 0) < iota(shape, 1))


def chunk_index(j, plan, parity, full):
    cap = plan.cap
    spill = (j >= DEC_RANK) & (j < cap) & jnp.logical_not(full)
    last = j >= 2 * cap
    block = jnp.where(last | spill, 2, jnp.where(j < cap, 0, 1))
    start = jnp.where(full, parity * plan.half_pre, 0)
    slot = jnp.where(
        spill, j - DEC_RANK + plan.half_dec, jnp.where(last, j - 2 * cap + start, j - block * cap)
    )
    kept = jnp.logical_not(last) | (j - 2 * cap < jnp.where(full, plan.half_pre, plan.half_dec))
    return jnp.where(kept, block, 3), slot


def named_ranks(plan, full, routes_ref):
    shape = (plan.ranks, plan.rows)
    live = iota(shape, 1) < jnp.where(full, plan.rows, DEC_RANK)
    rank = iota(shape, 0)
    hits = [(routes_ref[k : k + 1, :].astype(I32) == rank) & live for k in range(DEV_TOP)]
    named = sum(jnp.where(hit, 1.0, 0.0) for hit in hits)
    return hits, named, places(plan, named)


def places(plan, named):
    before = dot(named.astype(BF16), earlier(plan))
    return jnp.where(named > 0.5, before, -1.0)


def pack_kernel(plan, info_ref, routes_ref, tok_ref, out_ref, x_ref, sems):
    lane, own = info_ref[0], info_ref[1]
    first_at = pl.multiple_of(lane * (2 * LANE), LANE)
    tail_at = pl.multiple_of((2 * plan.lanes + lane // 2) * LANE, LANE)
    copies = [
        pltpu.make_async_copy(
            tok_ref.at[:, pl.ds(first_at, 2 * LANE)], x_ref.at[:, 0 : 2 * LANE], sems.at[0]
        ),
        pltpu.make_async_copy(
            tok_ref.at[:, pl.ds(tail_at, LANE)], x_ref.at[:, 2 * LANE : 3 * LANE], sems.at[1]
        ),
    ]
    for copy in copies:
        copy.start()
    full = is_prefill(info_ref, plan, own)
    hits, named, place = named_ranks(plan, full, routes_ref)
    weights = []
    for e in range(2):
        total = jnp.zeros(named.shape, F32)
        for k, hit in enumerate(hits):
            for j in (2 * k, 2 * k + 1):
                at = DEV_TOP + j
                chosen = hit & (routes_ref[at : at + 1, :] == float(e))
                at += TOPK
                total += jnp.where(chosen, routes_ref[at : at + 1, :], 0.0)
        weights.append(total)
    full_shape = (plan.ranks, plan.chunk, LANE)
    flat = plan.ranks * plan.chunk
    j = iota(full_shape, 1)
    block, slot = chunk_index(j, plan, lane % 2, full)
    match = place.astype(I32)[:, None, :] == slot
    picks = [one_hot(match & (block == b)).reshape(flat, LANE) for b in range(3)]
    for copy in copies:
        copy.wait()
    total = sum(dot(picks[b], x_ref[:, b * LANE : (b + 1) * LANE]) for b in range(3))
    total = total.reshape(full_shape)
    total = jnp.where(j == plan.chunk - 2, weights[0][:, None, :], total)
    total = jnp.where(j == plan.chunk - 1, weights[1][:, None, :], total)
    out_ref[...] = total.astype(BF16)


def weight_rows(plan, data):
    shape = (plan.ranks, plan.ranks * plan.chunk)
    at = iota(shape, 0) * plan.chunk + plan.chunk - 2
    return [dot(one_hot(iota(shape, 1) == at + e), data) for e in range(2)]


def target_row(info_ref, plan, named):
    lane = info_ref[0]
    ranks, total = plan.ranks, plan.ranks * plan.chunk
    rank = iota((8, ranks), 1)
    fulls = jnp.zeros((8, ranks), I32)
    for i in range(plan.prefill):
        fulls += jnp.where(rank == info_ref[2 + i], 1, 0)
    ones = jnp.full((8, plan.rows), 1.0, BF16)
    counts = lax.dot_general(
        ones, named.astype(BF16), (((1,), (1,)), ((), ())), preferred_element_type=F32
    )
    decode = jnp.where(fulls > 0, 0.0, counts).astype(BF16)
    full = jnp.where(fulls > 0, 1.0, 0.0).astype(BF16)
    spread = (ranks, total)
    source = iota(spread, 1) // plan.chunk
    below = one_hot(iota(spread, 0) < source)
    here = one_hot(iota(spread, 0) == source)
    base = dot(decode, below).astype(I32)
    held = dot(decode, here).astype(I32)
    index = dot(full, below).astype(I32)
    full = dot(full, here) > 0.5
    needed = jnp.sum(decode.astype(F32), axis=1, keepdims=True)
    j = iota((8, total), 1) % plan.chunk
    block, slot = chunk_index(j, plan, lane % 2, full)
    half_rows = plan.decode // 2
    place = base + slot
    second = jnp.where(jnp.where(full, slot - plan.half_pre, place - half_rows) >= 0, 1, 0)
    row = jnp.where(
        full,
        index * plan.half_pre + slot - second * plan.half_pre,
        plan.prefill * plan.half_pre + place - second * half_rows,
    )
    kept = full | ((slot < held) & (place < plan.decode) & ((block < 2) | (second == lane % 2)))
    piece = jnp.where(block == 2, 4, 2 * block + second)
    return jnp.where(kept & (block < 3), piece * plan.half + row, -1), needed


def compact_kernel(plan, info_ref, in_ref, out_ref, target_ref, needed_ref):
    total = plan.ranks * plan.chunk
    data = in_ref[...].reshape(total, LANE)
    first = weight_rows(plan, data)[0]
    named = jnp.where(first > 0.0, 1.0, 0.0)
    target, needed = target_row(info_ref, plan, named)
    target_ref[...] = target
    needed_ref[...] = jnp.broadcast_to(needed, (8, LANE))
    for at in range(0, plan.packed, plan.half):
        take = one_hot(iota((plan.half, total), 0) + at == target[0:1, :])
        out_ref[at : at + plan.half, :] = dot(take, data).astype(BF16)


def weights_kernel(plan, in_ref, target_ref, weight_ref):
    total = plan.ranks * plan.chunk
    data = in_ref[...].reshape(total, LANE)
    first, second = weight_rows(plan, data)
    place = places(plan, jnp.where(first > 0.0, 1.0, 0.0)).astype(I32)
    full_shape = (plan.ranks, plan.chunk, LANE)
    j = iota(full_shape, 1)
    match = (place[:, None, :] == j) & (j < plan.cap)
    target = target_ref[0:1, :]
    wide = []
    for value in (first, second):
        kept = jnp.where(match, value[:, None, :], 0.0)
        column = jnp.sum(kept, axis=2, keepdims=True)
        wide.append(jnp.broadcast_to(column, full_shape).reshape(total, LANE).astype(BF16))
    for piece in range(2):
        at = piece * plan.half
        take = one_hot(iota((plan.half, total), 0) + at == target)
        for e in range(2):
            weight_ref[at : at + plan.half, e * LANE : (e + 1) * LANE] = dot(take, wide[e])


def spread_table_kernel(plan, target_ref, spread_ref):
    total = plan.ranks * plan.chunk
    col = iota((LANE, LANE), 1)
    for g in range(0, total, LANE):
        wide = jnp.broadcast_to(target_ref[0:1, g : g + LANE], (LANE, LANE))
        column = wide.astype(F32).T.astype(I32)
        for at in range(0, plan.packed_up, LANE):
            spread_ref[g : g + LANE, at : at + LANE] = one_hot(col + at == column)


def combine_table_kernel(plan, info_ref, routes_ref, combine_ref):
    lane, own = info_ref[0], info_ref[1]
    ranks, rows = plan.ranks, plan.rows
    total = ranks * plan.chunk
    full = is_prefill(info_ref, plan, own)
    _, _, place = named_ranks(plan, full, routes_ref)
    square = jnp.concatenate([place, jnp.zeros((rows - ranks, rows), F32)], axis=0)
    turned = square.T[:, :ranks].astype(BF16)
    spread = (ranks, total)
    expand = one_hot(iota(spread, 1) // plan.chunk == iota(spread, 0))
    spots = dot(turned, expand).astype(I32)
    j = iota((1, total), 1) % plan.chunk
    block, slot = chunk_index(j, plan, lane % 2, full)
    match = spots == slot
    for b in range(3):
        combine_ref[:, b * total : (b + 1) * total] = one_hot(match & (block == b))


def expert_kernel(plan, offsets, info_ref, *refs):
    n = len(offsets)
    weight_ref, wg, wu, wd, out_ref, x_ref, h_ref = refs[n:]
    me = info_ref[0]
    lanes, half, slots = plan.lanes, plan.half, plan.slots
    for offset, part in zip(offsets, refs):
        lane = lax.rem(me + offset + lanes, lanes)
        first = pl.multiple_of(lane * (2 * LANE), LANE)
        tail = pl.multiple_of((2 * lanes + lane // 2) * LANE, LANE)
        start = pl.multiple_of(lax.rem(lane, 2) * half, 8)
        x_ref[:, pl.ds(first, LANE)] = part[0:slots, :]
        x_ref[:, pl.ds(pl.multiple_of(first + LANE, LANE), LANE)] = part[slots : 2 * slots, :]
        x_ref[pl.ds(start, half), pl.ds(tail, LANE)] = part[2 * slots : 2 * slots + half, :]
    turned = (((1,), (1,)), ((), ()))
    x = x_ref[...]
    gate = lax.dot_general(x, wg[...], turned, preferred_element_type=F32)
    up = lax.dot_general(x, wu[...], turned, preferred_element_type=F32)
    hidden = gate / (1.0 + jnp.exp(-gate)) * up * weight_ref[...]
    h_ref[...] = hidden.astype(BF16)
    for lane in range(lanes):
        at = lane * 2 * LANE
        y = dot(h_ref[...], wd[:, at : at + 2 * LANE]).astype(BF16)
        out_ref[lane, 0:slots, :] = y[:, :LANE]
        out_ref[lane, slots : 2 * slots, :] = y[:, LANE:]
    for pair in range(0, lanes // 2, 2):
        at = (2 * lanes + pair) * LANE
        y = dot(h_ref[...], wd[:, at : at + 2 * LANE]).astype(BF16)
        for k in range(2):
            for p in range(2):
                piece = y[p * half : (p + 1) * half, k * LANE : (k + 1) * LANE]
                out_ref[2 * (pair + k) + p, 2 * slots : 2 * slots + half, :] = piece


def spread_kernel(plan, take_ref, needed_ref, in_ref, out_ref, sum_ref):
    total = in_ref[0].astype(F32)
    for lane in range(1, plan.lanes):
        total += in_ref[lane].astype(F32)
    sum_ref[0 : plan.packed, :] = total.astype(BF16)
    sum_ref[plan.packed :, :] = jnp.zeros((plan.packed_up - plan.packed, LANE), BF16)
    shape = (plan.ranks, plan.chunk, LANE)
    spread = dot(take_ref[...], sum_ref[...]).reshape(shape)
    over = jnp.where(needed_ref[0:1, :] > float(plan.decode), 1.0, 0.0)
    spread = jnp.where(iota(shape, 1) == plan.chunk - 1, over[None], spread)
    out_ref[...] = spread.astype(BF16)


def combine_kernel(plan, take_ref, in_ref, out_ref, over_ref):
    total = plan.ranks * plan.chunk
    data = in_ref[...].reshape(total, LANE)
    own_rows = plan.own_rows
    for b in range(3):
        mine = dot(take_ref[:, b * total : (b + 1) * total], data).astype(BF16)
        for to in range(plan.lanes):
            out_ref[to, b * own_rows : (b + 1) * own_rows, :] = mine[
                to * own_rows : (to + 1) * own_rows
            ]
    shape = (8, total)
    flags = one_hot(iota(shape, 1) % plan.chunk == plan.chunk - 1)
    over_ref[...] = dot(flags, data)


def finish_kernel(plan, in_ref, out_ref):
    n = plan.own_rows
    for lane in range(plan.lanes):
        at = lane * 2 * LANE
        out_ref[:, at : at + LANE] = in_ref[lane, 0:n, :]
        out_ref[:, at + LANE : at + 2 * LANE] = in_ref[lane, n : 2 * n, :]
    for pair in range(plan.lanes // 2):
        at = (2 * plan.lanes + pair) * LANE
        first = in_ref[2 * pair, 2 * n : 3 * n, :].astype(F32)
        second = in_ref[2 * pair + 1, 2 * n : 3 * n, :].astype(F32)
        out_ref[:, at : at + LANE] = (first + second).astype(BF16)


SMEM = pl.BlockSpec(memory_space=pltpu.SMEM)
VMEM = pl.BlockSpec(memory_space=pltpu.VMEM)
HBM = pl.BlockSpec(memory_space=pltpu.HBM)

def call(kernel, name, out, specs, *args, scratch=(), limit=24 << 20, flops=0):
    cost = None
    if flops:
        cost = pl.CostEstimate(flops=flops, bytes_accessed=1 << 20, transcendentals=0)
    return pl.pallas_call(
        kernel,
        out_shape=out,
        in_specs=specs,
        out_specs=jax.tree.map(lambda _: VMEM, out),
        scratch_shapes=scratch,
        compiler_params=pltpu.CompilerParams(vmem_limit_bytes=limit),
        cost_estimate=cost,
        interpret=INTERPRET,
        name=name,
    )(*args)


def pack(plan, info, routes, tokens):
    return call(
        lambda *refs: pack_kernel(plan, *refs),
        "pack",
        jax.ShapeDtypeStruct((plan.ranks, plan.chunk, LANE), BF16),
        [SMEM, VMEM, HBM],
        info,
        routes,
        tokens,
        scratch=[pltpu.VMEM((plan.rows, 3 * LANE), BF16), pltpu.SemaphoreType.DMA((2,))],
    )


def compact(plan, info, received):
    return call(
        lambda *refs: compact_kernel(plan, *refs),
        "compact",
        (
            jax.ShapeDtypeStruct((plan.packed, LANE), BF16),
            jax.ShapeDtypeStruct((8, plan.ranks * plan.chunk), I32),
            jax.ShapeDtypeStruct((8, LANE), F32),
        ),
        [SMEM, VMEM],
        info,
        received,
    )


def weights_table(plan, received, target):
    return call(
        lambda *refs: weights_kernel(plan, *refs),
        "weights",
        jax.ShapeDtypeStruct((plan.slots, 2 * LANE), F32),
        [VMEM, VMEM],
        received,
        target,
        flops=1 << 29,
    )


def spread_table(plan, target):
    return call(
        lambda *refs: spread_table_kernel(plan, *refs),
        "spread_table",
        jax.ShapeDtypeStruct((plan.ranks * plan.chunk, plan.packed_up), BF16),
        [VMEM],
        target,
        flops=1 << 29,
    )


def combine_table(plan, info, routes):
    return call(
        lambda *refs: combine_table_kernel(plan, *refs),
        "combine_table",
        jax.ShapeDtypeStruct((plan.rows, 3 * plan.ranks * plan.chunk), BF16),
        [SMEM, VMEM],
        info,
        routes,
        flops=1 << 29,
    )


def experts(plan, offsets, info, parts, weights, w_gate, w_up, w_down):
    hidden = w_gate.shape[0] * w_gate.shape[1]
    flat = [w.reshape(hidden, plan.width) for w in (w_gate, w_up, w_down)]
    return call(
        lambda *refs: expert_kernel(plan, offsets, *refs),
        "experts",
        jax.ShapeDtypeStruct((plan.lanes, plan.packed, LANE), BF16),
        [SMEM] + [VMEM] * (len(parts) + 4),
        info,
        *parts,
        weights,
        *flat,
        scratch=[
            pltpu.VMEM((plan.slots, plan.width), BF16),
            pltpu.VMEM((plan.slots, hidden), BF16),
        ],
        limit=32 << 20,
    )


def spread(plan, take, needed, returned):
    return call(
        lambda *refs: spread_kernel(plan, *refs),
        "spread",
        jax.ShapeDtypeStruct((plan.ranks, plan.chunk, LANE), BF16),
        [VMEM] * 3,
        take,
        needed,
        returned,
        scratch=[pltpu.VMEM((plan.packed_up, LANE), BF16)],
    )


def combine(plan, take, back):
    return call(
        lambda *refs: combine_kernel(plan, *refs),
        "combine",
        (
            jax.ShapeDtypeStruct((plan.lanes, 3 * plan.own_rows, LANE), BF16),
            jax.ShapeDtypeStruct((8, LANE), F32),
        ),
        [VMEM, VMEM],
        take,
        back,
    )


def finish(plan, shares):
    return call(
        lambda *refs: finish_kernel(plan, *refs),
        "finish",
        jax.ShapeDtypeStruct((plan.own_rows, plan.width), BF16),
        [VMEM],
        shares,
    )


def gather_lanes(packed, lanes, beside):
    right = [(i, (i + 1) % lanes) for i in range(lanes)]
    left = [(i, (i - 1) % lanes) for i in range(lanes)]
    parts, offsets, values = [packed], [0], []
    held = [packed, packed]
    for hop in range(1, lanes // 2 + 1):
        if hop > 1 and hop - 2 < len(beside):
            held, value = lax.optimization_barrier((held, beside[hop - 2]))
            values.append(value)
        got = [lax.ppermute(held[0], "tp", right)]
        offsets.append(-hop)
        if hop < lanes // 2:
            got.append(lax.ppermute(held[1], "tp", left))
            offsets.append(hop)
        parts += got
        held = got
    return parts, offsets, values


def through_experts(plan, info, received, take_in, matrices):
    packed, target, needed = compact(plan, info, received)
    beside = [weights_table(plan, received, target), spread_table(plan, target), take_in]
    parts, offsets, beside = gather_lanes(packed, plan.lanes, beside)
    weights, take_out, take_in = beside
    partial = experts(plan, offsets, info, parts, weights, *matrices)
    returned = lax.all_to_all(partial, "tp", 0, 0, tiled=True)
    back = lax.all_to_all(spread(plan, take_out, needed, returned), "ep", 0, 0, tiled=True)
    return combine(plan, take_in, back)


def on_device(
    tokens, device_choice, local_expert, route_weight, prefill_ranks, w_gate, w_up, w_down
):
    ranks, prefill = lax.axis_size("ep"), prefill_ranks.shape[0]
    sizes = (ranks, lax.axis_size("tp"), *tokens.shape, prefill)
    most = (ranks - prefill) * DEC_RANK
    plan, whole = Plan(*sizes, min(USUAL_DECODE, most)), Plan(*sizes, most)
    places = jnp.stack([lax.axis_index("tp"), lax.axis_index("ep")]).astype(I32)
    info = jnp.concatenate([places, prefill_ranks])
    tables = (device_choice, local_expert, route_weight)
    wide = sum(x.shape[1] for x in tables)
    routes, at = 0.0, 0
    for x in tables:
        routes += jnp.pad(x.astype(F32), ((0, 0), (at, wide - at - x.shape[1])))
        at += x.shape[1]
    routes = routes.T
    outgoing = pack(plan, info, routes, tokens)
    received = lax.all_to_all(outgoing, "ep", 0, 0, tiled=True)
    take_in = combine_table(plan, info, routes)
    rest = (info, received, take_in, (w_gate, w_up, w_down))
    shares, over = through_experts(plan, *rest)
    rest, over = lax.optimization_barrier((rest, over))
    shares = lax.cond(
        over[0, 0] > 0.0, lambda: through_experts(whole, *rest)[0], lambda: shares
    )
    shares = lax.all_to_all(shares, "tp", 0, 0, tiled=True)
    return finish(plan, shares)


def solution(mesh):
    in_specs = (
        P(("groups", "ep"), None),
        P(("groups", "ep"), None),
        P(("groups", "ep"), None),
        P(("groups", "ep"), None),
        P("groups"),
        P("ep", "tp", None),
        P("ep", "tp", None),
        P("ep", "tp", None),
    )
    out_specs = P(("groups", "ep", "tp"), None)
    return jax.shard_map(
        on_device, mesh=mesh, in_specs=in_specs, out_specs=out_specs, check_vma=False
    )
```

```python
import jax
import jax.numpy as jnp
from jax import lax
from jax.experimental import pallas as pl
from jax.experimental.pallas import tpu as pltpu
from jax.sharding import PartitionSpec as P

TOPK = 6
DEV_TOP = 3
DEC_RANK = 8
USUAL_DECODE = 32
LANE = 128
F32, BF16, I32 = jnp.float32, jnp.bfloat16, jnp.int32
INTERPRET = False


class Plan:
    def __init__(self, ranks, lanes, rows, width, prefill, decode):
        self.ranks, self.lanes, self.rows, self.width = ranks, lanes, rows, width
        self.cap = (DEV_TOP * rows + ranks - 1) // ranks
        self.prefill, self.decode = prefill, decode
        self.half_pre = self.cap // 2
        self.half_dec = DEC_RANK // 2
        self.half = prefill * self.half_pre + decode // 2
        self.slots = 2 * self.half
        self.packed = 5 * self.half
        self.packed_up = -(-self.packed // LANE) * LANE
        self.chunk = 2 * self.cap + self.half_pre + 2
        self.own_rows = rows // lanes
        assert width == (2 * lanes + lanes // 2) * LANE and self.chunk % 8 == 0
        assert rows == LANE and self.half_dec <= self.cap - DEC_RANK and ranks <= LANE


class Info:
    def __init__(self, pre_ref):
        self.places, self.pre_ref = (lax.axis_index("tp"), lax.axis_index("ep")), pre_ref

    def __getitem__(self, i):
        return self.places[i] if i < 2 else self.pre_ref[i - 2]


def iota(shape, dim):
    return lax.broadcasted_iota(I32, shape, dim)


def one_hot(mask):
    return jnp.where(mask, 1.0, 0.0).astype(BF16)


def dot(a, b):
    return jnp.dot(a, b, preferred_element_type=F32)


def is_prefill(info_ref, plan, own):
    found = info_ref[2] == own
    for i in range(1, plan.prefill):
        found = found | (info_ref[2 + i] == own)
    return found


def earlier(plan):
    shape = (plan.rows, plan.rows)
    return one_hot(iota(shape, 0) < iota(shape, 1))


def chunk_index(j, plan, parity, full):
    cap = plan.cap
    spill = (j >= DEC_RANK) & (j < cap) & jnp.logical_not(full)
    last = j >= 2 * cap
    block = jnp.where(last | spill, 2, jnp.where(j < cap, 0, 1))
    start = jnp.where(full, parity * plan.half_pre, 0)
    slot = jnp.where(
        spill, j - DEC_RANK + plan.half_dec, jnp.where(last, j - 2 * cap + start, j - block * cap)
    )
    kept = jnp.logical_not(last) | (j - 2 * cap < jnp.where(full, plan.half_pre, plan.half_dec))
    return jnp.where(kept, block, 3), slot


def named_ranks(plan, full, choice_ref):
    shape = (plan.ranks, plan.rows)
    live = iota(shape, 1) < jnp.where(full, plan.rows, DEC_RANK)
    rank = iota(shape, 0)
    hits = [(choice_ref[k : k + 1, :] == rank) & live for k in range(DEV_TOP)]
    named = sum(jnp.where(hit, 1.0, 0.0) for hit in hits)
    return hits, named, places(plan, named)


def places(plan, named):
    before = dot(named.astype(BF16), earlier(plan))
    return jnp.where(named > 0.5, before, -1.0)


def pack_kernel(plan, pre_hbm, choice_hbm, le_hbm, rw_hbm, tok_ref, out_ref, *scratch):
    pre_ref, choice_ref, le_ref, rw_ref, x_ref, sems = scratch
    info_ref = Info(pre_ref)
    lane, own = info_ref[0], info_ref[1]
    first_at = pl.multiple_of(lane * (2 * LANE), LANE)
    tail_at = pl.multiple_of((2 * plan.lanes + lane // 2) * LANE, LANE)
    ends = [
        (pre_hbm, pre_ref),
        (choice_hbm, choice_ref),
        (le_hbm, le_ref),
        (rw_hbm, rw_ref),
        (tok_ref.at[:, pl.ds(first_at, 2 * LANE)], x_ref.at[:, 0 : 2 * LANE]),
        (tok_ref.at[:, pl.ds(tail_at, LANE)], x_ref.at[:, 2 * LANE : 3 * LANE]),
    ]
    copies = [pltpu.make_async_copy(a, b, sems.at[i]) for i, (a, b) in enumerate(ends)]
    for copy in copies:
        copy.start()
    for copy in copies[:4]:
        copy.wait()
    full = is_prefill(info_ref, plan, own)
    hits, named, place = named_ranks(plan, full, choice_ref)
    weights = []
    for e in range(2):
        total = jnp.zeros(named.shape, F32)
        for k, hit in enumerate(hits):
            for j in (2 * k, 2 * k + 1):
                chosen = hit & (le_ref[j : j + 1, :] == e)
                total += jnp.where(chosen, rw_ref[j : j + 1, :], 0.0)
        weights.append(total)
    full_shape = (plan.ranks, plan.chunk, LANE)
    flat = plan.ranks * plan.chunk
    j = iota(full_shape, 1)
    block, slot = chunk_index(j, plan, lane % 2, full)
    match = place.astype(I32)[:, None, :] == slot
    picks = [one_hot(match & (block == b)).reshape(flat, LANE) for b in range(3)]
    for copy in copies[4:]:
        copy.wait()
    total = sum(dot(picks[b], x_ref[:, b * LANE : (b + 1) * LANE]) for b in range(3))
    total = total.reshape(full_shape)
    total = jnp.where(j == plan.chunk - 2, weights[0][:, None, :], total)
    total = jnp.where(j == plan.chunk - 1, weights[1][:, None, :], total)
    out_ref[...] = total.astype(BF16)


def weight_rows(plan, data):
    shape = (plan.ranks, plan.ranks * plan.chunk)
    at = iota(shape, 0) * plan.chunk + plan.chunk - 2
    return [dot(one_hot(iota(shape, 1) == at + e), data) for e in range(2)]


def target_row(info_ref, plan, named):
    lane = info_ref[0]
    ranks, total = plan.ranks, plan.ranks * plan.chunk
    rank = iota((8, ranks), 1)
    fulls = jnp.zeros((8, ranks), I32)
    for i in range(plan.prefill):
        fulls += jnp.where(rank == info_ref[2 + i], 1, 0)
    ones = jnp.full((8, plan.rows), 1.0, BF16)
    counts = lax.dot_general(
        ones, named.astype(BF16), (((1,), (1,)), ((), ())), preferred_element_type=F32
    )
    decode = jnp.where(fulls > 0, 0.0, counts).astype(BF16)
    full = jnp.where(fulls > 0, 1.0, 0.0).astype(BF16)
    spread = (ranks, total)
    source = iota(spread, 1) // plan.chunk
    below = one_hot(iota(spread, 0) < source)
    here = one_hot(iota(spread, 0) == source)
    base = dot(decode, below).astype(I32)
    held = dot(decode, here).astype(I32)
    index = dot(full, below).astype(I32)
    full = dot(full, here) > 0.5
    needed = jnp.sum(decode.astype(F32), axis=1, keepdims=True)
    j = iota((8, total), 1) % plan.chunk
    block, slot = chunk_index(j, plan, lane % 2, full)
    half_rows = plan.decode // 2
    place = base + slot
    second = jnp.where(jnp.where(full, slot - plan.half_pre, place - half_rows) >= 0, 1, 0)
    row = jnp.where(
        full,
        index * plan.half_pre + slot - second * plan.half_pre,
        plan.prefill * plan.half_pre + place - second * half_rows,
    )
    kept = full | ((slot < held) & (place < plan.decode) & ((block < 2) | (second == lane % 2)))
    piece = jnp.where(block == 2, 4, 2 * block + second)
    return jnp.where(kept & (block < 3), piece * plan.half + row, -1), needed


def compact_kernel(plan, info_ref, in_ref, out_ref, target_ref, needed_ref):
    total = plan.ranks * plan.chunk
    data = in_ref[...].reshape(total, LANE)
    first = weight_rows(plan, data)[0]
    named = jnp.where(first > 0.0, 1.0, 0.0)
    target, needed = target_row(info_ref, plan, named)
    target_ref[...] = target
    needed_ref[...] = jnp.broadcast_to(needed, (8, LANE))
    for at in range(0, plan.packed, plan.half):
        take = one_hot(iota((plan.half, total), 0) + at == target[0:1, :])
        out_ref[at : at + plan.half, :] = dot(take, data).astype(BF16)


def weights_kernel(plan, in_ref, target_ref, weight_ref):
    total = plan.ranks * plan.chunk
    data = in_ref[...].reshape(total, LANE)
    first, second = weight_rows(plan, data)
    place = places(plan, jnp.where(first > 0.0, 1.0, 0.0)).astype(I32)
    full_shape = (plan.ranks, plan.chunk, LANE)
    j = iota(full_shape, 1)
    match = (place[:, None, :] == j) & (j < plan.cap)
    target = target_ref[0:1, :]
    wide = []
    for value in (first, second):
        kept = jnp.where(match, value[:, None, :], 0.0)
        column = jnp.sum(kept, axis=2, keepdims=True)
        wide.append(jnp.broadcast_to(column, full_shape).reshape(total, LANE).astype(BF16))
    for piece in range(2):
        at = piece * plan.half
        take = one_hot(iota((plan.half, total), 0) + at == target)
        for e in range(2):
            weight_ref[at : at + plan.half, e * LANE : (e + 1) * LANE] = dot(take, wide[e])


def spread_table_kernel(plan, target_ref, spread_ref):
    total = plan.ranks * plan.chunk
    col = iota((LANE, LANE), 1)
    for g in range(0, total, LANE):
        wide = jnp.broadcast_to(target_ref[0:1, g : g + LANE], (LANE, LANE))
        column = wide.astype(F32).T.astype(I32)
        for at in range(0, plan.packed_up, LANE):
            spread_ref[g : g + LANE, at : at + LANE] = one_hot(col + at == column)


def combine_table_kernel(plan, info_ref, choice_ref, combine_ref):
    lane, own = info_ref[0], info_ref[1]
    ranks, rows = plan.ranks, plan.rows
    total = ranks * plan.chunk
    full = is_prefill(info_ref, plan, own)
    _, _, place = named_ranks(plan, full, choice_ref)
    square = jnp.concatenate([place, jnp.zeros((rows - ranks, rows), F32)], axis=0)
    turned = square.T[:, :ranks].astype(BF16)
    spread = (ranks, total)
    expand = one_hot(iota(spread, 1) // plan.chunk == iota(spread, 0))
    spots = dot(turned, expand).astype(I32)
    j = iota((1, total), 1) % plan.chunk
    block, slot = chunk_index(j, plan, lane % 2, full)
    match = spots == slot
    for b in range(3):
        combine_ref[:, b * total : (b + 1) * total] = one_hot(match & (block == b))


def expert_kernel(plan, offsets, info_ref, *refs):
    n = len(offsets)
    weight_ref, wg, wu, wd, out_ref, x_ref, h_ref = refs[n:]
    me = info_ref[0]
    lanes, half, slots = plan.lanes, plan.half, plan.slots
    for offset, part in zip(offsets, refs):
        lane = lax.rem(me + offset + lanes, lanes)
        first = pl.multiple_of(lane * (2 * LANE), LANE)
        tail = pl.multiple_of((2 * lanes + lane // 2) * LANE, LANE)
        start = pl.multiple_of(lax.rem(lane, 2) * half, 8)
        x_ref[:, pl.ds(first, LANE)] = part[0:slots, :]
        x_ref[:, pl.ds(pl.multiple_of(first + LANE, LANE), LANE)] = part[slots : 2 * slots, :]
        x_ref[pl.ds(start, half), pl.ds(tail, LANE)] = part[2 * slots : 2 * slots + half, :]
    turned = (((1,), (1,)), ((), ()))
    x = x_ref[...]
    gate = lax.dot_general(x, wg[...], turned, preferred_element_type=F32)
    up = lax.dot_general(x, wu[...], turned, preferred_element_type=F32)
    hidden = gate / (1.0 + jnp.exp(-gate)) * up * weight_ref[...]
    h_ref[...] = hidden.astype(BF16)
    for lane in range(lanes):
        at = lane * 2 * LANE
        y = dot(h_ref[...], wd[:, at : at + 2 * LANE]).astype(BF16)
        out_ref[lane, 0:slots, :] = y[:, :LANE]
        out_ref[lane, slots : 2 * slots, :] = y[:, LANE:]
    for pair in range(0, lanes // 2, 2):
        at = (2 * lanes + pair) * LANE
        y = dot(h_ref[...], wd[:, at : at + 2 * LANE]).astype(BF16)
        for k in range(2):
            for p in range(2):
                piece = y[p * half : (p + 1) * half, k * LANE : (k + 1) * LANE]
                out_ref[2 * (pair + k) + p, 2 * slots : 2 * slots + half, :] = piece


def spread_kernel(plan, take_ref, needed_ref, in_ref, out_ref, sum_ref):
    total = in_ref[0].astype(F32)
    for lane in range(1, plan.lanes):
        total += in_ref[lane].astype(F32)
    sum_ref[0 : plan.packed, :] = total.astype(BF16)
    sum_ref[plan.packed :, :] = jnp.zeros((plan.packed_up - plan.packed, LANE), BF16)
    shape = (plan.ranks, plan.chunk, LANE)
    spread = dot(take_ref[...], sum_ref[...]).reshape(shape)
    over = jnp.where(needed_ref[0:1, :] > float(plan.decode), 1.0, 0.0)
    spread = jnp.where(iota(shape, 1) == plan.chunk - 1, over[None], spread)
    out_ref[...] = spread.astype(BF16)


def combine_kernel(plan, take_ref, in_ref, out_ref, over_ref):
    total = plan.ranks * plan.chunk
    data = in_ref[...].reshape(total, LANE)
    own_rows = plan.own_rows
    for b in range(3):
        mine = dot(take_ref[:, b * total : (b + 1) * total], data).astype(BF16)
        for to in range(plan.lanes):
            out_ref[to, b * own_rows : (b + 1) * own_rows, :] = mine[
                to * own_rows : (to + 1) * own_rows
            ]
    shape = (8, total)
    flags = one_hot(iota(shape, 1) % plan.chunk == plan.chunk - 1)
    over_ref[0] = jnp.where(jnp.max(dot(flags, data)) > 0.0, 1, 0)


def finish_kernel(plan, in_ref, out_ref):
    n = plan.own_rows
    for lane in range(plan.lanes):
        at = lane * 2 * LANE
        out_ref[:, at : at + LANE] = in_ref[lane, 0:n, :]
        out_ref[:, at + LANE : at + 2 * LANE] = in_ref[lane, n : 2 * n, :]
    for pair in range(plan.lanes // 2):
        at = (2 * plan.lanes + pair) * LANE
        first = in_ref[2 * pair, 2 * n : 3 * n, :].astype(F32)
        second = in_ref[2 * pair + 1, 2 * n : 3 * n, :].astype(F32)
        out_ref[:, at : at + LANE] = (first + second).astype(BF16)


SMEM = pl.BlockSpec(memory_space=pltpu.SMEM)
VMEM = pl.BlockSpec(memory_space=pltpu.VMEM)
HBM = pl.BlockSpec(memory_space=pltpu.HBM)

def call(kernel, name, out, specs, *args, scratch=(), limit=24 << 20, flops=0):
    cost = None
    if flops:
        cost = pl.CostEstimate(flops=flops, bytes_accessed=1 << 20, transcendentals=0)
    return pl.pallas_call(
        kernel,
        out_shape=out,
        in_specs=specs,
        out_specs=jax.tree.map(lambda o: SMEM if o.shape == (1,) else VMEM, out),
        scratch_shapes=scratch,
        compiler_params=pltpu.CompilerParams(vmem_limit_bytes=limit),
        cost_estimate=cost,
        interpret=INTERPRET,
        name=name,
    )(*args)


def pack(plan, prefill_ranks, choice, local, weights, tokens):
    return call(
        lambda *refs: pack_kernel(plan, *refs),
        "pack",
        jax.ShapeDtypeStruct((plan.ranks, plan.chunk, LANE), BF16),
        [HBM] * 5,
        prefill_ranks,
        choice,
        local,
        weights,
        tokens,
        scratch=[
            pltpu.SMEM(prefill_ranks.shape, I32),
            pltpu.VMEM(choice.shape, I32),
            pltpu.VMEM(local.shape, I32),
            pltpu.VMEM(weights.shape, F32),
            pltpu.VMEM((plan.rows, 3 * LANE), BF16),
            pltpu.SemaphoreType.DMA((6,)),
        ],
    )


def compact(plan, info, received):
    return call(
        lambda *refs: compact_kernel(plan, Info(refs[0]), *refs[1:]),
        "compact",
        (
            jax.ShapeDtypeStruct((plan.packed, LANE), BF16),
            jax.ShapeDtypeStruct((8, plan.ranks * plan.chunk), I32),
            jax.ShapeDtypeStruct((8, LANE), F32),
        ),
        [SMEM, VMEM],
        info,
        received,
    )


def weights_table(plan, received, target):
    return call(
        lambda *refs: weights_kernel(plan, *refs),
        "weights",
        jax.ShapeDtypeStruct((plan.slots, 2 * LANE), F32),
        [VMEM, VMEM],
        received,
        target,
        flops=1 << 29,
    )


def spread_table(plan, target):
    return call(
        lambda *refs: spread_table_kernel(plan, *refs),
        "spread_table",
        jax.ShapeDtypeStruct((plan.ranks * plan.chunk, plan.packed_up), BF16),
        [VMEM],
        target,
        flops=1 << 29,
    )


def combine_table(plan, info, choice):
    return call(
        lambda *refs: combine_table_kernel(plan, Info(refs[0]), *refs[1:]),
        "combine_table",
        jax.ShapeDtypeStruct((plan.rows, 3 * plan.ranks * plan.chunk), BF16),
        [SMEM, VMEM],
        info,
        choice,
        flops=1 << 29,
    )


def experts(plan, offsets, info, parts, weights, w_gate, w_up, w_down):
    hidden = w_gate.shape[0] * w_gate.shape[1]
    flat = [w.reshape(hidden, plan.width) for w in (w_gate, w_up, w_down)]
    return call(
        lambda *refs: expert_kernel(plan, offsets, Info(refs[0]), *refs[1:]),
        "experts",
        jax.ShapeDtypeStruct((plan.lanes, plan.packed, LANE), BF16),
        [SMEM] + [VMEM] * (len(parts) + 4),
        info,
        *parts,
        weights,
        *flat,
        scratch=[
            pltpu.VMEM((plan.slots, plan.width), BF16),
            pltpu.VMEM((plan.slots, hidden), BF16),
        ],
        limit=32 << 20,
    )


def spread(plan, take, needed, returned):
    return call(
        lambda *refs: spread_kernel(plan, *refs),
        "spread",
        jax.ShapeDtypeStruct((plan.ranks, plan.chunk, LANE), BF16),
        [VMEM] * 3,
        take,
        needed,
        returned,
        scratch=[pltpu.VMEM((plan.packed_up, LANE), BF16)],
    )


def combine(plan, take, back):
    return call(
        lambda *refs: combine_kernel(plan, *refs),
        "combine",
        (
            jax.ShapeDtypeStruct((plan.lanes, 3 * plan.own_rows, LANE), BF16),
            jax.ShapeDtypeStruct((1,), I32),
        ),
        [VMEM, VMEM],
        take,
        back,
    )


def finish(plan, shares):
    return call(
        lambda *refs: finish_kernel(plan, *refs),
        "finish",
        jax.ShapeDtypeStruct((plan.own_rows, plan.width), BF16),
        [VMEM],
        shares,
    )


def gather_lanes(packed, lanes, beside):
    right = [(i, (i + 1) % lanes) for i in range(lanes)]
    left = [(i, (i - 1) % lanes) for i in range(lanes)]
    parts, offsets, values = [packed], [0], []
    held = [packed, packed]
    for hop in range(1, lanes // 2 + 1):
        if hop > 1 and hop - 2 < len(beside):
            first, value = lax.optimization_barrier((held[0], beside[hop - 2]))
            held = [first, held[1]]
            values.append(value)
        got = [lax.ppermute(held[0], "tp", right)]
        offsets.append(-hop)
        if hop < lanes // 2:
            got.append(lax.ppermute(held[1], "tp", left))
            offsets.append(hop)
        parts += got
        held = got
    return parts, offsets, values


def through_experts(plan, info, received, take_in, matrices):
    packed, target, needed = compact(plan, info, received)
    beside = [weights_table(plan, received, target), spread_table(plan, target), take_in]
    parts, offsets, beside = gather_lanes(packed, plan.lanes, beside)
    weights, take_out, take_in = beside
    partial = experts(plan, offsets, info, parts, weights, *matrices)
    returned = lax.all_to_all(partial, "tp", 0, 0, tiled=True)
    back = lax.all_to_all(spread(plan, take_out, needed, returned), "ep", 0, 0, tiled=True)
    return combine(plan, take_in, back)


def on_device(
    tokens, device_choice, local_expert, route_weight, prefill_ranks, w_gate, w_up, w_down
):
    ranks, prefill = lax.axis_size("ep"), prefill_ranks.shape[0]
    sizes = (ranks, lax.axis_size("tp"), *tokens.shape, prefill)
    most = (ranks - prefill) * DEC_RANK
    plan, whole = Plan(*sizes, min(USUAL_DECODE, most)), Plan(*sizes, most)
    stay = [prefill_ranks, device_choice.T, local_expert.T, route_weight.T, tokens]
    stay = [pltpu.with_memory_space_constraint(x, pltpu.HBM) for x in stay]
    outgoing = pack(plan, *stay)
    received = lax.all_to_all(outgoing, "ep", 0, 0, tiled=True)
    received, info, choice = lax.optimization_barrier((received, stay[0], stay[1]))
    take_in = combine_table(plan, info, choice)
    rest = (info, received, take_in, (w_gate, w_up, w_down))
    shares, over = through_experts(plan, *rest)
    rest, over = lax.optimization_barrier((rest, over))
    shares = lax.cond(
        over[0] > 0, lambda: through_experts(whole, *rest)[0], lambda: shares
    )
    shares = lax.all_to_all(shares, "tp", 0, 0, tiled=True)
    return finish(plan, shares)


def solution(mesh):
    in_specs = (
        P(("groups", "ep"), None),
        P(("groups", "ep"), None),
        P(("groups", "ep"), None),
        P(("groups", "ep"), None),
        P("groups"),
        P("ep", "tp", None),
        P("ep", "tp", None),
        P("ep", "tp", None),
    )
    out_specs = P(("groups", "ep", "tp"), None)
    return jax.shard_map(
        on_device, mesh=mesh, in_specs=in_specs, out_specs=out_specs, check_vma=False
    )
```

```python
import jax
import jax.numpy as jnp
from jax import lax
from jax.experimental import pallas as pl
from jax.experimental.pallas import tpu as pltpu
from jax.sharding import PartitionSpec as P

TOPK = 6
DEV_TOP = 3
DEC_RANK = 8
USUAL_DECODE = 32
LANE = 128
F32, BF16, I32 = jnp.float32, jnp.bfloat16, jnp.int32
INTERPRET = False


class Plan:
    def __init__(self, ranks, lanes, rows, width, prefill, decode):
        self.ranks, self.lanes, self.rows, self.width = ranks, lanes, rows, width
        self.cap = (DEV_TOP * rows + ranks - 1) // ranks
        self.prefill, self.decode = prefill, decode
        self.half_pre = self.cap // 2
        self.half_dec = DEC_RANK // 2
        self.half = prefill * self.half_pre + decode // 2
        self.slots = 2 * self.half
        self.packed = 5 * self.half
        self.packed_up = -(-self.packed // LANE) * LANE
        self.chunk = 2 * self.cap + self.half_pre + 2
        self.own_rows = rows // lanes
        assert width == (2 * lanes + lanes // 2) * LANE and self.chunk % 8 == 0
        assert rows == LANE and self.half_dec <= self.cap - DEC_RANK and ranks <= LANE


class Info:
    def __init__(self, pre_ref):
        self.places, self.pre_ref = (lax.axis_index("tp"), lax.axis_index("ep")), pre_ref

    def __getitem__(self, i):
        return self.places[i] if i < 2 else self.pre_ref[i - 2]


def iota(shape, dim):
    return lax.broadcasted_iota(I32, shape, dim)


def one_hot(mask):
    return jnp.where(mask, 1.0, 0.0).astype(BF16)


def dot(a, b):
    return jnp.dot(a, b, preferred_element_type=F32)


def is_prefill(info_ref, plan, own):
    found = info_ref[2] == own
    for i in range(1, plan.prefill):
        found = found | (info_ref[2 + i] == own)
    return found


def earlier(plan):
    shape = (plan.rows, plan.rows)
    return one_hot(iota(shape, 0) < iota(shape, 1))


def chunk_index(j, plan, parity, full):
    cap = plan.cap
    spill = (j >= DEC_RANK) & (j < cap) & jnp.logical_not(full)
    last = j >= 2 * cap
    block = jnp.where(last | spill, 2, jnp.where(j < cap, 0, 1))
    start = jnp.where(full, parity * plan.half_pre, 0)
    slot = jnp.where(
        spill, j - DEC_RANK + plan.half_dec, jnp.where(last, j - 2 * cap + start, j - block * cap)
    )
    kept = jnp.logical_not(last) | (j - 2 * cap < jnp.where(full, plan.half_pre, plan.half_dec))
    return jnp.where(kept, block, 3), slot


def named_ranks(plan, full, choice_ref):
    shape = (plan.ranks, plan.rows)
    live = iota(shape, 1) < jnp.where(full, plan.rows, DEC_RANK)
    rank = iota(shape, 0)
    hits = [(choice_ref[k : k + 1, :] == rank) & live for k in range(DEV_TOP)]
    named = sum(jnp.where(hit, 1.0, 0.0) for hit in hits)
    return hits, named, places(plan, named)


def places(plan, named):
    before = dot(named.astype(BF16), earlier(plan))
    return jnp.where(named > 0.5, before, -1.0)


def pack_kernel(plan, pre_hbm, choice_hbm, le_hbm, rw_hbm, tok_ref, out_ref, *scratch):
    pre_ref, choice_ref, le_ref, rw_ref, x_ref, sems = scratch
    info_ref = Info(pre_ref)
    lane, own = info_ref[0], info_ref[1]
    first_at = pl.multiple_of(lane * (2 * LANE), LANE)
    tail_at = pl.multiple_of((2 * plan.lanes + lane // 2) * LANE, LANE)
    ends = [
        (pre_hbm, pre_ref),
        (choice_hbm, choice_ref),
        (le_hbm, le_ref),
        (rw_hbm, rw_ref),
        (tok_ref.at[:, pl.ds(first_at, 2 * LANE)], x_ref.at[:, 0 : 2 * LANE]),
        (tok_ref.at[:, pl.ds(tail_at, LANE)], x_ref.at[:, 2 * LANE : 3 * LANE]),
    ]
    copies = [pltpu.make_async_copy(a, b, sems.at[i]) for i, (a, b) in enumerate(ends)]
    for copy in copies:
        copy.start()
    for copy in copies[:4]:
        copy.wait()
    full = is_prefill(info_ref, plan, own)
    hits, named, place = named_ranks(plan, full, choice_ref)
    weights = []
    for e in range(2):
        total = jnp.zeros(named.shape, F32)
        for k, hit in enumerate(hits):
            for j in (2 * k, 2 * k + 1):
                chosen = hit & (le_ref[j : j + 1, :] == e)
                total += jnp.where(chosen, rw_ref[j : j + 1, :], 0.0)
        weights.append(total)
    full_shape = (plan.ranks, plan.chunk, LANE)
    flat = plan.ranks * plan.chunk
    j = iota(full_shape, 1)
    block, slot = chunk_index(j, plan, lane % 2, full)
    match = place.astype(I32)[:, None, :] == slot
    picks = [one_hot(match & (block == b)).reshape(flat, LANE) for b in range(3)]
    for copy in copies[4:]:
        copy.wait()
    total = sum(dot(picks[b], x_ref[:, b * LANE : (b + 1) * LANE]) for b in range(3))
    total = total.reshape(full_shape)
    total = jnp.where(j == plan.chunk - 2, weights[0][:, None, :], total)
    total = jnp.where(j == plan.chunk - 1, weights[1][:, None, :], total)
    out_ref[...] = total.astype(BF16)


def weight_rows(plan, data):
    shape = (plan.ranks, plan.ranks * plan.chunk)
    at = iota(shape, 0) * plan.chunk + plan.chunk - 2
    return [dot(one_hot(iota(shape, 1) == at + e), data) for e in range(2)]


def target_row(info_ref, plan, named):
    lane = info_ref[0]
    ranks, total = plan.ranks, plan.ranks * plan.chunk
    rank = iota((8, ranks), 1)
    fulls = jnp.zeros((8, ranks), I32)
    for i in range(plan.prefill):
        fulls += jnp.where(rank == info_ref[2 + i], 1, 0)
    ones = jnp.full((8, plan.rows), 1.0, BF16)
    counts = lax.dot_general(
        ones, named.astype(BF16), (((1,), (1,)), ((), ())), preferred_element_type=F32
    )
    decode = jnp.where(fulls > 0, 0.0, counts).astype(BF16)
    full = jnp.where(fulls > 0, 1.0, 0.0).astype(BF16)
    spread = (ranks, total)
    source = iota(spread, 1) // plan.chunk
    below = one_hot(iota(spread, 0) < source)
    here = one_hot(iota(spread, 0) == source)
    base = dot(decode, below).astype(I32)
    held = dot(decode, here).astype(I32)
    index = dot(full, below).astype(I32)
    full = dot(full, here) > 0.5
    needed = jnp.sum(decode.astype(F32), axis=1, keepdims=True)
    j = iota((8, total), 1) % plan.chunk
    block, slot = chunk_index(j, plan, lane % 2, full)
    half_rows = plan.decode // 2
    place = base + slot
    second = jnp.where(jnp.where(full, slot - plan.half_pre, place - half_rows) >= 0, 1, 0)
    row = jnp.where(
        full,
        index * plan.half_pre + slot - second * plan.half_pre,
        plan.prefill * plan.half_pre + place - second * half_rows,
    )
    kept = full | ((slot < held) & (place < plan.decode) & ((block < 2) | (second == lane % 2)))
    piece = jnp.where(block == 2, 4, 2 * block + second)
    return jnp.where(kept & (block < 3), piece * plan.half + row, -1), needed


def compact_kernel(plan, info_ref, in_ref, out_ref, target_ref, needed_ref):
    total = plan.ranks * plan.chunk
    data = in_ref[...].reshape(total, LANE)
    first = weight_rows(plan, data)[0]
    named = jnp.where(first > 0.0, 1.0, 0.0)
    target, needed = target_row(info_ref, plan, named)
    target_ref[...] = target
    needed_ref[...] = jnp.broadcast_to(needed, (8, LANE))
    for at in range(0, plan.packed, plan.half):
        take = one_hot(iota((plan.half, total), 0) + at == target[0:1, :])
        out_ref[at : at + plan.half, :] = dot(take, data).astype(BF16)


def weights_kernel(plan, in_ref, target_ref, weight_ref):
    total = plan.ranks * plan.chunk
    data = in_ref[...].reshape(total, LANE)
    first, second = weight_rows(plan, data)
    place = places(plan, jnp.where(first > 0.0, 1.0, 0.0)).astype(I32)
    full_shape = (plan.ranks, plan.chunk, LANE)
    j = iota(full_shape, 1)
    match = (place[:, None, :] == j) & (j < plan.cap)
    target = target_ref[0:1, :]
    wide = []
    for value in (first, second):
        kept = jnp.where(match, value[:, None, :], 0.0)
        column = jnp.sum(kept, axis=2, keepdims=True)
        wide.append(jnp.broadcast_to(column, full_shape).reshape(total, LANE).astype(BF16))
    for piece in range(2):
        at = piece * plan.half
        take = one_hot(iota((plan.half, total), 0) + at == target)
        for e in range(2):
            weight_ref[at : at + plan.half, e * LANE : (e + 1) * LANE] = dot(take, wide[e])


def spread_table_kernel(plan, target_ref, spread_ref):
    total = plan.ranks * plan.chunk
    col = iota((LANE, LANE), 1)
    for g in range(0, total, LANE):
        wide = jnp.broadcast_to(target_ref[0:1, g : g + LANE], (LANE, LANE))
        column = wide.astype(F32).T.astype(I32)
        for at in range(0, plan.packed_up, LANE):
            spread_ref[g : g + LANE, at : at + LANE] = one_hot(col + at == column)


def combine_table_kernel(plan, info_ref, choice_ref, combine_ref):
    lane, own = info_ref[0], info_ref[1]
    ranks, rows = plan.ranks, plan.rows
    total = ranks * plan.chunk
    full = is_prefill(info_ref, plan, own)
    _, _, place = named_ranks(plan, full, choice_ref)
    square = jnp.concatenate([place, jnp.zeros((rows - ranks, rows), F32)], axis=0)
    turned = square.T[:, :ranks].astype(BF16)
    spread = (ranks, total)
    expand = one_hot(iota(spread, 1) // plan.chunk == iota(spread, 0))
    spots = dot(turned, expand).astype(I32)
    j = iota((1, total), 1) % plan.chunk
    block, slot = chunk_index(j, plan, lane % 2, full)
    match = spots == slot
    for b in range(3):
        combine_ref[:, b * total : (b + 1) * total] = one_hot(match & (block == b))


def expert_kernel(plan, offsets, info_ref, *refs):
    n = len(offsets)
    weight_ref, wg, wu, wd, out_ref, x_ref, h_ref = refs[n:]
    me, way = info_ref[0], 1 - 2 * lax.rem(info_ref[1], 2)
    lanes, half, slots = plan.lanes, plan.half, plan.slots
    for offset, part in zip(offsets, refs):
        lane = lax.rem(me + way * offset + lanes, lanes)
        first = pl.multiple_of(lane * (2 * LANE), LANE)
        tail = pl.multiple_of((2 * lanes + lane // 2) * LANE, LANE)
        start = pl.multiple_of(lax.rem(lane, 2) * half, 8)
        x_ref[:, pl.ds(first, LANE)] = part[0:slots, :]
        x_ref[:, pl.ds(pl.multiple_of(first + LANE, LANE), LANE)] = part[slots : 2 * slots, :]
        x_ref[pl.ds(start, half), pl.ds(tail, LANE)] = part[2 * slots : 2 * slots + half, :]
    turned = (((1,), (1,)), ((), ()))
    x = x_ref[...]
    gate = lax.dot_general(x, wg[...], turned, preferred_element_type=F32)
    up = lax.dot_general(x, wu[...], turned, preferred_element_type=F32)
    hidden = gate / (1.0 + jnp.exp(-gate)) * up * weight_ref[...]
    h_ref[...] = hidden.astype(BF16)
    for lane in range(lanes):
        at = lane * 2 * LANE
        y = dot(h_ref[...], wd[:, at : at + 2 * LANE]).astype(BF16)
        out_ref[lane, 0:slots, :] = y[:, :LANE]
        out_ref[lane, slots : 2 * slots, :] = y[:, LANE:]
    for pair in range(0, lanes // 2, 2):
        at = (2 * lanes + pair) * LANE
        y = dot(h_ref[...], wd[:, at : at + 2 * LANE]).astype(BF16)
        for k in range(2):
            for p in range(2):
                piece = y[p * half : (p + 1) * half, k * LANE : (k + 1) * LANE]
                out_ref[2 * (pair + k) + p, 2 * slots : 2 * slots + half, :] = piece


def spread_kernel(plan, take_ref, needed_ref, in_ref, out_ref, sum_ref):
    total = in_ref[0].astype(F32)
    for lane in range(1, plan.lanes):
        total += in_ref[lane].astype(F32)
    sum_ref[0 : plan.packed, :] = total.astype(BF16)
    sum_ref[plan.packed :, :] = jnp.zeros((plan.packed_up - plan.packed, LANE), BF16)
    shape = (plan.ranks, plan.chunk, LANE)
    spread = dot(take_ref[...], sum_ref[...]).reshape(shape)
    over = jnp.where(needed_ref[0:1, :] > float(plan.decode), 1.0, 0.0)
    spread = jnp.where(iota(shape, 1) == plan.chunk - 1, over[None], spread)
    out_ref[...] = spread.astype(BF16)


def combine_kernel(plan, take_ref, in_ref, out_ref, over_ref):
    total = plan.ranks * plan.chunk
    data = in_ref[...].reshape(total, LANE)
    own_rows = plan.own_rows
    for b in range(3):
        mine = dot(take_ref[:, b * total : (b + 1) * total], data).astype(BF16)
        for to in range(plan.lanes):
            out_ref[to, b * own_rows : (b + 1) * own_rows, :] = mine[
                to * own_rows : (to + 1) * own_rows
            ]
    shape = (8, total)
    flags = one_hot(iota(shape, 1) % plan.chunk == plan.chunk - 1)
    over_ref[0] = jnp.where(jnp.max(dot(flags, data)) > 0.0, 1, 0)


def finish_kernel(plan, in_ref, out_ref):
    n = plan.own_rows
    for lane in range(plan.lanes):
        at = lane * 2 * LANE
        out_ref[:, at : at + LANE] = in_ref[lane, 0:n, :]
        out_ref[:, at + LANE : at + 2 * LANE] = in_ref[lane, n : 2 * n, :]
    for pair in range(plan.lanes // 2):
        at = (2 * plan.lanes + pair) * LANE
        first = in_ref[2 * pair, 2 * n : 3 * n, :].astype(F32)
        second = in_ref[2 * pair + 1, 2 * n : 3 * n, :].astype(F32)
        out_ref[:, at : at + LANE] = (first + second).astype(BF16)


SMEM = pl.BlockSpec(memory_space=pltpu.SMEM)
VMEM = pl.BlockSpec(memory_space=pltpu.VMEM)
HBM = pl.BlockSpec(memory_space=pltpu.HBM)

def call(kernel, name, out, specs, *args, scratch=(), limit=24 << 20, flops=0):
    cost = None
    if flops:
        cost = pl.CostEstimate(flops=flops, bytes_accessed=1 << 20, transcendentals=0)
    return pl.pallas_call(
        kernel,
        out_shape=out,
        in_specs=specs,
        out_specs=jax.tree.map(lambda o: SMEM if o.shape == (1,) else VMEM, out),
        scratch_shapes=scratch,
        compiler_params=pltpu.CompilerParams(vmem_limit_bytes=limit),
        cost_estimate=cost,
        interpret=INTERPRET,
        name=name,
    )(*args)


def pack(plan, prefill_ranks, choice, local, weights, tokens):
    return call(
        lambda *refs: pack_kernel(plan, *refs),
        "pack",
        jax.ShapeDtypeStruct((plan.ranks, plan.chunk, LANE), BF16),
        [HBM] * 5,
        prefill_ranks,
        choice,
        local,
        weights,
        tokens,
        scratch=[
            pltpu.SMEM(prefill_ranks.shape, I32),
            pltpu.VMEM(choice.shape, I32),
            pltpu.VMEM(local.shape, I32),
            pltpu.VMEM(weights.shape, F32),
            pltpu.VMEM((plan.rows, 3 * LANE), BF16),
            pltpu.SemaphoreType.DMA((6,)),
        ],
    )


def compact(plan, info, received):
    return call(
        lambda *refs: compact_kernel(plan, Info(refs[0]), *refs[1:]),
        "compact",
        (
            jax.ShapeDtypeStruct((plan.packed, LANE), BF16),
            jax.ShapeDtypeStruct((8, plan.ranks * plan.chunk), I32),
            jax.ShapeDtypeStruct((8, LANE), F32),
        ),
        [SMEM, VMEM],
        info,
        received,
    )


def weights_table(plan, received, target):
    return call(
        lambda *refs: weights_kernel(plan, *refs),
        "weights",
        jax.ShapeDtypeStruct((plan.slots, 2 * LANE), F32),
        [VMEM, VMEM],
        received,
        target,
        flops=1 << 29,
    )


def spread_table(plan, target):
    return call(
        lambda *refs: spread_table_kernel(plan, *refs),
        "spread_table",
        jax.ShapeDtypeStruct((plan.ranks * plan.chunk, plan.packed_up), BF16),
        [VMEM],
        target,
        flops=1 << 29,
    )


def combine_table(plan, info, choice):
    return call(
        lambda *refs: combine_table_kernel(plan, Info(refs[0]), *refs[1:]),
        "combine_table",
        jax.ShapeDtypeStruct((plan.rows, 3 * plan.ranks * plan.chunk), BF16),
        [SMEM, VMEM],
        info,
        choice,
        flops=1 << 29,
    )


def experts(plan, offsets, info, parts, weights, w_gate, w_up, w_down):
    hidden = w_gate.shape[0] * w_gate.shape[1]
    flat = [w.reshape(hidden, plan.width) for w in (w_gate, w_up, w_down)]
    return call(
        lambda *refs: expert_kernel(plan, offsets, Info(refs[0]), *refs[1:]),
        "experts",
        jax.ShapeDtypeStruct((plan.lanes, plan.packed, LANE), BF16),
        [SMEM] + [VMEM] * (len(parts) + 4),
        info,
        *parts,
        weights,
        *flat,
        scratch=[
            pltpu.VMEM((plan.slots, plan.width), BF16),
            pltpu.VMEM((plan.slots, hidden), BF16),
        ],
        limit=32 << 20,
    )


def spread(plan, take, needed, returned):
    return call(
        lambda *refs: spread_kernel(plan, *refs),
        "spread",
        jax.ShapeDtypeStruct((plan.ranks, plan.chunk, LANE), BF16),
        [VMEM] * 3,
        take,
        needed,
        returned,
        scratch=[pltpu.VMEM((plan.packed_up, LANE), BF16)],
    )


def combine(plan, take, back):
    return call(
        lambda *refs: combine_kernel(plan, *refs),
        "combine",
        (
            jax.ShapeDtypeStruct((plan.lanes, 3 * plan.own_rows, LANE), BF16),
            jax.ShapeDtypeStruct((1,), I32),
        ),
        [VMEM, VMEM],
        take,
        back,
    )


def finish(plan, shares):
    return call(
        lambda *refs: finish_kernel(plan, *refs),
        "finish",
        jax.ShapeDtypeStruct((plan.own_rows, plan.width), BF16),
        [VMEM],
        shares,
    )


def gather_lanes(packed, lanes, beside):
    ranks = lax.axis_size("ep")
    ways = []
    for way in (1, -1):
        steps = [way if rank % 2 == 0 else -way for rank in range(ranks)]
        ways.append(
            [
                (rank * lanes + i, rank * lanes + (i + steps[rank]) % lanes)
                for rank in range(ranks)
                for i in range(lanes)
            ]
        )
    right, left = ways
    axes = ("ep", "tp")
    parts, offsets, values = [packed], [0], []
    held = [packed, packed]
    for hop in range(1, lanes // 2 + 1):
        if hop > 1 and hop - 2 < len(beside):
            first, value = lax.optimization_barrier((held[0], beside[hop - 2]))
            held = [first, held[1]]
            values.append(value)
        got = [lax.ppermute(held[0], axes, right)]
        offsets.append(-hop)
        if hop < lanes // 2:
            got.append(lax.ppermute(held[1], axes, left))
            offsets.append(hop)
        parts += got
        held = got
    return parts, offsets, values


def through_experts(plan, info, received, take_in, matrices):
    packed, target, needed = compact(plan, info, received)
    beside = [weights_table(plan, received, target), spread_table(plan, target), take_in]
    parts, offsets, beside = gather_lanes(packed, plan.lanes, beside)
    weights, take_out, take_in = beside
    partial = experts(plan, offsets, info, parts, weights, *matrices)
    returned = lax.all_to_all(partial, "tp", 0, 0, tiled=True)
    back = lax.all_to_all(spread(plan, take_out, needed, returned), "ep", 0, 0, tiled=True)
    return combine(plan, take_in, back)


def on_device(
    tokens, device_choice, local_expert, route_weight, prefill_ranks, w_gate, w_up, w_down
):
    ranks, prefill = lax.axis_size("ep"), prefill_ranks.shape[0]
    sizes = (ranks, lax.axis_size("tp"), *tokens.shape, prefill)
    most = (ranks - prefill) * DEC_RANK
    plan, whole = Plan(*sizes, min(USUAL_DECODE, most)), Plan(*sizes, most)
    stay = [prefill_ranks, device_choice.T, local_expert.T, route_weight.T, tokens]
    stay = [pltpu.with_memory_space_constraint(x, pltpu.HBM) for x in stay]
    outgoing = pack(plan, *stay)
    received = lax.all_to_all(outgoing, "ep", 0, 0, tiled=True)
    received, info, choice = lax.optimization_barrier((received, stay[0], stay[1]))
    take_in = combine_table(plan, info, choice)
    rest = (info, received, take_in, (w_gate, w_up, w_down))
    shares, over = through_experts(plan, *rest)
    rest, over = lax.optimization_barrier((rest, over))
    shares = lax.cond(
        over[0] > 0, lambda: through_experts(whole, *rest)[0], lambda: shares
    )
    shares = lax.all_to_all(shares, "tp", 0, 0, tiled=True)
    return finish(plan, shares)


def solution(mesh):
    in_specs = (
        P(("groups", "ep"), None),
        P(("groups", "ep"), None),
        P(("groups", "ep"), None),
        P(("groups", "ep"), None),
        P("groups"),
        P("ep", "tp", None),
        P("ep", "tp", None),
        P("ep", "tp", None),
    )
    out_specs = P(("groups", "ep", "tp"), None)
    return jax.shard_map(
        on_device, mesh=mesh, in_specs=in_specs, out_specs=out_specs, check_vma=False
    )
```

```python
import jax
import jax.numpy as jnp
from jax import lax
from jax.experimental import pallas as pl
from jax.experimental.pallas import tpu as pltpu
from jax.sharding import PartitionSpec as P

TOPK = 6
DEV_TOP = 3
DEC_RANK = 8
USUAL_DECODE = 32
LANE = 128
F32, BF16, I32 = jnp.float32, jnp.bfloat16, jnp.int32
INTERPRET = False


class Plan:
    def __init__(self, ranks, lanes, rows, width, prefill, decode):
        self.ranks, self.lanes, self.rows, self.width = ranks, lanes, rows, width
        self.cap = (DEV_TOP * rows + ranks - 1) // ranks
        self.prefill, self.decode = prefill, decode
        self.half_pre = self.cap // 2
        self.half_dec = DEC_RANK // 2
        self.half = prefill * self.half_pre + decode // 2
        self.slots = 2 * self.half
        self.packed = 5 * self.half
        self.packed_up = -(-self.packed // LANE) * LANE
        self.chunk = 2 * self.cap + self.half_pre + 2
        self.own_rows = rows // lanes
        assert width == (2 * lanes + lanes // 2) * LANE and self.chunk % 8 == 0
        assert rows == LANE and self.half_dec <= self.cap - DEC_RANK and ranks <= LANE


class Info:
    def __init__(self, pre_ref):
        self.places, self.pre_ref = (lax.axis_index("tp"), lax.axis_index("ep")), pre_ref

    def __getitem__(self, i):
        return self.places[i] if i < 2 else self.pre_ref[i - 2]


def iota(shape, dim):
    return lax.broadcasted_iota(I32, shape, dim)


def one_hot(mask):
    return jnp.where(mask, 1.0, 0.0).astype(BF16)


def dot(a, b):
    return jnp.dot(a, b, preferred_element_type=F32)


def is_prefill(info_ref, plan, own):
    found = info_ref[2] == own
    for i in range(1, plan.prefill):
        found = found | (info_ref[2 + i] == own)
    return found


def earlier(plan):
    shape = (plan.rows, plan.rows)
    return one_hot(iota(shape, 0) < iota(shape, 1))


def chunk_index(j, plan, parity, full):
    cap = plan.cap
    spill = (j >= DEC_RANK) & (j < cap) & jnp.logical_not(full)
    last = j >= 2 * cap
    block = jnp.where(last | spill, 2, jnp.where(j < cap, 0, 1))
    start = jnp.where(full, parity * plan.half_pre, 0)
    slot = jnp.where(
        spill, j - DEC_RANK + plan.half_dec, jnp.where(last, j - 2 * cap + start, j - block * cap)
    )
    kept = jnp.logical_not(last) | (j - 2 * cap < jnp.where(full, plan.half_pre, plan.half_dec))
    return jnp.where(kept, block, 3), slot


def named_ranks(plan, full, choice_ref):
    shape = (plan.ranks, plan.rows)
    live = iota(shape, 1) < jnp.where(full, plan.rows, DEC_RANK)
    rank = iota(shape, 0)
    hits = [(choice_ref[k : k + 1, :] == rank) & live for k in range(DEV_TOP)]
    named = sum(jnp.where(hit, 1.0, 0.0) for hit in hits)
    return hits, named, places(plan, named)


def places(plan, named):
    before = dot(named.astype(BF16), earlier(plan))
    return jnp.where(named > 0.5, before, -1.0)


def pack_kernel(plan, pre_hbm, choice_hbm, le_hbm, rw_hbm, tok_ref, out_ref, *scratch):
    pre_ref, choice_ref, le_ref, rw_ref, x_ref, sems = scratch
    info_ref = Info(pre_ref)
    lane, own = info_ref[0], info_ref[1]
    first_at = pl.multiple_of(lane * (2 * LANE), LANE)
    tail_at = pl.multiple_of((2 * plan.lanes + lane // 2) * LANE, LANE)
    ends = [
        (pre_hbm, pre_ref),
        (choice_hbm, choice_ref),
        (le_hbm, le_ref),
        (rw_hbm, rw_ref),
        (tok_ref.at[:, pl.ds(first_at, 2 * LANE)], x_ref.at[:, 0 : 2 * LANE]),
        (tok_ref.at[:, pl.ds(tail_at, LANE)], x_ref.at[:, 2 * LANE : 3 * LANE]),
    ]
    copies = [pltpu.make_async_copy(a, b, sems.at[i]) for i, (a, b) in enumerate(ends)]
    for copy in copies:
        copy.start()
    for copy in copies[:4]:
        copy.wait()
    full = is_prefill(info_ref, plan, own)
    hits, named, place = named_ranks(plan, full, choice_ref)
    weights = []
    for e in range(2):
        total = jnp.zeros(named.shape, F32)
        for k, hit in enumerate(hits):
            for j in (2 * k, 2 * k + 1):
                chosen = hit & (le_ref[j : j + 1, :] == e)
                total += jnp.where(chosen, rw_ref[j : j + 1, :], 0.0)
        weights.append(total)
    full_shape = (plan.ranks, plan.chunk, LANE)
    flat = plan.ranks * plan.chunk
    j = iota(full_shape, 1)
    block, slot = chunk_index(j, plan, lane % 2, full)
    match = place.astype(I32)[:, None, :] == slot
    picks = [one_hot(match & (block == b)).reshape(flat, LANE) for b in range(3)]
    for copy in copies[4:]:
        copy.wait()
    total = sum(dot(picks[b], x_ref[:, b * LANE : (b + 1) * LANE]) for b in range(3))
    total = total.reshape(full_shape)
    total = jnp.where(j == plan.chunk - 2, weights[0][:, None, :], total)
    total = jnp.where(j == plan.chunk - 1, weights[1][:, None, :], total)
    out_ref[...] = total.astype(BF16)


def weight_rows(plan, data):
    shape = (plan.ranks, plan.ranks * plan.chunk)
    at = iota(shape, 0) * plan.chunk + plan.chunk - 2
    return [dot(one_hot(iota(shape, 1) == at + e), data) for e in range(2)]


def target_row(info_ref, plan, named):
    lane = info_ref[0]
    ranks, total = plan.ranks, plan.ranks * plan.chunk
    rank = iota((8, ranks), 1)
    fulls = jnp.zeros((8, ranks), I32)
    for i in range(plan.prefill):
        fulls += jnp.where(rank == info_ref[2 + i], 1, 0)
    ones = jnp.full((8, plan.rows), 1.0, BF16)
    counts = lax.dot_general(
        ones, named.astype(BF16), (((1,), (1,)), ((), ())), preferred_element_type=F32
    )
    decode = jnp.where(fulls > 0, 0.0, counts).astype(BF16)
    full = jnp.where(fulls > 0, 1.0, 0.0).astype(BF16)
    spread = (ranks, total)
    source = iota(spread, 1) // plan.chunk
    below = one_hot(iota(spread, 0) < source)
    here = one_hot(iota(spread, 0) == source)
    base = dot(decode, below).astype(I32)
    held = dot(decode, here).astype(I32)
    index = dot(full, below).astype(I32)
    full = dot(full, here) > 0.5
    needed = jnp.sum(decode.astype(F32), axis=1, keepdims=True)
    j = iota((8, total), 1) % plan.chunk
    block, slot = chunk_index(j, plan, lane % 2, full)
    half_rows = plan.decode // 2
    place = base + slot
    second = jnp.where(jnp.where(full, slot - plan.half_pre, place - half_rows) >= 0, 1, 0)
    row = jnp.where(
        full,
        index * plan.half_pre + slot - second * plan.half_pre,
        plan.prefill * plan.half_pre + place - second * half_rows,
    )
    kept = full | ((slot < held) & (place < plan.decode) & ((block < 2) | (second == lane % 2)))
    piece = jnp.where(block == 2, 4, 2 * block + second)
    return jnp.where(kept & (block < 3), piece * plan.half + row, -1), needed


def compact_kernel(plan, info_ref, in_ref, out_ref, target_ref, needed_ref):
    total = plan.ranks * plan.chunk
    data = in_ref[...].reshape(total, LANE)
    first = weight_rows(plan, data)[0]
    named = jnp.where(first > 0.0, 1.0, 0.0)
    target, needed = target_row(info_ref, plan, named)
    target_ref[...] = target
    needed_ref[...] = jnp.broadcast_to(needed, (8, LANE))
    for at in range(0, plan.packed, plan.half):
        take = one_hot(iota((plan.half, total), 0) + at == target[0:1, :])
        out_ref[at : at + plan.half, :] = dot(take, data).astype(BF16)


def weights_kernel(plan, in_ref, target_ref, weight_ref):
    total = plan.ranks * plan.chunk
    data = in_ref[...].reshape(total, LANE)
    first, second = weight_rows(plan, data)
    place = places(plan, jnp.where(first > 0.0, 1.0, 0.0)).astype(I32)
    full_shape = (plan.ranks, plan.chunk, LANE)
    j = iota(full_shape, 1)
    match = (place[:, None, :] == j) & (j < plan.cap)
    target = target_ref[0:1, :]
    wide = []
    for value in (first, second):
        kept = jnp.where(match, value[:, None, :], 0.0)
        column = jnp.sum(kept, axis=2, keepdims=True)
        wide.append(jnp.broadcast_to(column, full_shape).reshape(total, LANE).astype(BF16))
    for piece in range(2):
        at = piece * plan.half
        take = one_hot(iota((plan.half, total), 0) + at == target)
        for e in range(2):
            weight_ref[at : at + plan.half, e * LANE : (e + 1) * LANE] = dot(take, wide[e])


def spread_table_kernel(plan, target_ref, spread_ref):
    total = plan.ranks * plan.chunk
    col = iota((LANE, LANE), 1)
    for g in range(0, total, LANE):
        wide = jnp.broadcast_to(target_ref[0:1, g : g + LANE], (LANE, LANE))
        column = wide.astype(F32).T.astype(I32)
        for at in range(0, plan.packed_up, LANE):
            spread_ref[g : g + LANE, at : at + LANE] = one_hot(col + at == column)


def combine_table_kernel(plan, info_ref, choice_ref, combine_ref):
    lane, own = info_ref[0], info_ref[1]
    ranks, rows = plan.ranks, plan.rows
    total = ranks * plan.chunk
    full = is_prefill(info_ref, plan, own)
    _, _, place = named_ranks(plan, full, choice_ref)
    square = jnp.concatenate([place, jnp.zeros((rows - ranks, rows), F32)], axis=0)
    turned = square.T[:, :ranks].astype(BF16)
    spread = (ranks, total)
    expand = one_hot(iota(spread, 1) // plan.chunk == iota(spread, 0))
    spots = dot(turned, expand).astype(I32)
    j = iota((1, total), 1) % plan.chunk
    block, slot = chunk_index(j, plan, lane % 2, full)
    match = spots == slot
    for b in range(3):
        combine_ref[:, b * total : (b + 1) * total] = one_hot(match & (block == b))


def share_columns(plan, info_ref, offset):
    way = 1 - 2 * lax.rem(info_ref[1], 2)
    lane = lax.rem(info_ref[0] + way * offset + plan.lanes, plan.lanes)
    first = pl.multiple_of(lane * (2 * LANE), LANE)
    tail = pl.multiple_of((2 * plan.lanes + lane // 2) * LANE, LANE)
    start = pl.multiple_of(lax.rem(lane, 2) * plan.half, 8)
    return first, tail, pl.ds(start, plan.half)


TURNED = (((1,), (1,)), ((), ()))


def early_kernel(plan, offsets, late, info_ref, *refs):
    n = len(offsets)
    wg, wu, gate_ref, up_ref, x_ref = refs[n:]
    half, slots = plan.half, plan.slots
    for offset, part in zip(offsets + [late], refs[:n] + (None,)):
        first, tail, rows = share_columns(plan, info_ref, offset)
        if part is None:
            x_ref[:, pl.ds(first, 2 * LANE)] = jnp.zeros((slots, 2 * LANE), BF16)
            x_ref[rows, pl.ds(tail, LANE)] = jnp.zeros((half, LANE), BF16)
        else:
            x_ref[:, pl.ds(first, LANE)] = part[0:slots, :]
            x_ref[:, pl.ds(pl.multiple_of(first + LANE, LANE), LANE)] = part[slots : 2 * slots, :]
            x_ref[rows, pl.ds(tail, LANE)] = part[2 * slots : 2 * slots + half, :]
    x = x_ref[...]
    gate_ref[...] = lax.dot_general(x, wg[...], TURNED, preferred_element_type=F32)
    up_ref[...] = lax.dot_general(x, wu[...], TURNED, preferred_element_type=F32)


def expert_kernel(plan, late, info_ref, part, gate_ref, up_ref, weight_ref, wg, wu, wd, out_ref, x_ref, h_ref):
    lanes, half, slots = plan.lanes, plan.half, plan.slots
    first, tail, rows = share_columns(plan, info_ref, late)
    x_ref[:, 0:LANE] = part[0:slots, :]
    x_ref[:, LANE : 2 * LANE] = part[slots : 2 * slots, :]
    x_ref[:, 2 * LANE : 3 * LANE] = jnp.zeros((slots, LANE), BF16)
    x_ref[rows, 2 * LANE : 3 * LANE] = part[2 * slots : 2 * slots + half, :]
    gate, up = gate_ref[...], up_ref[...]
    for at, columns in ((0, pl.ds(first, 2 * LANE)), (2 * LANE, pl.ds(tail, LANE))):
        x = x_ref[:, at : at + columns.size]
        gate += lax.dot_general(x, wg[:, columns], TURNED, preferred_element_type=F32)
        up += lax.dot_general(x, wu[:, columns], TURNED, preferred_element_type=F32)
    hidden = gate / (1.0 + jnp.exp(-gate)) * up * weight_ref[...]
    h_ref[...] = hidden.astype(BF16)
    for lane in range(lanes):
        at = lane * 2 * LANE
        y = dot(h_ref[...], wd[:, at : at + 2 * LANE]).astype(BF16)
        out_ref[lane, 0:slots, :] = y[:, :LANE]
        out_ref[lane, slots : 2 * slots, :] = y[:, LANE:]
    for pair in range(0, lanes // 2, 2):
        at = (2 * lanes + pair) * LANE
        y = dot(h_ref[...], wd[:, at : at + 2 * LANE]).astype(BF16)
        for k in range(2):
            for p in range(2):
                piece = y[p * half : (p + 1) * half, k * LANE : (k + 1) * LANE]
                out_ref[2 * (pair + k) + p, 2 * slots : 2 * slots + half, :] = piece


def spread_kernel(plan, take_ref, needed_ref, in_ref, out_ref, sum_ref):
    total = in_ref[0].astype(F32)
    for lane in range(1, plan.lanes):
        total += in_ref[lane].astype(F32)
    sum_ref[0 : plan.packed, :] = total.astype(BF16)
    sum_ref[plan.packed :, :] = jnp.zeros((plan.packed_up - plan.packed, LANE), BF16)
    shape = (plan.ranks, plan.chunk, LANE)
    spread = dot(take_ref[...], sum_ref[...]).reshape(shape)
    over = jnp.where(needed_ref[0:1, :] > float(plan.decode), 1.0, 0.0)
    spread = jnp.where(iota(shape, 1) == plan.chunk - 1, over[None], spread)
    out_ref[...] = spread.astype(BF16)


def combine_kernel(plan, take_ref, in_ref, out_ref, over_ref):
    total = plan.ranks * plan.chunk
    data = in_ref[...].reshape(total, LANE)
    own_rows = plan.own_rows
    for b in range(3):
        mine = dot(take_ref[:, b * total : (b + 1) * total], data).astype(BF16)
        for to in range(plan.lanes):
            out_ref[to, b * own_rows : (b + 1) * own_rows, :] = mine[
                to * own_rows : (to + 1) * own_rows
            ]
    shape = (8, total)
    flags = one_hot(iota(shape, 1) % plan.chunk == plan.chunk - 1)
    over_ref[0] = jnp.where(jnp.max(dot(flags, data)) > 0.0, 1, 0)


def finish_kernel(plan, in_ref, out_ref):
    n = plan.own_rows
    for lane in range(plan.lanes):
        at = lane * 2 * LANE
        out_ref[:, at : at + LANE] = in_ref[lane, 0:n, :]
        out_ref[:, at + LANE : at + 2 * LANE] = in_ref[lane, n : 2 * n, :]
    for pair in range(plan.lanes // 2):
        at = (2 * plan.lanes + pair) * LANE
        first = in_ref[2 * pair, 2 * n : 3 * n, :].astype(F32)
        second = in_ref[2 * pair + 1, 2 * n : 3 * n, :].astype(F32)
        out_ref[:, at : at + LANE] = (first + second).astype(BF16)


SMEM = pl.BlockSpec(memory_space=pltpu.SMEM)
VMEM = pl.BlockSpec(memory_space=pltpu.VMEM)
HBM = pl.BlockSpec(memory_space=pltpu.HBM)

def call(kernel, name, out, specs, *args, scratch=(), limit=24 << 20, flops=0):
    cost = None
    if flops:
        cost = pl.CostEstimate(flops=flops, bytes_accessed=1 << 20, transcendentals=0)
    return pl.pallas_call(
        kernel,
        out_shape=out,
        in_specs=specs,
        out_specs=jax.tree.map(lambda o: SMEM if o.shape == (1,) else VMEM, out),
        scratch_shapes=scratch,
        compiler_params=pltpu.CompilerParams(vmem_limit_bytes=limit),
        cost_estimate=cost,
        interpret=INTERPRET,
        name=name,
    )(*args)


def pack(plan, prefill_ranks, choice, local, weights, tokens):
    return call(
        lambda *refs: pack_kernel(plan, *refs),
        "pack",
        jax.ShapeDtypeStruct((plan.ranks, plan.chunk, LANE), BF16),
        [HBM] * 5,
        prefill_ranks,
        choice,
        local,
        weights,
        tokens,
        scratch=[
            pltpu.SMEM(prefill_ranks.shape, I32),
            pltpu.VMEM(choice.shape, I32),
            pltpu.VMEM(local.shape, I32),
            pltpu.VMEM(weights.shape, F32),
            pltpu.VMEM((plan.rows, 3 * LANE), BF16),
            pltpu.SemaphoreType.DMA((6,)),
        ],
    )


def compact(plan, info, received):
    return call(
        lambda *refs: compact_kernel(plan, Info(refs[0]), *refs[1:]),
        "compact",
        (
            jax.ShapeDtypeStruct((plan.packed, LANE), BF16),
            jax.ShapeDtypeStruct((8, plan.ranks * plan.chunk), I32),
            jax.ShapeDtypeStruct((8, LANE), F32),
        ),
        [SMEM, VMEM],
        info,
        received,
    )


def weights_table(plan, received, target):
    return call(
        lambda *refs: weights_kernel(plan, *refs),
        "weights",
        jax.ShapeDtypeStruct((plan.slots, 2 * LANE), F32),
        [VMEM, VMEM],
        received,
        target,
        flops=1 << 29,
    )


def spread_table(plan, target):
    return call(
        lambda *refs: spread_table_kernel(plan, *refs),
        "spread_table",
        jax.ShapeDtypeStruct((plan.ranks * plan.chunk, plan.packed_up), BF16),
        [VMEM],
        target,
        flops=1 << 29,
    )


def combine_table(plan, info, choice):
    return call(
        lambda *refs: combine_table_kernel(plan, Info(refs[0]), *refs[1:]),
        "combine_table",
        jax.ShapeDtypeStruct((plan.rows, 3 * plan.ranks * plan.chunk), BF16),
        [SMEM, VMEM],
        info,
        choice,
        flops=1 << 29,
    )


def experts(plan, offsets, info, parts, weights, w_gate, w_up, w_down):
    hidden = w_gate.shape[0] * w_gate.shape[1]
    w_gate, w_up, w_down = [w.reshape(hidden, plan.width) for w in (w_gate, w_up, w_down)]
    late = offsets[-1]
    product = jax.ShapeDtypeStruct((plan.slots, hidden), F32)
    gate, up = call(
        lambda *refs: early_kernel(plan, offsets[:-1], late, Info(refs[0]), *refs[1:]),
        "early",
        (product, product),
        [SMEM] + [VMEM] * (len(parts) + 1),
        info,
        *parts[:-1],
        w_gate,
        w_up,
        scratch=[pltpu.VMEM((plan.slots, plan.width), BF16)],
        flops=1 << 29,
    )
    return call(
        lambda *refs: expert_kernel(plan, late, Info(refs[0]), *refs[1:]),
        "experts",
        jax.ShapeDtypeStruct((plan.lanes, plan.packed, LANE), BF16),
        [SMEM] + [VMEM] * 7,
        info,
        parts[-1],
        gate,
        up,
        weights,
        w_gate,
        w_up,
        w_down,
        scratch=[
            pltpu.VMEM((plan.slots, 3 * LANE), BF16),
            pltpu.VMEM((plan.slots, hidden), BF16),
        ],
    )


def spread(plan, take, needed, returned):
    return call(
        lambda *refs: spread_kernel(plan, *refs),
        "spread",
        jax.ShapeDtypeStruct((plan.ranks, plan.chunk, LANE), BF16),
        [VMEM] * 3,
        take,
        needed,
        returned,
        scratch=[pltpu.VMEM((plan.packed_up, LANE), BF16)],
    )


def combine(plan, take, back):
    return call(
        lambda *refs: combine_kernel(plan, *refs),
        "combine",
        (
            jax.ShapeDtypeStruct((plan.lanes, 3 * plan.own_rows, LANE), BF16),
            jax.ShapeDtypeStruct((1,), I32),
        ),
        [VMEM, VMEM],
        take,
        back,
    )


def finish(plan, shares):
    return call(
        lambda *refs: finish_kernel(plan, *refs),
        "finish",
        jax.ShapeDtypeStruct((plan.own_rows, plan.width), BF16),
        [VMEM],
        shares,
    )


def gather_lanes(packed, lanes, beside):
    ranks = lax.axis_size("ep")
    ways = []
    for way in (1, -1):
        steps = [way if rank % 2 == 0 else -way for rank in range(ranks)]
        ways.append(
            [
                (rank * lanes + i, rank * lanes + (i + steps[rank]) % lanes)
                for rank in range(ranks)
                for i in range(lanes)
            ]
        )
    right, left = ways
    axes = ("ep", "tp")
    parts, offsets, values = [packed], [0], []
    held = [packed, packed]
    for hop in range(1, lanes // 2 + 1):
        if hop > 1 and hop - 2 < len(beside):
            first, value = lax.optimization_barrier((held[0], beside[hop - 2]))
            held = [first, held[1]]
            values.append(value)
        got = [lax.ppermute(held[0], axes, right)]
        offsets.append(-hop)
        if hop < lanes // 2:
            got.append(lax.ppermute(held[1], axes, left))
            offsets.append(hop)
        parts += got
        held = got
    return parts, offsets, values


def through_experts(plan, info, received, take_in, matrices):
    packed, target, needed = compact(plan, info, received)
    beside = [weights_table(plan, received, target), spread_table(plan, target), take_in]
    parts, offsets, beside = gather_lanes(packed, plan.lanes, beside)
    weights, take_out, take_in = beside
    partial = experts(plan, offsets, info, parts, weights, *matrices)
    returned = lax.all_to_all(partial, "tp", 0, 0, tiled=True)
    back = lax.all_to_all(spread(plan, take_out, needed, returned), "ep", 0, 0, tiled=True)
    return combine(plan, take_in, back)


def on_device(
    tokens, device_choice, local_expert, route_weight, prefill_ranks, w_gate, w_up, w_down
):
    ranks, prefill = lax.axis_size("ep"), prefill_ranks.shape[0]
    sizes = (ranks, lax.axis_size("tp"), *tokens.shape, prefill)
    most = (ranks - prefill) * DEC_RANK
    plan, whole = Plan(*sizes, min(USUAL_DECODE, most)), Plan(*sizes, most)
    stay = [prefill_ranks, device_choice.T, local_expert.T, route_weight.T, tokens]
    stay = [pltpu.with_memory_space_constraint(x, pltpu.HBM) for x in stay]
    outgoing = pack(plan, *stay)
    received = lax.all_to_all(outgoing, "ep", 0, 0, tiled=True)
    received, info, choice = lax.optimization_barrier((received, stay[0], stay[1]))
    take_in = combine_table(plan, info, choice)
    rest = (info, received, take_in, (w_gate, w_up, w_down))
    shares, over = through_experts(plan, *rest)
    rest, over = lax.optimization_barrier((rest, over))
    shares = lax.cond(
        over[0] > 0, lambda: through_experts(whole, *rest)[0], lambda: shares
    )
    shares = lax.all_to_all(shares, "tp", 0, 0, tiled=True)
    return finish(plan, shares)


def solution(mesh):
    in_specs = (
        P(("groups", "ep"), None),
        P(("groups", "ep"), None),
        P(("groups", "ep"), None),
        P(("groups", "ep"), None),
        P("groups"),
        P("ep", "tp", None),
        P("ep", "tp", None),
        P("ep", "tp", None),
    )
    out_specs = P(("groups", "ep", "tp"), None)
    return jax.shard_map(
        on_device, mesh=mesh, in_specs=in_specs, out_specs=out_specs, check_vma=False
    )
```

```python
import jax
import jax.numpy as jnp
from jax import lax
from jax.experimental import pallas as pl
from jax.experimental.pallas import tpu as pltpu
from jax.sharding import PartitionSpec as P

TOPK = 6
DEV_TOP = 3
DEC_RANK = 8
USUAL_DECODE = 32
LANE = 128
F32, BF16, I32 = jnp.float32, jnp.bfloat16, jnp.int32
INTERPRET = False


class Plan:
    def __init__(self, ranks, lanes, rows, width, prefill, decode):
        self.ranks, self.lanes, self.rows, self.width = ranks, lanes, rows, width
        self.cap = (DEV_TOP * rows + ranks - 1) // ranks
        self.prefill, self.decode = prefill, decode
        self.half_pre = self.cap // 2
        self.half_dec = DEC_RANK // 2
        self.half = prefill * self.half_pre + decode // 2
        self.slots = 2 * self.half
        self.packed = 5 * self.half
        self.packed_up = -(-self.packed // LANE) * LANE
        self.chunk = 2 * self.cap + self.half_pre + 2
        self.own_rows = rows // lanes
        assert width == (2 * lanes + lanes // 2) * LANE and self.chunk % 8 == 0
        assert rows == LANE and self.half_dec <= self.cap - DEC_RANK and ranks <= LANE


class Info:
    def __init__(self, pre_ref):
        self.places, self.pre_ref = (lax.axis_index("tp"), lax.axis_index("ep")), pre_ref

    def __getitem__(self, i):
        return self.places[i] if i < 2 else self.pre_ref[i - 2]


def iota(shape, dim):
    return lax.broadcasted_iota(I32, shape, dim)


def one_hot(mask):
    return jnp.where(mask, 1.0, 0.0).astype(BF16)


def dot(a, b):
    return jnp.dot(a, b, preferred_element_type=F32)


def is_prefill(info_ref, plan, own):
    found = info_ref[2] == own
    for i in range(1, plan.prefill):
        found = found | (info_ref[2 + i] == own)
    return found


def earlier(plan):
    shape = (plan.rows, plan.rows)
    return one_hot(iota(shape, 0) < iota(shape, 1))


def chunk_index(j, plan, parity, full):
    cap = plan.cap
    spill = (j >= DEC_RANK) & (j < cap) & jnp.logical_not(full)
    last = j >= 2 * cap
    block = jnp.where(last | spill, 2, jnp.where(j < cap, 0, 1))
    start = jnp.where(full, parity * plan.half_pre, 0)
    slot = jnp.where(
        spill, j - DEC_RANK + plan.half_dec, jnp.where(last, j - 2 * cap + start, j - block * cap)
    )
    kept = jnp.logical_not(last) | (j - 2 * cap < jnp.where(full, plan.half_pre, plan.half_dec))
    return jnp.where(kept, block, 3), slot


def named_ranks(plan, full, choice_ref):
    shape = (plan.ranks, plan.rows)
    live = iota(shape, 1) < jnp.where(full, plan.rows, DEC_RANK)
    rank = iota(shape, 0)
    hits = [(choice_ref[k : k + 1, :] == rank) & live for k in range(DEV_TOP)]
    named = sum(jnp.where(hit, 1.0, 0.0) for hit in hits)
    return hits, named, places(plan, named)


def places(plan, named):
    before = dot(named.astype(BF16), earlier(plan))
    return jnp.where(named > 0.5, before, -1.0)


def pack_kernel(plan, pre_hbm, choice_hbm, le_hbm, rw_hbm, tok_ref, out_ref, *scratch):
    pre_ref, choice_ref, le_ref, rw_ref, x_ref, sems = scratch
    info_ref = Info(pre_ref)
    lane, own = info_ref[0], info_ref[1]
    first_at = pl.multiple_of(lane * (2 * LANE), LANE)
    tail_at = pl.multiple_of((2 * plan.lanes + lane // 2) * LANE, LANE)
    ends = [
        (pre_hbm, pre_ref),
        (choice_hbm, choice_ref),
        (le_hbm, le_ref),
        (rw_hbm, rw_ref),
        (tok_ref.at[:, pl.ds(first_at, 2 * LANE)], x_ref.at[:, 0 : 2 * LANE]),
        (tok_ref.at[:, pl.ds(tail_at, LANE)], x_ref.at[:, 2 * LANE : 3 * LANE]),
    ]
    copies = [pltpu.make_async_copy(a, b, sems.at[i]) for i, (a, b) in enumerate(ends)]
    for copy in copies:
        copy.start()
    for copy in copies[:4]:
        copy.wait()
    full = is_prefill(info_ref, plan, own)
    hits, named, place = named_ranks(plan, full, choice_ref)
    weights = []
    for e in range(2):
        total = jnp.zeros(named.shape, F32)
        for k, hit in enumerate(hits):
            for j in (2 * k, 2 * k + 1):
                chosen = hit & (le_ref[j : j + 1, :] == e)
                total += jnp.where(chosen, rw_ref[j : j + 1, :], 0.0)
        weights.append(total)
    full_shape = (plan.ranks, plan.chunk, LANE)
    flat = plan.ranks * plan.chunk
    j = iota(full_shape, 1)
    block, slot = chunk_index(j, plan, lane % 2, full)
    match = place.astype(I32)[:, None, :] == slot
    picks = [one_hot(match & (block == b)).reshape(flat, LANE) for b in range(3)]
    for copy in copies[4:]:
        copy.wait()
    total = sum(dot(picks[b], x_ref[:, b * LANE : (b + 1) * LANE]) for b in range(3))
    total = total.reshape(full_shape)
    total = jnp.where(j == plan.chunk - 2, weights[0][:, None, :], total)
    total = jnp.where(j == plan.chunk - 1, weights[1][:, None, :], total)
    out_ref[...] = total.astype(BF16)


def weight_rows(plan, data):
    shape = (plan.ranks, plan.ranks * plan.chunk)
    at = iota(shape, 0) * plan.chunk + plan.chunk - 2
    return [dot(one_hot(iota(shape, 1) == at + e), data) for e in range(2)]


def target_row(info_ref, plan, named):
    lane = info_ref[0]
    ranks, total = plan.ranks, plan.ranks * plan.chunk
    rank = iota((8, ranks), 1)
    fulls = jnp.zeros((8, ranks), I32)
    for i in range(plan.prefill):
        fulls += jnp.where(rank == info_ref[2 + i], 1, 0)
    ones = jnp.full((8, plan.rows), 1.0, BF16)
    counts = lax.dot_general(
        ones, named.astype(BF16), (((1,), (1,)), ((), ())), preferred_element_type=F32
    )
    decode = jnp.where(fulls > 0, 0.0, counts).astype(BF16)
    full = jnp.where(fulls > 0, 1.0, 0.0).astype(BF16)
    spread = (ranks, total)
    source = iota(spread, 1) // plan.chunk
    below = one_hot(iota(spread, 0) < source)
    here = one_hot(iota(spread, 0) == source)
    base = dot(decode, below).astype(I32)
    held = dot(decode, here).astype(I32)
    index = dot(full, below).astype(I32)
    full = dot(full, here) > 0.5
    needed = jnp.sum(decode.astype(F32), axis=1, keepdims=True)
    j = iota((8, total), 1) % plan.chunk
    block, slot = chunk_index(j, plan, lane % 2, full)
    half_rows = plan.decode // 2
    place = base + slot
    second = jnp.where(jnp.where(full, slot - plan.half_pre, place - half_rows) >= 0, 1, 0)
    row = jnp.where(
        full,
        index * plan.half_pre + slot - second * plan.half_pre,
        plan.prefill * plan.half_pre + place - second * half_rows,
    )
    kept = full | ((slot < held) & (place < plan.decode) & ((block < 2) | (second == lane % 2)))
    piece = jnp.where(block == 2, 4, 2 * block + second)
    return jnp.where(kept & (block < 3), piece * plan.half + row, -1), needed


def compact_kernel(plan, info_ref, in_ref, out_ref, target_ref, needed_ref):
    total = plan.ranks * plan.chunk
    data = in_ref[...].reshape(total, LANE)
    first = weight_rows(plan, data)[0]
    named = jnp.where(first > 0.0, 1.0, 0.0)
    target, needed = target_row(info_ref, plan, named)
    target_ref[...] = target
    needed_ref[...] = jnp.broadcast_to(needed, (8, LANE))
    for at in range(0, plan.packed, plan.half):
        take = one_hot(iota((plan.half, total), 0) + at == target[0:1, :])
        out_ref[at : at + plan.half, :] = dot(take, data).astype(BF16)


def weights_kernel(plan, in_ref, target_ref, weight_ref):
    total = plan.ranks * plan.chunk
    data = in_ref[...].reshape(total, LANE)
    first, second = weight_rows(plan, data)
    place = places(plan, jnp.where(first > 0.0, 1.0, 0.0)).astype(I32)
    full_shape = (plan.ranks, plan.chunk, LANE)
    j = iota(full_shape, 1)
    match = (place[:, None, :] == j) & (j < plan.cap)
    target = target_ref[0:1, :]
    wide = []
    for value in (first, second):
        kept = jnp.where(match, value[:, None, :], 0.0)
        column = jnp.sum(kept, axis=2, keepdims=True)
        wide.append(jnp.broadcast_to(column, full_shape).reshape(total, LANE).astype(BF16))
    for piece in range(2):
        at = piece * plan.half
        take = one_hot(iota((plan.half, total), 0) + at == target)
        for e in range(2):
            weight_ref[at : at + plan.half, e * LANE : (e + 1) * LANE] = dot(take, wide[e])


def spread_table_kernel(plan, target_ref, spread_ref):
    total = plan.ranks * plan.chunk
    col = iota((LANE, LANE), 1)
    for g in range(0, total, LANE):
        wide = jnp.broadcast_to(target_ref[0:1, g : g + LANE], (LANE, LANE))
        column = wide.astype(F32).T.astype(I32)
        for at in range(0, plan.packed_up, LANE):
            spread_ref[g : g + LANE, at : at + LANE] = one_hot(col + at == column)


def combine_table_kernel(plan, info_ref, choice_ref, combine_ref):
    lane, own = info_ref[0], info_ref[1]
    ranks, rows = plan.ranks, plan.rows
    total = ranks * plan.chunk
    full = is_prefill(info_ref, plan, own)
    _, _, place = named_ranks(plan, full, choice_ref)
    square = jnp.concatenate([place, jnp.zeros((rows - ranks, rows), F32)], axis=0)
    turned = square.T[:, :ranks].astype(BF16)
    spread = (ranks, total)
    expand = one_hot(iota(spread, 1) // plan.chunk == iota(spread, 0))
    spots = dot(turned, expand).astype(I32)
    j = iota((1, total), 1) % plan.chunk
    block, slot = chunk_index(j, plan, lane % 2, full)
    match = spots == slot
    for b in range(3):
        combine_ref[:, b * total : (b + 1) * total] = one_hot(match & (block == b))


def expert_kernel(plan, offsets, info_ref, *refs):
    n = len(offsets)
    weight_ref, wg, wu, wd, out_ref, x_ref, h_ref = refs[n:]
    me, way = info_ref[0], 1 - 2 * lax.rem(info_ref[1], 2)
    lanes, half, slots = plan.lanes, plan.half, plan.slots
    for offset, part in zip(offsets, refs):
        lane = lax.rem(me + way * offset + lanes, lanes)
        first = pl.multiple_of(lane * (2 * LANE), LANE)
        tail = pl.multiple_of((2 * lanes + lane // 2) * LANE, LANE)
        start = pl.multiple_of(lax.rem(lane, 2) * half, 8)
        x_ref[:, pl.ds(first, LANE)] = part[0:slots, :]
        x_ref[:, pl.ds(pl.multiple_of(first + LANE, LANE), LANE)] = part[slots : 2 * slots, :]
        x_ref[pl.ds(start, half), pl.ds(tail, LANE)] = part[2 * slots : 2 * slots + half, :]
    turned = (((1,), (1,)), ((), ()))
    x = x_ref[...]
    gate = lax.dot_general(x, wg[...], turned, preferred_element_type=F32)
    up = lax.dot_general(x, wu[...], turned, preferred_element_type=F32)
    hidden = gate / (1.0 + jnp.exp(-gate)) * up * weight_ref[...]
    h_ref[...] = hidden.astype(BF16)
    for lane in range(lanes):
        at = lane * 2 * LANE
        y = dot(h_ref[...], wd[:, at : at + 2 * LANE]).astype(BF16)
        out_ref[lane, 0:slots, :] = y[:, :LANE]
        out_ref[lane, slots : 2 * slots, :] = y[:, LANE:]
    for pair in range(0, lanes // 2, 2):
        at = (2 * lanes + pair) * LANE
        y = dot(h_ref[...], wd[:, at : at + 2 * LANE]).astype(BF16)
        for k in range(2):
            for p in range(2):
                piece = y[p * half : (p + 1) * half, k * LANE : (k + 1) * LANE]
                out_ref[2 * (pair + k) + p, 2 * slots : 2 * slots + half, :] = piece


def spread_kernel(plan, take_ref, needed_ref, in_ref, out_ref, sum_ref):
    total = in_ref[0].astype(F32)
    for lane in range(1, plan.lanes):
        total += in_ref[lane].astype(F32)
    sum_ref[0 : plan.packed, :] = total.astype(BF16)
    sum_ref[plan.packed :, :] = jnp.zeros((plan.packed_up - plan.packed, LANE), BF16)
    shape = (plan.ranks, plan.chunk, LANE)
    spread = dot(take_ref[...], sum_ref[...]).reshape(shape)
    over = jnp.where(needed_ref[0:1, :] > float(plan.decode), 1.0, 0.0)
    spread = jnp.where(iota(shape, 1) == plan.chunk - 1, over[None], spread)
    out_ref[...] = spread.astype(BF16)


def combine_kernel(plan, take_ref, in_ref, out_ref, over_ref):
    total = plan.ranks * plan.chunk
    data = in_ref[...].reshape(total, LANE)
    own_rows = plan.own_rows
    for b in range(3):
        mine = dot(take_ref[:, b * total : (b + 1) * total], data).astype(BF16)
        for to in range(plan.lanes):
            out_ref[to, b * own_rows : (b + 1) * own_rows, :] = mine[
                to * own_rows : (to + 1) * own_rows
            ]
    shape = (8, total)
    flags = one_hot(iota(shape, 1) % plan.chunk == plan.chunk - 1)
    over_ref[0] = jnp.where(jnp.max(dot(flags, data)) > 0.0, 1, 0)


def finish_kernel(plan, in_ref, out_ref):
    n = plan.own_rows
    for lane in range(plan.lanes):
        at = lane * 2 * LANE
        out_ref[:, at : at + LANE] = in_ref[lane, 0:n, :]
        out_ref[:, at + LANE : at + 2 * LANE] = in_ref[lane, n : 2 * n, :]
    for pair in range(plan.lanes // 2):
        at = (2 * plan.lanes + pair) * LANE
        first = in_ref[2 * pair, 2 * n : 3 * n, :].astype(F32)
        second = in_ref[2 * pair + 1, 2 * n : 3 * n, :].astype(F32)
        out_ref[:, at : at + LANE] = (first + second).astype(BF16)


SMEM = pl.BlockSpec(memory_space=pltpu.SMEM)
VMEM = pl.BlockSpec(memory_space=pltpu.VMEM)
HBM = pl.BlockSpec(memory_space=pltpu.HBM)

def call(kernel, name, out, specs, *args, scratch=(), limit=24 << 20, flops=0):
    cost = None
    if flops:
        cost = pl.CostEstimate(flops=flops, bytes_accessed=1 << 20, transcendentals=0)
    return pl.pallas_call(
        kernel,
        out_shape=out,
        in_specs=specs,
        out_specs=jax.tree.map(lambda o: SMEM if o.shape == (1,) else VMEM, out),
        scratch_shapes=scratch,
        compiler_params=pltpu.CompilerParams(vmem_limit_bytes=limit),
        cost_estimate=cost,
        interpret=INTERPRET,
        name=name,
    )(*args)


def pack(plan, prefill_ranks, choice, local, weights, tokens):
    return call(
        lambda *refs: pack_kernel(plan, *refs),
        "pack",
        jax.ShapeDtypeStruct((plan.ranks, plan.chunk, LANE), BF16),
        [HBM] * 5,
        prefill_ranks,
        choice,
        local,
        weights,
        tokens,
        scratch=[
            pltpu.SMEM(prefill_ranks.shape, I32),
            pltpu.VMEM(choice.shape, I32),
            pltpu.VMEM(local.shape, I32),
            pltpu.VMEM(weights.shape, F32),
            pltpu.VMEM((plan.rows, 3 * LANE), BF16),
            pltpu.SemaphoreType.DMA((6,)),
        ],
    )


def compact(plan, info, received):
    return call(
        lambda *refs: compact_kernel(plan, Info(refs[0]), *refs[1:]),
        "compact",
        (
            jax.ShapeDtypeStruct((plan.packed, LANE), BF16),
            jax.ShapeDtypeStruct((8, plan.ranks * plan.chunk), I32),
            jax.ShapeDtypeStruct((8, LANE), F32),
        ),
        [SMEM, VMEM],
        info,
        received,
    )


def weights_table(plan, received, target):
    return call(
        lambda *refs: weights_kernel(plan, *refs),
        "weights",
        jax.ShapeDtypeStruct((plan.slots, 2 * LANE), F32),
        [VMEM, VMEM],
        received,
        target,
        flops=1 << 29,
    )


def spread_table(plan, target):
    return call(
        lambda *refs: spread_table_kernel(plan, *refs),
        "spread_table",
        jax.ShapeDtypeStruct((plan.ranks * plan.chunk, plan.packed_up), BF16),
        [VMEM],
        target,
        flops=1 << 29,
    )


def combine_table(plan, info, choice):
    return call(
        lambda *refs: combine_table_kernel(plan, Info(refs[0]), *refs[1:]),
        "combine_table",
        jax.ShapeDtypeStruct((plan.rows, 3 * plan.ranks * plan.chunk), BF16),
        [SMEM, VMEM],
        info,
        choice,
        flops=1 << 29,
    )


def experts(plan, offsets, info, parts, weights, w_gate, w_up, w_down):
    hidden = w_gate.shape[0] * w_gate.shape[1]
    flat = [w.reshape(hidden, plan.width) for w in (w_gate, w_up, w_down)]
    return call(
        lambda *refs: expert_kernel(plan, offsets, Info(refs[0]), *refs[1:]),
        "experts",
        jax.ShapeDtypeStruct((plan.lanes, plan.packed, LANE), BF16),
        [SMEM] + [VMEM] * (len(parts) + 4),
        info,
        *parts,
        weights,
        *flat,
        scratch=[
            pltpu.VMEM((plan.slots, plan.width), BF16),
            pltpu.VMEM((plan.slots, hidden), BF16),
        ],
        limit=32 << 20,
    )


def spread(plan, take, needed, returned):
    return call(
        lambda *refs: spread_kernel(plan, *refs),
        "spread",
        jax.ShapeDtypeStruct((plan.ranks, plan.chunk, LANE), BF16),
        [VMEM] * 3,
        take,
        needed,
        returned,
        scratch=[pltpu.VMEM((plan.packed_up, LANE), BF16)],
    )


def combine(plan, take, back):
    return call(
        lambda *refs: combine_kernel(plan, *refs),
        "combine",
        (
            jax.ShapeDtypeStruct((plan.lanes, 3 * plan.own_rows, LANE), BF16),
            jax.ShapeDtypeStruct((1,), I32),
        ),
        [VMEM, VMEM],
        take,
        back,
    )


def finish(plan, shares):
    return call(
        lambda *refs: finish_kernel(plan, *refs),
        "finish",
        jax.ShapeDtypeStruct((plan.own_rows, plan.width), BF16),
        [VMEM],
        shares,
    )


def gather_lanes(packed, lanes, beside):
    ranks = lax.axis_size("ep")
    pairs = [
        (rank * lanes + i, rank * lanes + (i + 1 - 2 * (rank % 2)) % lanes)
        for rank in range(ranks)
        for i in range(lanes)
    ]
    parts, values = [packed], []
    for hop in range(lanes - 1):
        held = parts[-1]
        if 0 < hop <= len(beside):
            held, value = lax.optimization_barrier((held, beside[hop - 1]))
            values.append(value)
        parts.append(lax.ppermute(held, ("ep", "tp"), pairs))
    return parts, [-hop for hop in range(lanes)], values


def through_experts(plan, info, received, take_in, matrices):
    packed, target, needed = compact(plan, info, received)
    beside = [weights_table(plan, received, target), spread_table(plan, target), take_in]
    parts, offsets, beside = gather_lanes(packed, plan.lanes, beside)
    weights, take_out, take_in = beside
    partial = experts(plan, offsets, info, parts, weights, *matrices)
    returned = lax.all_to_all(partial, "tp", 0, 0, tiled=True)
    back = lax.all_to_all(spread(plan, take_out, needed, returned), "ep", 0, 0, tiled=True)
    return combine(plan, take_in, back)


def on_device(
    tokens, device_choice, local_expert, route_weight, prefill_ranks, w_gate, w_up, w_down
):
    ranks, prefill = lax.axis_size("ep"), prefill_ranks.shape[0]
    sizes = (ranks, lax.axis_size("tp"), *tokens.shape, prefill)
    most = (ranks - prefill) * DEC_RANK
    plan, whole = Plan(*sizes, min(USUAL_DECODE, most)), Plan(*sizes, most)
    stay = [prefill_ranks, device_choice.T, local_expert.T, route_weight.T, tokens]
    stay = [pltpu.with_memory_space_constraint(x, pltpu.HBM) for x in stay]
    outgoing = pack(plan, *stay)
    received = lax.all_to_all(outgoing, "ep", 0, 0, tiled=True)
    received, info, choice = lax.optimization_barrier((received, stay[0], stay[1]))
    take_in = combine_table(plan, info, choice)
    rest = (info, received, take_in, (w_gate, w_up, w_down))
    shares, over = through_experts(plan, *rest)
    rest, over = lax.optimization_barrier((rest, over))
    shares = lax.cond(
        over[0] > 0, lambda: through_experts(whole, *rest)[0], lambda: shares
    )
    shares = lax.all_to_all(shares, "tp", 0, 0, tiled=True)
    return finish(plan, shares)


def solution(mesh):
    in_specs = (
        P(("groups", "ep"), None),
        P(("groups", "ep"), None),
        P(("groups", "ep"), None),
        P(("groups", "ep"), None),
        P("groups"),
        P("ep", "tp", None),
        P("ep", "tp", None),
        P("ep", "tp", None),
    )
    out_specs = P(("groups", "ep", "tp"), None)
    return jax.shard_map(
        on_device, mesh=mesh, in_specs=in_specs, out_specs=out_specs, check_vma=False
    )
```

```python
import jax
import jax.numpy as jnp
from jax import lax
from jax.experimental import pallas as pl
from jax.experimental.pallas import tpu as pltpu
from jax.sharding import PartitionSpec as P

TOPK = 6
DEV_TOP = 3
DEC_RANK = 8
USUAL_DECODE = 32
LANE = 128
F32, BF16, I32 = jnp.float32, jnp.bfloat16, jnp.int32
INTERPRET = False


class Plan:
    def __init__(self, ranks, lanes, rows, width, prefill, decode):
        self.ranks, self.lanes, self.rows, self.width = ranks, lanes, rows, width
        self.cap = (DEV_TOP * rows + ranks - 1) // ranks
        self.prefill, self.decode = prefill, decode
        self.half_pre = self.cap // 2
        self.half_dec = DEC_RANK // 2
        self.half = prefill * self.half_pre + decode // 2
        self.slots = 2 * self.half
        self.packed = 5 * self.half
        self.packed_up = -(-self.packed // LANE) * LANE
        self.chunk = 2 * self.cap + self.half_pre + 2
        self.own_rows = rows // lanes
        assert width == (2 * lanes + lanes // 2) * LANE and self.chunk % 8 == 0
        assert rows == LANE and self.half_dec <= self.cap - DEC_RANK and ranks <= LANE


class Info:
    def __init__(self, pre_ref):
        self.places, self.pre_ref = (lax.axis_index("tp"), lax.axis_index("ep")), pre_ref

    def __getitem__(self, i):
        return self.places[i] if i < 2 else self.pre_ref[i - 2]


def iota(shape, dim):
    return lax.broadcasted_iota(I32, shape, dim)


def one_hot(mask):
    return jnp.where(mask, 1.0, 0.0).astype(BF16)


def dot(a, b):
    return jnp.dot(a, b, preferred_element_type=F32)


def is_prefill(info_ref, plan, own):
    found = info_ref[2] == own
    for i in range(1, plan.prefill):
        found = found | (info_ref[2 + i] == own)
    return found


def earlier(plan):
    shape = (plan.rows, plan.rows)
    return one_hot(iota(shape, 0) < iota(shape, 1))


def chunk_index(j, plan, parity, full):
    cap = plan.cap
    spill = (j >= DEC_RANK) & (j < cap) & jnp.logical_not(full)
    last = j >= 2 * cap
    block = jnp.where(last | spill, 2, jnp.where(j < cap, 0, 1))
    start = jnp.where(full, parity * plan.half_pre, 0)
    slot = jnp.where(
        spill, j - DEC_RANK + plan.half_dec, jnp.where(last, j - 2 * cap + start, j - block * cap)
    )
    kept = jnp.logical_not(last) | (j - 2 * cap < jnp.where(full, plan.half_pre, plan.half_dec))
    return jnp.where(kept, block, 3), slot


def named_ranks(plan, full, choice_ref):
    shape = (plan.ranks, plan.rows)
    live = iota(shape, 1) < jnp.where(full, plan.rows, DEC_RANK)
    rank = iota(shape, 0)
    hits = [(choice_ref[k : k + 1, :] == rank) & live for k in range(DEV_TOP)]
    named = sum(jnp.where(hit, 1.0, 0.0) for hit in hits)
    return hits, named, places(plan, named)


def places(plan, named):
    before = dot(named.astype(BF16), earlier(plan))
    return jnp.where(named > 0.5, before, -1.0)


def pack_kernel(plan, pre_hbm, choice_hbm, le_hbm, rw_hbm, tok_ref, out_ref, *scratch):
    pre_ref, choice_ref, le_ref, rw_ref, x_ref, sems = scratch
    info_ref = Info(pre_ref)
    lane, own = info_ref[0], info_ref[1]
    first_at = pl.multiple_of(lane * (2 * LANE), LANE)
    tail_at = pl.multiple_of((2 * plan.lanes + lane // 2) * LANE, LANE)
    ends = [
        (pre_hbm, pre_ref),
        (choice_hbm, choice_ref),
        (le_hbm, le_ref),
        (rw_hbm, rw_ref),
        (tok_ref.at[:, pl.ds(first_at, 2 * LANE)], x_ref.at[:, 0 : 2 * LANE]),
        (tok_ref.at[:, pl.ds(tail_at, LANE)], x_ref.at[:, 2 * LANE : 3 * LANE]),
    ]
    copies = [pltpu.make_async_copy(a, b, sems.at[i]) for i, (a, b) in enumerate(ends)]
    for copy in copies:
        copy.start()
    for copy in copies[:4]:
        copy.wait()
    full = is_prefill(info_ref, plan, own)
    hits, named, place = named_ranks(plan, full, choice_ref)
    weights = []
    for e in range(2):
        total = jnp.zeros(named.shape, F32)
        for k, hit in enumerate(hits):
            for j in (2 * k, 2 * k + 1):
                chosen = hit & (le_ref[j : j + 1, :] == e)
                total += jnp.where(chosen, rw_ref[j : j + 1, :], 0.0)
        weights.append(total)
    full_shape = (plan.ranks, plan.chunk, LANE)
    flat = plan.ranks * plan.chunk
    j = iota(full_shape, 1)
    block, slot = chunk_index(j, plan, lane % 2, full)
    match = place.astype(I32)[:, None, :] == slot
    picks = [one_hot(match & (block == b)).reshape(flat, LANE) for b in range(3)]
    for copy in copies[4:]:
        copy.wait()
    total = sum(dot(picks[b], x_ref[:, b * LANE : (b + 1) * LANE]) for b in range(3))
    total = total.reshape(full_shape)
    total = jnp.where(j == plan.chunk - 2, weights[0][:, None, :], total)
    total = jnp.where(j == plan.chunk - 1, weights[1][:, None, :], total)
    out_ref[...] = total.astype(BF16)


def weight_rows(plan, data):
    shape = (plan.ranks, plan.ranks * plan.chunk)
    at = iota(shape, 0) * plan.chunk + plan.chunk - 2
    return [dot(one_hot(iota(shape, 1) == at + e), data) for e in range(2)]


def target_row(info_ref, plan, named):
    lane = info_ref[0]
    ranks, total = plan.ranks, plan.ranks * plan.chunk
    rank = iota((8, ranks), 1)
    fulls = jnp.zeros((8, ranks), I32)
    for i in range(plan.prefill):
        fulls += jnp.where(rank == info_ref[2 + i], 1, 0)
    ones = jnp.full((8, plan.rows), 1.0, BF16)
    counts = lax.dot_general(
        ones, named.astype(BF16), (((1,), (1,)), ((), ())), preferred_element_type=F32
    )
    decode = jnp.where(fulls > 0, 0.0, counts).astype(BF16)
    full = jnp.where(fulls > 0, 1.0, 0.0).astype(BF16)
    spread = (ranks, total)
    source = iota(spread, 1) // plan.chunk
    below = one_hot(iota(spread, 0) < source)
    here = one_hot(iota(spread, 0) == source)
    base = dot(decode, below).astype(I32)
    held = dot(decode, here).astype(I32)
    index = dot(full, below).astype(I32)
    full = dot(full, here) > 0.5
    needed = jnp.sum(decode.astype(F32), axis=1, keepdims=True)
    j = iota((8, total), 1) % plan.chunk
    block, slot = chunk_index(j, plan, lane % 2, full)
    half_rows = plan.decode // 2
    place = base + slot
    second = jnp.where(jnp.where(full, slot - plan.half_pre, place - half_rows) >= 0, 1, 0)
    row = jnp.where(
        full,
        index * plan.half_pre + slot - second * plan.half_pre,
        plan.prefill * plan.half_pre + place - second * half_rows,
    )
    kept = full | ((slot < held) & (place < plan.decode) & ((block < 2) | (second == lane % 2)))
    piece = jnp.where(block == 2, 4, 2 * block + second)
    return jnp.where(kept & (block < 3), piece * plan.half + row, -1), needed


def compact_kernel(plan, info_ref, in_ref, out_ref, target_ref, needed_ref):
    total = plan.ranks * plan.chunk
    data = in_ref[...].reshape(total, LANE)
    first = weight_rows(plan, data)[0]
    named = jnp.where(first > 0.0, 1.0, 0.0)
    target, needed = target_row(info_ref, plan, named)
    target_ref[...] = target
    needed_ref[...] = jnp.broadcast_to(needed, (8, LANE))
    for at in range(0, plan.packed, plan.half):
        take = one_hot(iota((plan.half, total), 0) + at == target[0:1, :])
        out_ref[at : at + plan.half, :] = dot(take, data).astype(BF16)


def weights_kernel(plan, in_ref, target_ref, weight_ref):
    total = plan.ranks * plan.chunk
    data = in_ref[...].reshape(total, LANE)
    first, second = weight_rows(plan, data)
    place = places(plan, jnp.where(first > 0.0, 1.0, 0.0)).astype(I32)
    full_shape = (plan.ranks, plan.chunk, LANE)
    j = iota(full_shape, 1)
    match = (place[:, None, :] == j) & (j < plan.cap)
    target = target_ref[0:1, :]
    wide = []
    for value in (first, second):
        kept = jnp.where(match, value[:, None, :], 0.0)
        column = jnp.sum(kept, axis=2, keepdims=True)
        wide.append(jnp.broadcast_to(column, full_shape).reshape(total, LANE).astype(BF16))
    for piece in range(2):
        at = piece * plan.half
        take = one_hot(iota((plan.half, total), 0) + at == target)
        for e in range(2):
            weight_ref[at : at + plan.half, e * LANE : (e + 1) * LANE] = dot(take, wide[e])


def spread_table_kernel(plan, target_ref, spread_ref):
    total = plan.ranks * plan.chunk
    col = iota((LANE, LANE), 1)
    for g in range(0, total, LANE):
        wide = jnp.broadcast_to(target_ref[0:1, g : g + LANE], (LANE, LANE))
        column = wide.astype(F32).T.astype(I32)
        for at in range(0, plan.packed_up, LANE):
            spread_ref[g : g + LANE, at : at + LANE] = one_hot(col + at == column)


def combine_table_kernel(plan, info_ref, choice_ref, combine_ref):
    lane, own = info_ref[0], info_ref[1]
    ranks, rows = plan.ranks, plan.rows
    total = ranks * plan.chunk
    full = is_prefill(info_ref, plan, own)
    _, _, place = named_ranks(plan, full, choice_ref)
    square = jnp.concatenate([place, jnp.zeros((rows - ranks, rows), F32)], axis=0)
    turned = square.T[:, :ranks].astype(BF16)
    spread = (ranks, total)
    expand = one_hot(iota(spread, 1) // plan.chunk == iota(spread, 0))
    spots = dot(turned, expand).astype(I32)
    j = iota((1, total), 1) % plan.chunk
    block, slot = chunk_index(j, plan, lane % 2, full)
    match = spots == slot
    for b in range(3):
        combine_ref[:, b * total : (b + 1) * total] = one_hot(match & (block == b))


def expert_kernel(plan, offsets, info_ref, *refs):
    n = len(offsets)
    weight_ref, wg, wu, wd, out_ref, x_ref, h_ref = refs[n:]
    me, way = info_ref[0], 1 - 2 * lax.rem(info_ref[1], 2)
    lanes, half, slots = plan.lanes, plan.half, plan.slots
    for offset, part in zip(offsets, refs):
        lane = lax.rem(me + way * offset + lanes, lanes)
        first = pl.multiple_of(lane * (2 * LANE), LANE)
        tail = pl.multiple_of((2 * lanes + lane // 2) * LANE, LANE)
        start = pl.multiple_of(lax.rem(lane, 2) * half, 8)
        x_ref[:, pl.ds(first, LANE)] = part[0:slots, :]
        x_ref[:, pl.ds(pl.multiple_of(first + LANE, LANE), LANE)] = part[slots : 2 * slots, :]
        x_ref[pl.ds(start, half), pl.ds(tail, LANE)] = part[2 * slots : 2 * slots + half, :]
    turned = (((1,), (1,)), ((), ()))
    x = x_ref[...]
    gate = lax.dot_general(x, wg[...], turned, preferred_element_type=F32)
    up = lax.dot_general(x, wu[...], turned, preferred_element_type=F32)
    hidden = gate / (1.0 + jnp.exp(-gate)) * up * weight_ref[...]
    h_ref[...] = hidden.astype(BF16)
    for lane in range(lanes):
        at = lane * 2 * LANE
        y = dot(h_ref[...], wd[:, at : at + 2 * LANE]).astype(BF16)
        out_ref[lane, 0:slots, :] = y[:, :LANE]
        out_ref[lane, slots : 2 * slots, :] = y[:, LANE:]
    for pair in range(0, lanes // 2, 2):
        at = (2 * lanes + pair) * LANE
        y = dot(h_ref[...], wd[:, at : at + 2 * LANE]).astype(BF16)
        for k in range(2):
            for p in range(2):
                piece = y[p * half : (p + 1) * half, k * LANE : (k + 1) * LANE]
                out_ref[2 * (pair + k) + p, 2 * slots : 2 * slots + half, :] = piece


def spread_kernel(plan, take_ref, needed_ref, in_ref, out_ref, sum_ref):
    total = in_ref[0].astype(F32)
    for lane in range(1, plan.lanes):
        total += in_ref[lane].astype(F32)
    sum_ref[0 : plan.packed, :] = total.astype(BF16)
    sum_ref[plan.packed :, :] = jnp.zeros((plan.packed_up - plan.packed, LANE), BF16)
    shape = (plan.ranks, plan.chunk, LANE)
    spread = dot(take_ref[...], sum_ref[...]).reshape(shape)
    over = jnp.where(needed_ref[0:1, :] > float(plan.decode), 1.0, 0.0)
    spread = jnp.where(iota(shape, 1) == plan.chunk - 1, over[None], spread)
    out_ref[...] = spread.astype(BF16)


def combine_kernel(plan, take_ref, in_ref, out_ref, over_ref):
    total = plan.ranks * plan.chunk
    data = in_ref[...].reshape(total, LANE)
    own_rows = plan.own_rows
    for b in range(3):
        mine = dot(take_ref[:, b * total : (b + 1) * total], data).astype(BF16)
        for to in range(plan.lanes):
            out_ref[to, b * own_rows : (b + 1) * own_rows, :] = mine[
                to * own_rows : (to + 1) * own_rows
            ]
    shape = (8, total)
    flags = one_hot(iota(shape, 1) % plan.chunk == plan.chunk - 1)
    over_ref[0] = jnp.where(jnp.max(dot(flags, data)) > 0.0, 1, 0)


def finish_kernel(plan, in_ref, out_ref):
    n = plan.own_rows
    for lane in range(plan.lanes):
        at = lane * 2 * LANE
        out_ref[:, at : at + LANE] = in_ref[lane, 0:n, :]
        out_ref[:, at + LANE : at + 2 * LANE] = in_ref[lane, n : 2 * n, :]
    for pair in range(plan.lanes // 2):
        at = (2 * plan.lanes + pair) * LANE
        first = in_ref[2 * pair, 2 * n : 3 * n, :].astype(F32)
        second = in_ref[2 * pair + 1, 2 * n : 3 * n, :].astype(F32)
        out_ref[:, at : at + LANE] = (first + second).astype(BF16)


SMEM = pl.BlockSpec(memory_space=pltpu.SMEM)
VMEM = pl.BlockSpec(memory_space=pltpu.VMEM)
HBM = pl.BlockSpec(memory_space=pltpu.HBM)

def call(kernel, name, out, specs, *args, scratch=(), limit=24 << 20, flops=0):
    cost = None
    if flops:
        cost = pl.CostEstimate(flops=flops, bytes_accessed=1 << 20, transcendentals=0)
    return pl.pallas_call(
        kernel,
        out_shape=out,
        in_specs=specs,
        out_specs=jax.tree.map(lambda o: SMEM if o.shape == (1,) else VMEM, out),
        scratch_shapes=scratch,
        compiler_params=pltpu.CompilerParams(vmem_limit_bytes=limit),
        cost_estimate=cost,
        interpret=INTERPRET,
        name=name,
    )(*args)


def pack(plan, prefill_ranks, choice, local, weights, tokens):
    return call(
        lambda *refs: pack_kernel(plan, *refs),
        "pack",
        jax.ShapeDtypeStruct((plan.ranks, plan.chunk, LANE), BF16),
        [HBM] * 5,
        prefill_ranks,
        choice,
        local,
        weights,
        tokens,
        scratch=[
            pltpu.SMEM(prefill_ranks.shape, I32),
            pltpu.VMEM(choice.shape, I32),
            pltpu.VMEM(local.shape, I32),
            pltpu.VMEM(weights.shape, F32),
            pltpu.VMEM((plan.rows, 3 * LANE), BF16),
            pltpu.SemaphoreType.DMA((6,)),
        ],
    )


def compact(plan, info, received):
    return call(
        lambda *refs: compact_kernel(plan, Info(refs[0]), *refs[1:]),
        "compact",
        (
            jax.ShapeDtypeStruct((plan.packed, LANE), BF16),
            jax.ShapeDtypeStruct((8, plan.ranks * plan.chunk), I32),
            jax.ShapeDtypeStruct((8, LANE), F32),
        ),
        [SMEM, VMEM],
        info,
        received,
    )


def weights_table(plan, received, target):
    return call(
        lambda *refs: weights_kernel(plan, *refs),
        "weights",
        jax.ShapeDtypeStruct((plan.slots, 2 * LANE), F32),
        [VMEM, VMEM],
        received,
        target,
        flops=1 << 29,
    )


def spread_table(plan, target):
    return call(
        lambda *refs: spread_table_kernel(plan, *refs),
        "spread_table",
        jax.ShapeDtypeStruct((plan.ranks * plan.chunk, plan.packed_up), BF16),
        [VMEM],
        target,
        flops=1 << 29,
    )


def combine_table(plan, info, choice):
    return call(
        lambda *refs: combine_table_kernel(plan, Info(refs[0]), *refs[1:]),
        "combine_table",
        jax.ShapeDtypeStruct((plan.rows, 3 * plan.ranks * plan.chunk), BF16),
        [SMEM, VMEM],
        info,
        choice,
        flops=1 << 29,
    )


def experts(plan, offsets, info, parts, weights, w_gate, w_up, w_down):
    hidden = w_gate.shape[0] * w_gate.shape[1]
    flat = [w.reshape(hidden, plan.width) for w in (w_gate, w_up, w_down)]
    return call(
        lambda *refs: expert_kernel(plan, offsets, Info(refs[0]), *refs[1:]),
        "experts",
        jax.ShapeDtypeStruct((plan.lanes, plan.packed, LANE), BF16),
        [SMEM] + [VMEM] * (len(parts) + 4),
        info,
        *parts,
        weights,
        *flat,
        scratch=[
            pltpu.VMEM((plan.slots, plan.width), BF16),
            pltpu.VMEM((plan.slots, hidden), BF16),
        ],
        limit=32 << 20,
    )


def spread(plan, take, needed, returned):
    return call(
        lambda *refs: spread_kernel(plan, *refs),
        "spread",
        jax.ShapeDtypeStruct((plan.ranks, plan.chunk, LANE), BF16),
        [VMEM] * 3,
        take,
        needed,
        returned,
        scratch=[pltpu.VMEM((plan.packed_up, LANE), BF16)],
    )


def combine(plan, take, back):
    return call(
        lambda *refs: combine_kernel(plan, *refs),
        "combine",
        (
            jax.ShapeDtypeStruct((plan.lanes, 3 * plan.own_rows, LANE), BF16),
            jax.ShapeDtypeStruct((1,), I32),
        ),
        [VMEM, VMEM],
        take,
        back,
    )


def finish(plan, shares):
    return call(
        lambda *refs: finish_kernel(plan, *refs),
        "finish",
        jax.ShapeDtypeStruct((plan.own_rows, plan.width), BF16),
        [VMEM],
        shares,
    )


def gather_lanes(packed, lanes, beside):
    ranks = lax.axis_size("ep")
    ways = []
    for way in (1, -1):
        steps = [way if rank % 2 == 0 else -way for rank in range(ranks)]
        ways.append(
            [
                (rank * lanes + i, rank * lanes + (i + steps[rank]) % lanes)
                for rank in range(ranks)
                for i in range(lanes)
            ]
        )
    right, left = ways
    axes = ("ep", "tp")
    parts, offsets = [packed], [0]
    held = [packed, packed]
    for hop in range(1, lanes // 2 + 1):
        got = [lax.ppermute(held[0], axes, right)]
        offsets.append(-hop)
        if hop < lanes // 2:
            got.append(lax.ppermute(held[1], axes, left))
            offsets.append(hop)
        parts += got
        held = got
    last, beside = lax.optimization_barrier((parts[-1], beside))
    return parts[:-1] + [last], offsets, beside


def through_experts(plan, info, received, take_in, matrices):
    packed, target, needed = compact(plan, info, received)
    beside = [weights_table(plan, received, target), spread_table(plan, target), take_in]
    parts, offsets, beside = gather_lanes(packed, plan.lanes, beside)
    weights, take_out, take_in = beside
    partial = experts(plan, offsets, info, parts, weights, *matrices)
    returned = lax.all_to_all(partial, "tp", 0, 0, tiled=True)
    back = lax.all_to_all(spread(plan, take_out, needed, returned), "ep", 0, 0, tiled=True)
    return combine(plan, take_in, back)


def on_device(
    tokens, device_choice, local_expert, route_weight, prefill_ranks, w_gate, w_up, w_down
):
    ranks, prefill = lax.axis_size("ep"), prefill_ranks.shape[0]
    sizes = (ranks, lax.axis_size("tp"), *tokens.shape, prefill)
    most = (ranks - prefill) * DEC_RANK
    plan, whole = Plan(*sizes, min(USUAL_DECODE, most)), Plan(*sizes, most)
    stay = [prefill_ranks, device_choice.T, local_expert.T, route_weight.T, tokens]
    stay = [pltpu.with_memory_space_constraint(x, pltpu.HBM) for x in stay]
    outgoing = pack(plan, *stay)
    received = lax.all_to_all(outgoing, "ep", 0, 0, tiled=True)
    received, info, choice = lax.optimization_barrier((received, stay[0], stay[1]))
    take_in = combine_table(plan, info, choice)
    rest = (info, received, take_in, (w_gate, w_up, w_down))
    shares, over = through_experts(plan, *rest)
    rest, over = lax.optimization_barrier((rest, over))
    shares = lax.cond(
        over[0] > 0, lambda: through_experts(whole, *rest)[0], lambda: shares
    )
    shares = lax.all_to_all(shares, "tp", 0, 0, tiled=True)
    return finish(plan, shares)


def solution(mesh):
    in_specs = (
        P(("groups", "ep"), None),
        P(("groups", "ep"), None),
        P(("groups", "ep"), None),
        P(("groups", "ep"), None),
        P("groups"),
        P("ep", "tp", None),
        P("ep", "tp", None),
        P("ep", "tp", None),
    )
    out_specs = P(("groups", "ep", "tp"), None)
    return jax.shard_map(
        on_device, mesh=mesh, in_specs=in_specs, out_specs=out_specs, check_vma=False
    )
```

```python
import jax
import jax.numpy as jnp
from jax import lax
from jax.experimental import pallas as pl
from jax.experimental.pallas import tpu as pltpu
from jax.sharding import PartitionSpec as P

TOPK = 6
DEV_TOP = 3
DEC_RANK = 8
USUAL_DECODE = 32
LANE = 128
F32, BF16, I32 = jnp.float32, jnp.bfloat16, jnp.int32
INTERPRET = False


class Plan:
    def __init__(self, ranks, lanes, rows, width, prefill, decode):
        self.ranks, self.lanes, self.rows, self.width = ranks, lanes, rows, width
        self.cap = (DEV_TOP * rows + ranks - 1) // ranks
        self.prefill, self.decode = prefill, decode
        self.half_pre = self.cap // 2
        self.half_dec = DEC_RANK // 2
        self.half = prefill * self.half_pre + decode // 2
        self.slots = 2 * self.half
        self.packed = 5 * self.half
        self.packed_up = -(-self.packed // LANE) * LANE
        self.chunk = 2 * self.cap + self.half_pre + 2
        self.own_rows = rows // lanes
        assert width == (2 * lanes + lanes // 2) * LANE and self.chunk % 8 == 0
        assert rows == LANE and self.half_dec <= self.cap - DEC_RANK and ranks <= LANE


class Info:
    def __init__(self, pre_ref):
        self.places, self.pre_ref = (lax.axis_index("tp"), lax.axis_index("ep")), pre_ref

    def __getitem__(self, i):
        return self.places[i] if i < 2 else self.pre_ref[i - 2]


def iota(shape, dim):
    return lax.broadcasted_iota(I32, shape, dim)


def one_hot(mask):
    return jnp.where(mask, 1.0, 0.0).astype(BF16)


def dot(a, b):
    return jnp.dot(a, b, preferred_element_type=F32)


def is_prefill(info_ref, plan, own):
    found = info_ref[2] == own
    for i in range(1, plan.prefill):
        found = found | (info_ref[2 + i] == own)
    return found


def earlier(plan):
    shape = (plan.rows, plan.rows)
    return one_hot(iota(shape, 0) < iota(shape, 1))


def chunk_index(j, plan, parity, full):
    cap = plan.cap
    spill = (j >= DEC_RANK) & (j < cap) & jnp.logical_not(full)
    last = j >= 2 * cap
    block = jnp.where(last | spill, 2, jnp.where(j < cap, 0, 1))
    start = jnp.where(full, parity * plan.half_pre, 0)
    slot = jnp.where(
        spill, j - DEC_RANK + plan.half_dec, jnp.where(last, j - 2 * cap + start, j - block * cap)
    )
    kept = jnp.logical_not(last) | (j - 2 * cap < jnp.where(full, plan.half_pre, plan.half_dec))
    return jnp.where(kept, block, 3), slot


def named_ranks(plan, full, choice_ref):
    shape = (plan.ranks, plan.rows)
    live = iota(shape, 1) < jnp.where(full, plan.rows, DEC_RANK)
    rank = iota(shape, 0)
    hits = [(choice_ref[k : k + 1, :] == rank) & live for k in range(DEV_TOP)]
    named = sum(jnp.where(hit, 1.0, 0.0) for hit in hits)
    return hits, named, places(plan, named)


def places(plan, named):
    before = dot(named.astype(BF16), earlier(plan))
    return jnp.where(named > 0.5, before, -1.0)


def pack_kernel(plan, pre_hbm, choice_hbm, le_hbm, rw_hbm, tok_ref, out_ref, *scratch):
    pre_ref, choice_ref, le_ref, rw_ref, x_ref, sems = scratch
    info_ref = Info(pre_ref)
    lane, own = info_ref[0], info_ref[1]
    first_at = pl.multiple_of(lane * (2 * LANE), LANE)
    tail_at = pl.multiple_of((2 * plan.lanes + lane // 2) * LANE, LANE)
    ends = [
        (pre_hbm, pre_ref),
        (choice_hbm, choice_ref),
        (le_hbm, le_ref),
        (rw_hbm, rw_ref),
        (tok_ref.at[:, pl.ds(first_at, 2 * LANE)], x_ref.at[:, 0 : 2 * LANE]),
        (tok_ref.at[:, pl.ds(tail_at, LANE)], x_ref.at[:, 2 * LANE : 3 * LANE]),
    ]
    copies = [pltpu.make_async_copy(a, b, sems.at[i]) for i, (a, b) in enumerate(ends)]
    for copy in copies:
        copy.start()
    for copy in copies[:4]:
        copy.wait()
    full = is_prefill(info_ref, plan, own)
    hits, named, place = named_ranks(plan, full, choice_ref)
    weights = []
    for e in range(2):
        total = jnp.zeros(named.shape, F32)
        for k, hit in enumerate(hits):
            for j in (2 * k, 2 * k + 1):
                chosen = hit & (le_ref[j : j + 1, :] == e)
                total += jnp.where(chosen, rw_ref[j : j + 1, :], 0.0)
        weights.append(total)
    full_shape = (plan.ranks, plan.chunk, LANE)
    flat = plan.ranks * plan.chunk
    j = iota(full_shape, 1)
    block, slot = chunk_index(j, plan, lane % 2, full)
    match = place.astype(I32)[:, None, :] == slot
    picks = [one_hot(match & (block == b)).reshape(flat, LANE) for b in range(3)]
    for copy in copies[4:]:
        copy.wait()
    total = sum(dot(picks[b], x_ref[:, b * LANE : (b + 1) * LANE]) for b in range(3))
    total = total.reshape(full_shape)
    total = jnp.where(j == plan.chunk - 2, weights[0][:, None, :], total)
    total = jnp.where(j == plan.chunk - 1, weights[1][:, None, :], total)
    out_ref[...] = total.astype(BF16)


def weight_rows(plan, data, expert):
    shape = (plan.ranks, plan.ranks * plan.chunk)
    at = iota(shape, 0) * plan.chunk + plan.chunk - 2 + expert
    return dot(one_hot(iota(shape, 1) == at), data)


def target_row(info_ref, plan, named):
    lane = info_ref[0]
    ranks, total = plan.ranks, plan.ranks * plan.chunk
    rank = iota((8, ranks), 1)
    fulls = jnp.zeros((8, ranks), I32)
    for i in range(plan.prefill):
        fulls += jnp.where(rank == info_ref[2 + i], 1, 0)
    ones = jnp.full((8, plan.rows), 1.0, BF16)
    counts = lax.dot_general(
        ones, named.astype(BF16), (((1,), (1,)), ((), ())), preferred_element_type=F32
    )
    decode = jnp.where(fulls > 0, 0.0, counts).astype(BF16)
    full = jnp.where(fulls > 0, 1.0, 0.0).astype(BF16)
    spread = (ranks, total)
    source = iota(spread, 1) // plan.chunk
    below = one_hot(iota(spread, 0) < source)
    here = one_hot(iota(spread, 0) == source)
    base = dot(decode, below).astype(I32)
    held = dot(decode, here).astype(I32)
    index = dot(full, below).astype(I32)
    full = dot(full, here) > 0.5
    needed = jnp.sum(decode.astype(F32), axis=1, keepdims=True)
    j = iota((8, total), 1) % plan.chunk
    block, slot = chunk_index(j, plan, lane % 2, full)
    half_rows = plan.decode // 2
    place = base + slot
    second = jnp.where(jnp.where(full, slot - plan.half_pre, place - half_rows) >= 0, 1, 0)
    row = jnp.where(
        full,
        index * plan.half_pre + slot - second * plan.half_pre,
        plan.prefill * plan.half_pre + place - second * half_rows,
    )
    kept = full | ((slot < held) & (place < plan.decode) & ((block < 2) | (second == lane % 2)))
    piece = jnp.where(block == 2, 4, 2 * block + second)
    return jnp.where(kept & (block < 3), piece * plan.half + row, -1), needed


def compact_kernel(plan, info_ref, in_ref, out_ref, target_ref, needed_ref):
    total = plan.ranks * plan.chunk
    data = in_ref[...].reshape(total, LANE)
    first = weight_rows(plan, data, 0)
    named = jnp.where(first > 0.0, 1.0, 0.0)
    target, needed = target_row(info_ref, plan, named)
    target_ref[...] = target
    needed_ref[...] = jnp.broadcast_to(needed, (8, LANE))
    for at in range(0, plan.packed, plan.half):
        take = one_hot(iota((plan.half, total), 0) + at == target[0:1, :])
        out_ref[at : at + plan.half, :] = dot(take, data).astype(BF16)


def weights_kernel(plan, in_ref, target_ref, weight_ref):
    total = plan.ranks * plan.chunk
    data = in_ref[...].reshape(total, LANE)
    first, second = weight_rows(plan, data, 0), weight_rows(plan, data, 1)
    place = places(plan, jnp.where(first > 0.0, 1.0, 0.0)).astype(I32)
    full_shape = (plan.ranks, plan.chunk, LANE)
    j = iota(full_shape, 1)
    match = (place[:, None, :] == j) & (j < plan.cap)
    target = target_ref[0:1, :]
    wide = []
    for value in (first, second):
        kept = jnp.where(match, value[:, None, :], 0.0)
        column = jnp.sum(kept, axis=2, keepdims=True)
        wide.append(jnp.broadcast_to(column, full_shape).reshape(total, LANE).astype(BF16))
    for piece in range(2):
        at = piece * plan.half
        take = one_hot(iota((plan.half, total), 0) + at == target)
        for e in range(2):
            weight_ref[at : at + plan.half, e * LANE : (e + 1) * LANE] = dot(take, wide[e])


def spread_table_kernel(plan, target_ref, spread_ref):
    total = plan.ranks * plan.chunk
    col = iota((LANE, LANE), 1)
    for g in range(0, total, LANE):
        wide = jnp.broadcast_to(target_ref[0:1, g : g + LANE], (LANE, LANE))
        column = wide.astype(F32).T.astype(I32)
        for at in range(0, plan.packed_up, LANE):
            spread_ref[g : g + LANE, at : at + LANE] = one_hot(col + at == column)


def combine_table_kernel(plan, info_ref, choice_ref, combine_ref):
    lane, own = info_ref[0], info_ref[1]
    ranks, rows = plan.ranks, plan.rows
    total = ranks * plan.chunk
    full = is_prefill(info_ref, plan, own)
    _, _, place = named_ranks(plan, full, choice_ref)
    square = jnp.concatenate([place, jnp.zeros((rows - ranks, rows), F32)], axis=0)
    turned = square.T[:, :ranks].astype(BF16)
    spread = (ranks, total)
    expand = one_hot(iota(spread, 1) // plan.chunk == iota(spread, 0))
    spots = dot(turned, expand).astype(I32)
    j = iota((1, total), 1) % plan.chunk
    block, slot = chunk_index(j, plan, lane % 2, full)
    match = spots == slot
    for b in range(3):
        combine_ref[:, b * total : (b + 1) * total] = one_hot(match & (block == b))


def share_columns(plan, info_ref, offset):
    way = 1 - 2 * lax.rem(info_ref[1], 2)
    lane = lax.rem(info_ref[0] + way * offset + plan.lanes, plan.lanes)
    first = pl.multiple_of(lane * (2 * LANE), LANE)
    tail = pl.multiple_of((2 * plan.lanes + lane // 2) * LANE, LANE)
    start = pl.multiple_of(lax.rem(lane, 2) * plan.half, 8)
    return first, tail, pl.ds(start, plan.half)


TURNED = (((1,), (1,)), ((), ()))


def early_kernel(plan, offsets, late, info_ref, *refs):
    n = len(offsets)
    wg, wu, gate_ref, up_ref, x_ref = refs[n:]
    half, slots = plan.half, plan.slots
    for offset, part in zip(offsets + [late], refs[:n] + (None,)):
        first, tail, rows = share_columns(plan, info_ref, offset)
        if part is None:
            x_ref[:, pl.ds(first, 2 * LANE)] = jnp.zeros((slots, 2 * LANE), BF16)
            x_ref[rows, pl.ds(tail, LANE)] = jnp.zeros((half, LANE), BF16)
        else:
            x_ref[:, pl.ds(first, LANE)] = part[0:slots, :]
            x_ref[:, pl.ds(pl.multiple_of(first + LANE, LANE), LANE)] = part[slots : 2 * slots, :]
            x_ref[rows, pl.ds(tail, LANE)] = part[2 * slots : 2 * slots + half, :]
    x = x_ref[...]
    gate_ref[...] = lax.dot_general(x, wg[...], TURNED, preferred_element_type=F32)
    up_ref[...] = lax.dot_general(x, wu[...], TURNED, preferred_element_type=F32)


def expert_kernel(plan, late, info_ref, part, gate_ref, up_ref, weight_ref, wg, wu, wd, out_ref, x_ref, h_ref):
    lanes, half, slots = plan.lanes, plan.half, plan.slots
    first, tail, rows = share_columns(plan, info_ref, late)
    x_ref[:, 0:LANE] = part[0:slots, :]
    x_ref[:, LANE : 2 * LANE] = part[slots : 2 * slots, :]
    x_ref[:, 2 * LANE : 3 * LANE] = jnp.zeros((slots, LANE), BF16)
    x_ref[rows, 2 * LANE : 3 * LANE] = part[2 * slots : 2 * slots + half, :]
    gate, up = gate_ref[...], up_ref[...]
    for at, columns in ((0, pl.ds(first, 2 * LANE)), (2 * LANE, pl.ds(tail, LANE))):
        x = x_ref[:, at : at + columns.size]
        gate += lax.dot_general(x, wg[:, columns], TURNED, preferred_element_type=F32)
        up += lax.dot_general(x, wu[:, columns], TURNED, preferred_element_type=F32)
    hidden = gate / (1.0 + jnp.exp(-gate)) * up * weight_ref[...]
    h_ref[...] = hidden.astype(BF16)
    for lane in range(lanes):
        at = lane * 2 * LANE
        y = dot(h_ref[...], wd[:, at : at + 2 * LANE]).astype(BF16)
        out_ref[lane, 0:slots, :] = y[:, :LANE]
        out_ref[lane, slots : 2 * slots, :] = y[:, LANE:]
    for pair in range(0, lanes // 2, 2):
        at = (2 * lanes + pair) * LANE
        y = dot(h_ref[...], wd[:, at : at + 2 * LANE]).astype(BF16)
        for k in range(2):
            for p in range(2):
                piece = y[p * half : (p + 1) * half, k * LANE : (k + 1) * LANE]
                out_ref[2 * (pair + k) + p, 2 * slots : 2 * slots + half, :] = piece


def spread_kernel(plan, take_ref, needed_ref, in_ref, out_ref, sum_ref):
    total = in_ref[0].astype(F32)
    for lane in range(1, plan.lanes):
        total += in_ref[lane].astype(F32)
    sum_ref[0 : plan.packed, :] = total.astype(BF16)
    sum_ref[plan.packed :, :] = jnp.zeros((plan.packed_up - plan.packed, LANE), BF16)
    shape = (plan.ranks, plan.chunk, LANE)
    spread = dot(take_ref[...], sum_ref[...]).reshape(shape)
    over = jnp.where(needed_ref[0:1, :] > float(plan.decode), 1.0, 0.0)
    spread = jnp.where(iota(shape, 1) == plan.chunk - 1, over[None], spread)
    out_ref[...] = spread.astype(BF16)


def combine_kernel(plan, take_ref, in_ref, out_ref, over_ref):
    total = plan.ranks * plan.chunk
    data = in_ref[...].reshape(total, LANE)
    own_rows = plan.own_rows
    for b in range(3):
        mine = dot(take_ref[:, b * total : (b + 1) * total], data).astype(BF16)
        for to in range(plan.lanes):
            out_ref[to, b * own_rows : (b + 1) * own_rows, :] = mine[
                to * own_rows : (to + 1) * own_rows
            ]
    shape = (8, total)
    flags = one_hot(iota(shape, 1) % plan.chunk == plan.chunk - 1)
    over_ref[0] = jnp.where(jnp.max(dot(flags, data)) > 0.0, 1, 0)


def finish_kernel(plan, in_ref, out_ref):
    n = plan.own_rows
    for lane in range(plan.lanes):
        at = lane * 2 * LANE
        out_ref[:, at : at + LANE] = in_ref[lane, 0:n, :]
        out_ref[:, at + LANE : at + 2 * LANE] = in_ref[lane, n : 2 * n, :]
    for pair in range(plan.lanes // 2):
        at = (2 * plan.lanes + pair) * LANE
        first = in_ref[2 * pair, 2 * n : 3 * n, :].astype(F32)
        second = in_ref[2 * pair + 1, 2 * n : 3 * n, :].astype(F32)
        out_ref[:, at : at + LANE] = (first + second).astype(BF16)


SMEM = pl.BlockSpec(memory_space=pltpu.SMEM)
VMEM = pl.BlockSpec(memory_space=pltpu.VMEM)
HBM = pl.BlockSpec(memory_space=pltpu.HBM)

def call(kernel, name, out, specs, *args, scratch=(), limit=24 << 20, flops=0):
    cost = None
    if flops:
        cost = pl.CostEstimate(flops=flops, bytes_accessed=1 << 20, transcendentals=0)
    return pl.pallas_call(
        kernel,
        out_shape=out,
        in_specs=specs,
        out_specs=jax.tree.map(lambda o: SMEM if o.shape == (1,) else VMEM, out),
        scratch_shapes=scratch,
        compiler_params=pltpu.CompilerParams(vmem_limit_bytes=limit),
        cost_estimate=cost,
        interpret=INTERPRET,
        name=name,
    )(*args)


def pack(plan, prefill_ranks, choice, local, weights, tokens):
    return call(
        lambda *refs: pack_kernel(plan, *refs),
        "pack",
        jax.ShapeDtypeStruct((plan.ranks, plan.chunk, LANE), BF16),
        [HBM] * 5,
        prefill_ranks,
        choice,
        local,
        weights,
        tokens,
        scratch=[
            pltpu.SMEM(prefill_ranks.shape, I32),
            pltpu.VMEM(choice.shape, I32),
            pltpu.VMEM(local.shape, I32),
            pltpu.VMEM(weights.shape, F32),
            pltpu.VMEM((plan.rows, 3 * LANE), BF16),
            pltpu.SemaphoreType.DMA((6,)),
        ],
    )


def compact(plan, info, received):
    return call(
        lambda *refs: compact_kernel(plan, Info(refs[0]), *refs[1:]),
        "compact",
        (
            jax.ShapeDtypeStruct((plan.packed, LANE), BF16),
            jax.ShapeDtypeStruct((8, plan.ranks * plan.chunk), I32),
            jax.ShapeDtypeStruct((8, LANE), F32),
        ),
        [SMEM, VMEM],
        info,
        received,
    )


def weights_table(plan, received, target):
    return call(
        lambda *refs: weights_kernel(plan, *refs),
        "weights",
        jax.ShapeDtypeStruct((plan.slots, 2 * LANE), F32),
        [VMEM, VMEM],
        received,
        target,
        flops=1 << 29,
    )


def spread_table(plan, target):
    return call(
        lambda *refs: spread_table_kernel(plan, *refs),
        "spread_table",
        jax.ShapeDtypeStruct((plan.ranks * plan.chunk, plan.packed_up), BF16),
        [VMEM],
        target,
        flops=1 << 29,
    )


def combine_table(plan, info, choice):
    return call(
        lambda *refs: combine_table_kernel(plan, Info(refs[0]), *refs[1:]),
        "combine_table",
        jax.ShapeDtypeStruct((plan.rows, 3 * plan.ranks * plan.chunk), BF16),
        [SMEM, VMEM],
        info,
        choice,
        flops=1 << 29,
    )


def experts(plan, offsets, info, parts, weights, w_gate, w_up, w_down):
    hidden = w_gate.shape[0] * w_gate.shape[1]
    w_gate, w_up, w_down = [w.reshape(hidden, plan.width) for w in (w_gate, w_up, w_down)]
    late = offsets[-1]
    product = jax.ShapeDtypeStruct((plan.slots, hidden), F32)
    gate, up = call(
        lambda *refs: early_kernel(plan, offsets[:-1], late, Info(refs[0]), *refs[1:]),
        "early",
        (product, product),
        [SMEM] + [VMEM] * (len(parts) + 1),
        info,
        *parts[:-1],
        w_gate,
        w_up,
        scratch=[pltpu.VMEM((plan.slots, plan.width), BF16)],
        flops=1 << 29,
    )
    return call(
        lambda *refs: expert_kernel(plan, late, Info(refs[0]), *refs[1:]),
        "experts",
        jax.ShapeDtypeStruct((plan.lanes, plan.packed, LANE), BF16),
        [SMEM] + [VMEM] * 7,
        info,
        parts[-1],
        gate,
        up,
        weights,
        w_gate,
        w_up,
        w_down,
        scratch=[
            pltpu.VMEM((plan.slots, 3 * LANE), BF16),
            pltpu.VMEM((plan.slots, hidden), BF16),
        ],
    )


def spread(plan, take, needed, returned):
    return call(
        lambda *refs: spread_kernel(plan, *refs),
        "spread",
        jax.ShapeDtypeStruct((plan.ranks, plan.chunk, LANE), BF16),
        [VMEM] * 3,
        take,
        needed,
        returned,
        scratch=[pltpu.VMEM((plan.packed_up, LANE), BF16)],
    )


def combine(plan, take, back):
    return call(
        lambda *refs: combine_kernel(plan, *refs),
        "combine",
        (
            jax.ShapeDtypeStruct((plan.lanes, 3 * plan.own_rows, LANE), BF16),
            jax.ShapeDtypeStruct((1,), I32),
        ),
        [VMEM, VMEM],
        take,
        back,
    )


def finish(plan, shares):
    return call(
        lambda *refs: finish_kernel(plan, *refs),
        "finish",
        jax.ShapeDtypeStruct((plan.own_rows, plan.width), BF16),
        [VMEM],
        shares,
    )


def gather_lanes(packed, lanes, beside):
    ranks = lax.axis_size("ep")
    ways = []
    for way in (1, -1):
        steps = [way if rank % 2 == 0 else -way for rank in range(ranks)]
        ways.append(
            [
                (rank * lanes + i, rank * lanes + (i + steps[rank]) % lanes)
                for rank in range(ranks)
                for i in range(lanes)
            ]
        )
    right, left = ways
    axes = ("ep", "tp")
    parts, offsets = [packed], [0]
    held = [packed, packed]
    for hop in range(1, lanes // 2 + 1):
        got = [lax.ppermute(held[0], axes, right)]
        offsets.append(-hop)
        if hop < lanes // 2:
            got.append(lax.ppermute(held[1], axes, left))
            offsets.append(hop)
        parts += got
        held = got
    last, beside = lax.optimization_barrier((parts[-1], beside))
    return parts[:-1] + [last], offsets, beside


def through_experts(plan, info, received, take_in, matrices):
    packed, target, needed = compact(plan, info, received)
    beside = [weights_table(plan, received, target), spread_table(plan, target), take_in]
    parts, offsets, beside = gather_lanes(packed, plan.lanes, beside)
    weights, take_out, take_in = beside
    partial = experts(plan, offsets, info, parts, weights, *matrices)
    returned = lax.all_to_all(partial, "tp", 0, 0, tiled=True)
    back = lax.all_to_all(spread(plan, take_out, needed, returned), "ep", 0, 0, tiled=True)
    return combine(plan, take_in, back)


def on_device(
    tokens, device_choice, local_expert, route_weight, prefill_ranks, w_gate, w_up, w_down
):
    ranks, prefill = lax.axis_size("ep"), prefill_ranks.shape[0]
    sizes = (ranks, lax.axis_size("tp"), *tokens.shape, prefill)
    most = (ranks - prefill) * DEC_RANK
    plan, whole = Plan(*sizes, min(USUAL_DECODE, most)), Plan(*sizes, most)
    stay = [prefill_ranks, device_choice.T, local_expert.T, route_weight.T, tokens]
    stay = [pltpu.with_memory_space_constraint(x, pltpu.HBM) for x in stay]
    outgoing = pack(plan, *stay)
    received = lax.all_to_all(outgoing, "ep", 0, 0, tiled=True)
    received, info, choice = lax.optimization_barrier((received, stay[0], stay[1]))
    take_in = combine_table(plan, info, choice)
    rest = (info, received, take_in, (w_gate, w_up, w_down))
    shares, over = through_experts(plan, *rest)
    rest, over = lax.optimization_barrier((rest, over))
    shares = lax.cond(
        over[0] > 0, lambda: through_experts(whole, *rest)[0], lambda: shares
    )
    shares = lax.all_to_all(shares, "tp", 0, 0, tiled=True)
    return finish(plan, shares)


def solution(mesh):
    in_specs = (
        P(("groups", "ep"), None),
        P(("groups", "ep"), None),
        P(("groups", "ep"), None),
        P(("groups", "ep"), None),
        P("groups"),
        P("ep", "tp", None),
        P("ep", "tp", None),
        P("ep", "tp", None),
    )
    out_specs = P(("groups", "ep", "tp"), None)
    return jax.shard_map(
        on_device, mesh=mesh, in_specs=in_specs, out_specs=out_specs, check_vma=False
    )
```

```python
import jax
import jax.numpy as jnp
from jax import lax
from jax.experimental import pallas as pl
from jax.experimental.pallas import tpu as pltpu
from jax.sharding import PartitionSpec as P

TOPK = 6
DEV_TOP = 3
DEC_RANK = 8
USUAL_DECODE = 32
LANE = 128
F32, BF16, I32 = jnp.float32, jnp.bfloat16, jnp.int32
INTERPRET = False


class Plan:
    def __init__(self, ranks, lanes, rows, width, prefill, decode):
        self.ranks, self.lanes, self.rows, self.width = ranks, lanes, rows, width
        self.cap = (DEV_TOP * rows + ranks - 1) // ranks
        self.prefill, self.decode = prefill, decode
        self.half_pre = self.cap // 2
        self.half_dec = DEC_RANK // 2
        self.half = prefill * self.half_pre + decode // 2
        self.slots = 2 * self.half
        self.packed = 5 * self.half
        self.packed_up = -(-self.packed // LANE) * LANE
        self.chunk = 2 * self.cap + self.half_pre + 2
        self.own_rows = rows // lanes
        assert width == (2 * lanes + lanes // 2) * LANE and self.chunk % 8 == 0
        assert rows == LANE and self.half_dec <= self.cap - DEC_RANK and ranks <= LANE


class Info:
    def __init__(self, pre_ref):
        self.places, self.pre_ref = (lax.axis_index("tp"), lax.axis_index("ep")), pre_ref

    def __getitem__(self, i):
        return self.places[i] if i < 2 else self.pre_ref[i - 2]


def iota(shape, dim):
    return lax.broadcasted_iota(I32, shape, dim)


def one_hot(mask):
    return jnp.where(mask, 1.0, 0.0).astype(BF16)


def dot(a, b):
    return jnp.dot(a, b, preferred_element_type=F32)


def is_prefill(info_ref, plan, own):
    found = info_ref[2] == own
    for i in range(1, plan.prefill):
        found = found | (info_ref[2 + i] == own)
    return found


def earlier(plan):
    shape = (plan.rows, plan.rows)
    return one_hot(iota(shape, 0) < iota(shape, 1))


def chunk_index(j, plan, parity, full):
    cap = plan.cap
    spill = (j >= DEC_RANK) & (j < cap) & jnp.logical_not(full)
    last = j >= 2 * cap
    block = jnp.where(last | spill, 2, jnp.where(j < cap, 0, 1))
    start = jnp.where(full, parity * plan.half_pre, 0)
    slot = jnp.where(
        spill, j - DEC_RANK + plan.half_dec, jnp.where(last, j - 2 * cap + start, j - block * cap)
    )
    kept = jnp.logical_not(last) | (j - 2 * cap < jnp.where(full, plan.half_pre, plan.half_dec))
    return jnp.where(kept, block, 3), slot


def named_ranks(plan, full, choice_ref):
    shape = (plan.ranks, plan.rows)
    live = iota(shape, 1) < jnp.where(full, plan.rows, DEC_RANK)
    rank = iota(shape, 0)
    hits = [(choice_ref[k : k + 1, :] == rank) & live for k in range(DEV_TOP)]
    named = sum(jnp.where(hit, 1.0, 0.0) for hit in hits)
    return hits, named, places(plan, named)


def places(plan, named):
    before = dot(named.astype(BF16), earlier(plan))
    return jnp.where(named > 0.5, before, -1.0)


def pack_kernel(plan, pre_hbm, choice_hbm, le_hbm, rw_hbm, tok_ref, out_ref, *scratch):
    pre_ref, choice_ref, le_ref, rw_ref, x_ref, sems = scratch
    info_ref = Info(pre_ref)
    lane, own = info_ref[0], info_ref[1]
    first_at = pl.multiple_of(lane * (2 * LANE), LANE)
    tail_at = pl.multiple_of((2 * plan.lanes + lane // 2) * LANE, LANE)
    ends = [
        (pre_hbm, pre_ref),
        (choice_hbm, choice_ref),
        (le_hbm, le_ref),
        (rw_hbm, rw_ref),
        (tok_ref.at[:, pl.ds(first_at, 2 * LANE)], x_ref.at[:, 0 : 2 * LANE]),
        (tok_ref.at[:, pl.ds(tail_at, LANE)], x_ref.at[:, 2 * LANE : 3 * LANE]),
    ]
    copies = [pltpu.make_async_copy(a, b, sems.at[i]) for i, (a, b) in enumerate(ends)]
    for copy in copies:
        copy.start()
    for copy in copies[:4]:
        copy.wait()
    full = is_prefill(info_ref, plan, own)
    hits, named, place = named_ranks(plan, full, choice_ref)
    weights = []
    for e in range(2):
        total = jnp.zeros(named.shape, F32)
        for k, hit in enumerate(hits):
            for j in (2 * k, 2 * k + 1):
                chosen = hit & (le_ref[j : j + 1, :] == e)
                total += jnp.where(chosen, rw_ref[j : j + 1, :], 0.0)
        weights.append(total)
    full_shape = (plan.ranks, plan.chunk, LANE)
    flat = plan.ranks * plan.chunk
    j = iota(full_shape, 1)
    block, slot = chunk_index(j, plan, lane % 2, full)
    match = place.astype(I32)[:, None, :] == slot
    picks = [one_hot(match & (block == b)).reshape(flat, LANE) for b in range(3)]
    for copy in copies[4:]:
        copy.wait()
    total = sum(dot(picks[b], x_ref[:, b * LANE : (b + 1) * LANE]) for b in range(3))
    total = total.reshape(full_shape)
    total = jnp.where(j == plan.chunk - 2, weights[0][:, None, :], total)
    total = jnp.where(j == plan.chunk - 1, weights[1][:, None, :], total)
    out_ref[...] = total.astype(BF16)


def weight_rows(plan, data, expert):
    shape = (plan.ranks, plan.ranks * plan.chunk)
    at = iota(shape, 0) * plan.chunk + plan.chunk - 2 + expert
    return dot(one_hot(iota(shape, 1) == at), data)


def target_row(info_ref, plan, named):
    lane = info_ref[0]
    ranks, total = plan.ranks, plan.ranks * plan.chunk
    rank = iota((8, ranks), 1)
    fulls = jnp.zeros((8, ranks), I32)
    for i in range(plan.prefill):
        fulls += jnp.where(rank == info_ref[2 + i], 1, 0)
    ones = jnp.full((8, plan.rows), 1.0, BF16)
    counts = lax.dot_general(
        ones, named.astype(BF16), (((1,), (1,)), ((), ())), preferred_element_type=F32
    )
    decode = jnp.where(fulls > 0, 0.0, counts).astype(BF16)
    full = jnp.where(fulls > 0, 1.0, 0.0).astype(BF16)
    spread = (ranks, total)
    source = iota(spread, 1) // plan.chunk
    below = one_hot(iota(spread, 0) < source)
    here = one_hot(iota(spread, 0) == source)
    base = dot(decode, below).astype(I32)
    held = dot(decode, here).astype(I32)
    index = dot(full, below).astype(I32)
    full = dot(full, here) > 0.5
    needed = jnp.sum(decode.astype(F32), axis=1, keepdims=True)
    j = iota((8, total), 1) % plan.chunk
    block, slot = chunk_index(j, plan, lane % 2, full)
    half_rows = plan.decode // 2
    place = base + slot
    second = jnp.where(jnp.where(full, slot - plan.half_pre, place - half_rows) >= 0, 1, 0)
    row = jnp.where(
        full,
        index * plan.half_pre + slot - second * plan.half_pre,
        plan.prefill * plan.half_pre + place - second * half_rows,
    )
    kept = full | ((slot < held) & (place < plan.decode) & ((block < 2) | (second == lane % 2)))
    piece = jnp.where(block == 2, 4, 2 * block + second)
    return jnp.where(kept & (block < 3), piece * plan.half + row, -1), needed


def compact_kernel(plan, info_ref, in_ref, out_ref, target_ref, needed_ref):
    total = plan.ranks * plan.chunk
    data = in_ref[...].reshape(total, LANE)
    first = weight_rows(plan, data, 0)
    named = jnp.where(first > 0.0, 1.0, 0.0)
    target, needed = target_row(info_ref, plan, named)
    target_ref[...] = target
    needed_ref[...] = jnp.broadcast_to(needed, (8, LANE))
    for at in range(0, plan.packed, plan.half):
        take = one_hot(iota((plan.half, total), 0) + at == target[0:1, :])
        out_ref[at : at + plan.half, :] = dot(take, data).astype(BF16)


def weights_kernel(plan, in_ref, target_ref, weight_ref):
    total = plan.ranks * plan.chunk
    data = in_ref[...].reshape(total, LANE)
    first, second = weight_rows(plan, data, 0), weight_rows(plan, data, 1)
    place = places(plan, jnp.where(first > 0.0, 1.0, 0.0)).astype(I32)
    full_shape = (plan.ranks, plan.chunk, LANE)
    j = iota(full_shape, 1)
    match = (place[:, None, :] == j) & (j < plan.cap)
    target = target_ref[0:1, :]
    wide = []
    for value in (first, second):
        kept = jnp.where(match, value[:, None, :], 0.0)
        column = jnp.sum(kept, axis=2, keepdims=True)
        wide.append(jnp.broadcast_to(column, full_shape).reshape(total, LANE).astype(BF16))
    for piece in range(2):
        at = piece * plan.half
        take = one_hot(iota((plan.half, total), 0) + at == target)
        for e in range(2):
            weight_ref[at : at + plan.half, e * LANE : (e + 1) * LANE] = dot(take, wide[e])


def spread_table_kernel(plan, target_ref, spread_ref):
    total = plan.ranks * plan.chunk
    col = iota((LANE, LANE), 1)
    for g in range(0, total, LANE):
        wide = jnp.broadcast_to(target_ref[0:1, g : g + LANE], (LANE, LANE))
        column = wide.astype(F32).T.astype(I32)
        for at in range(0, plan.packed_up, LANE):
            spread_ref[g : g + LANE, at : at + LANE] = one_hot(col + at == column)


def combine_table_kernel(plan, info_ref, choice_ref, combine_ref):
    lane, own = info_ref[0], info_ref[1]
    ranks, rows = plan.ranks, plan.rows
    total = ranks * plan.chunk
    full = is_prefill(info_ref, plan, own)
    _, _, place = named_ranks(plan, full, choice_ref)
    square = jnp.concatenate([place, jnp.zeros((rows - ranks, rows), F32)], axis=0)
    turned = square.T[:, :ranks].astype(BF16)
    spread = (ranks, total)
    expand = one_hot(iota(spread, 1) // plan.chunk == iota(spread, 0))
    spots = dot(turned, expand).astype(I32)
    j = iota((1, total), 1) % plan.chunk
    block, slot = chunk_index(j, plan, lane % 2, full)
    match = spots == slot
    for b in range(3):
        combine_ref[:, b * total : (b + 1) * total] = one_hot(match & (block == b))


def expert_kernel(plan, offsets, info_ref, *refs):
    n = len(offsets)
    weight_ref, wg, wu, wd, out_ref, x_ref, h_ref = refs[n:]
    me, way = info_ref[0], 1 - 2 * lax.rem(info_ref[1], 2)
    lanes, half, slots = plan.lanes, plan.half, plan.slots
    for offset, part in zip(offsets, refs):
        lane = lax.rem(me + way * offset + lanes, lanes)
        first = pl.multiple_of(lane * (2 * LANE), LANE)
        tail = pl.multiple_of((2 * lanes + lane // 2) * LANE, LANE)
        start = pl.multiple_of(lax.rem(lane, 2) * half, 8)
        x_ref[:, pl.ds(first, LANE)] = part[0:slots, :]
        x_ref[:, pl.ds(pl.multiple_of(first + LANE, LANE), LANE)] = part[slots : 2 * slots, :]
        x_ref[pl.ds(start, half), pl.ds(tail, LANE)] = part[2 * slots : 2 * slots + half, :]
    turned = (((1,), (1,)), ((), ()))
    x = x_ref[...]
    gate = lax.dot_general(x, wg[...], turned, preferred_element_type=F32)
    up = lax.dot_general(x, wu[...], turned, preferred_element_type=F32)
    hidden = gate / (1.0 + jnp.exp(-gate)) * up * weight_ref[...]
    h_ref[...] = hidden.astype(BF16)
    for lane in range(lanes):
        at = lane * 2 * LANE
        y = dot(h_ref[...], wd[:, at : at + 2 * LANE]).astype(BF16)
        out_ref[lane, 0:slots, :] = y[:, :LANE]
        out_ref[lane, slots : 2 * slots, :] = y[:, LANE:]
    for pair in range(0, lanes // 2, 2):
        at = (2 * lanes + pair) * LANE
        y = dot(h_ref[...], wd[:, at : at + 2 * LANE]).astype(BF16)
        for k in range(2):
            for p in range(2):
                piece = y[p * half : (p + 1) * half, k * LANE : (k + 1) * LANE]
                out_ref[2 * (pair + k) + p, 2 * slots : 2 * slots + half, :] = piece


def spread_kernel(plan, take_ref, needed_ref, in_ref, out_ref, sum_ref):
    total = in_ref[0].astype(F32)
    for lane in range(1, plan.lanes):
        total += in_ref[lane].astype(F32)
    sum_ref[0 : plan.packed, :] = total.astype(BF16)
    sum_ref[plan.packed :, :] = jnp.zeros((plan.packed_up - plan.packed, LANE), BF16)
    shape = (plan.ranks, plan.chunk, LANE)
    spread = dot(take_ref[...], sum_ref[...]).reshape(shape)
    over = jnp.where(needed_ref[0:1, :] > float(plan.decode), 1.0, 0.0)
    spread = jnp.where(iota(shape, 1) == plan.chunk - 1, over[None], spread)
    out_ref[...] = spread.astype(BF16)


def combine_kernel(plan, take_ref, in_ref, out_ref, over_ref):
    total = plan.ranks * plan.chunk
    data = in_ref[...].reshape(total, LANE)
    own_rows = plan.own_rows
    for b in range(3):
        mine = dot(take_ref[:, b * total : (b + 1) * total], data).astype(BF16)
        for to in range(plan.lanes):
            out_ref[to, b * own_rows : (b + 1) * own_rows, :] = mine[
                to * own_rows : (to + 1) * own_rows
            ]
    shape = (8, total)
    flags = one_hot(iota(shape, 1) % plan.chunk == plan.chunk - 1)
    over_ref[0] = jnp.where(jnp.max(dot(flags, data)) > 0.0, 1, 0)


def finish_kernel(plan, in_ref, out_ref):
    n = plan.own_rows
    for lane in range(plan.lanes):
        at = lane * 2 * LANE
        out_ref[:, at : at + LANE] = in_ref[lane, 0:n, :]
        out_ref[:, at + LANE : at + 2 * LANE] = in_ref[lane, n : 2 * n, :]
    for pair in range(plan.lanes // 2):
        at = (2 * plan.lanes + pair) * LANE
        first = in_ref[2 * pair, 2 * n : 3 * n, :].astype(F32)
        second = in_ref[2 * pair + 1, 2 * n : 3 * n, :].astype(F32)
        out_ref[:, at : at + LANE] = (first + second).astype(BF16)


SMEM = pl.BlockSpec(memory_space=pltpu.SMEM)
VMEM = pl.BlockSpec(memory_space=pltpu.VMEM)
HBM = pl.BlockSpec(memory_space=pltpu.HBM)

def call(kernel, name, out, specs, *args, scratch=(), limit=24 << 20, flops=0):
    cost = None
    if flops:
        cost = pl.CostEstimate(flops=flops, bytes_accessed=1 << 20, transcendentals=0)
    return pl.pallas_call(
        kernel,
        out_shape=out,
        in_specs=specs,
        out_specs=jax.tree.map(lambda o: SMEM if o.shape == (1,) else VMEM, out),
        scratch_shapes=scratch,
        compiler_params=pltpu.CompilerParams(vmem_limit_bytes=limit),
        cost_estimate=cost,
        interpret=INTERPRET,
        name=name,
    )(*args)


def pack(plan, prefill_ranks, choice, local, weights, tokens):
    return call(
        lambda *refs: pack_kernel(plan, *refs),
        "pack",
        jax.ShapeDtypeStruct((plan.ranks, plan.chunk, LANE), BF16),
        [HBM] * 5,
        prefill_ranks,
        choice,
        local,
        weights,
        tokens,
        scratch=[
            pltpu.SMEM(prefill_ranks.shape, I32),
            pltpu.VMEM(choice.shape, I32),
            pltpu.VMEM(local.shape, I32),
            pltpu.VMEM(weights.shape, F32),
            pltpu.VMEM((plan.rows, 3 * LANE), BF16),
            pltpu.SemaphoreType.DMA((6,)),
        ],
    )


def compact(plan, info, received):
    return call(
        lambda *refs: compact_kernel(plan, Info(refs[0]), *refs[1:]),
        "compact",
        (
            jax.ShapeDtypeStruct((plan.packed, LANE), BF16),
            jax.ShapeDtypeStruct((8, plan.ranks * plan.chunk), I32),
            jax.ShapeDtypeStruct((8, LANE), F32),
        ),
        [SMEM, VMEM],
        info,
        received,
    )


def weights_table(plan, received, target):
    return call(
        lambda *refs: weights_kernel(plan, *refs),
        "weights",
        jax.ShapeDtypeStruct((plan.slots, 2 * LANE), F32),
        [VMEM, VMEM],
        received,
        target,
        flops=1 << 29,
    )


def spread_table(plan, target):
    return call(
        lambda *refs: spread_table_kernel(plan, *refs),
        "spread_table",
        jax.ShapeDtypeStruct((plan.ranks * plan.chunk, plan.packed_up), BF16),
        [VMEM],
        target,
        flops=1 << 29,
    )


def combine_table(plan, info, choice):
    return call(
        lambda *refs: combine_table_kernel(plan, Info(refs[0]), *refs[1:]),
        "combine_table",
        jax.ShapeDtypeStruct((plan.rows, 3 * plan.ranks * plan.chunk), BF16),
        [SMEM, VMEM],
        info,
        choice,
        flops=1 << 29,
    )


def experts(plan, offsets, info, parts, weights, w_gate, w_up, w_down):
    hidden = w_gate.shape[0] * w_gate.shape[1]
    flat = [w.reshape(hidden, plan.width) for w in (w_gate, w_up, w_down)]
    return call(
        lambda *refs: expert_kernel(plan, offsets, Info(refs[0]), *refs[1:]),
        "experts",
        jax.ShapeDtypeStruct((plan.lanes, plan.packed, LANE), BF16),
        [SMEM] + [VMEM] * (len(parts) + 4),
        info,
        *parts,
        weights,
        *flat,
        scratch=[
            pltpu.VMEM((plan.slots, plan.width), BF16),
            pltpu.VMEM((plan.slots, hidden), BF16),
        ],
        limit=32 << 20,
    )


def spread(plan, take, needed, returned):
    return call(
        lambda *refs: spread_kernel(plan, *refs),
        "spread",
        jax.ShapeDtypeStruct((plan.ranks, plan.chunk, LANE), BF16),
        [VMEM] * 3,
        take,
        needed,
        returned,
        scratch=[pltpu.VMEM((plan.packed_up, LANE), BF16)],
    )


def combine(plan, take, back):
    return call(
        lambda *refs: combine_kernel(plan, *refs),
        "combine",
        (
            jax.ShapeDtypeStruct((plan.lanes, 3 * plan.own_rows, LANE), BF16),
            jax.ShapeDtypeStruct((1,), I32),
        ),
        [VMEM, VMEM],
        take,
        back,
    )


def finish(plan, shares):
    return call(
        lambda *refs: finish_kernel(plan, *refs),
        "finish",
        jax.ShapeDtypeStruct((plan.own_rows, plan.width), BF16),
        [VMEM],
        shares,
    )


def gather_lanes(packed, lanes, beside):
    ranks = lax.axis_size("ep")
    ways = []
    for way in (1, -1):
        steps = [way if rank % 2 == 0 else -way for rank in range(ranks)]
        ways.append(
            [
                (rank * lanes + i, rank * lanes + (i + steps[rank]) % lanes)
                for rank in range(ranks)
                for i in range(lanes)
            ]
        )
    right, left = ways
    axes = ("ep", "tp")
    parts, offsets, values = [packed], [0], []
    held = [packed, packed]
    for hop in range(1, lanes // 2 + 1):
        if hop > 1 and hop - 2 < len(beside) - 1 and hop < lanes // 2:
            first, value = lax.optimization_barrier((held[0], beside[hop - 2]))
            held = [first, held[1]]
            values.append(value)
        got = [lax.ppermute(held[0], axes, right)]
        offsets.append(-hop)
        if hop < lanes // 2:
            got.append(lax.ppermute(held[1], axes, left))
            offsets.append(hop)
        parts += got
        held = got
    last, rest = lax.optimization_barrier((parts[-1], beside[len(values) :]))
    return parts[:-1] + [last], offsets, values + list(rest)


def through_experts(plan, info, received, take_in, matrices):
    packed, target, needed = compact(plan, info, received)
    beside = [weights_table(plan, received, target), spread_table(plan, target), take_in]
    parts, offsets, beside = gather_lanes(packed, plan.lanes, beside)
    weights, take_out, take_in = beside
    partial = experts(plan, offsets, info, parts, weights, *matrices)
    returned = lax.all_to_all(partial, "tp", 0, 0, tiled=True)
    back = lax.all_to_all(spread(plan, take_out, needed, returned), "ep", 0, 0, tiled=True)
    return combine(plan, take_in, back)


def on_device(
    tokens, device_choice, local_expert, route_weight, prefill_ranks, w_gate, w_up, w_down
):
    ranks, prefill = lax.axis_size("ep"), prefill_ranks.shape[0]
    sizes = (ranks, lax.axis_size("tp"), *tokens.shape, prefill)
    most = (ranks - prefill) * DEC_RANK
    plan, whole = Plan(*sizes, min(USUAL_DECODE, most)), Plan(*sizes, most)
    stay = [prefill_ranks, device_choice.T, local_expert.T, route_weight.T, tokens]
    stay = [pltpu.with_memory_space_constraint(x, pltpu.HBM) for x in stay]
    outgoing = pack(plan, *stay)
    received = lax.all_to_all(outgoing, "ep", 0, 0, tiled=True)
    received, info, choice = lax.optimization_barrier((received, stay[0], stay[1]))
    take_in = combine_table(plan, info, choice)
    rest = (info, received, take_in, (w_gate, w_up, w_down))
    shares, over = through_experts(plan, *rest)
    rest, over = lax.optimization_barrier((rest, over))
    shares = lax.cond(
        over[0] > 0, lambda: through_experts(whole, *rest)[0], lambda: shares
    )
    shares = lax.all_to_all(shares, "tp", 0, 0, tiled=True)
    return finish(plan, shares)


def solution(mesh):
    in_specs = (
        P(("groups", "ep"), None),
        P(("groups", "ep"), None),
        P(("groups", "ep"), None),
        P(("groups", "ep"), None),
        P("groups"),
        P("ep", "tp", None),
        P("ep", "tp", None),
        P("ep", "tp", None),
    )
    out_specs = P(("groups", "ep", "tp"), None)
    return jax.shard_map(
        on_device, mesh=mesh, in_specs=in_specs, out_specs=out_specs, check_vma=False
    )
```
